32 devices in a mesh: dp: 16 (over z, x, core), mp: 2 (over y).
Axes of the slice: x: 2, y: 2, z: 4, core: 2. Of those that a mesh axis runs over, the one named last changes fastest.
Arguments:
- tokens: bfloat16 [16384, 768], P('dp', 'mp'), may hold values from -6 to 6
- crop_counts: int32 [96], P('dp'), may hold values from 3 to 8, as said below
- crop_patches: int32 [96, 8], P('dp'), may hold values from 9 to 49, as said below
- rel_index: int32 [49, 49], replicated, may hold values from 0 to 168
- ln1_gain: float32 [768], replicated, may hold values from 0.5 to 1.5
- ln1_shift: float32 [768], replicated, may hold values from -4 to 4
- w_qkv: bfloat16 [768, 3, 768], P(None, None, 'mp'), may hold values from -0.21875 to 0.21875
- qv_bias: float32 [2, 768], P(None, 'mp'), may hold values from -4 to 4
- rel_table: float32 [169, 24], P(None, 'mp'), may hold values from -6 to 6
- w_out: bfloat16 [768, 768], P('mp'), may hold values from -0.875 to 0.875
- b_out: float32 [768], replicated, may hold values from -4 to 4
- ln2_gain: float32 [768], replicated, may hold values from 0.5 to 1.5
- ln2_shift: float32 [768], replicated, may hold values from -4 to 4
- w_in: bfloat16 [768, 3072], P(None, 'mp'), may hold values from -0.21875 to 0.21875
- b_in: float32 [3072], P('mp'), may hold values from -4 to 4
- w_back: bfloat16 [3072, 768], P('mp'), may hold values from -0.109375 to 0.109375
- b_back: float32 [768], replicated, may hold values from -4 to 4
- cotangent: bfloat16 [16384, 768], P('dp', 'mp'), may hold values from -6 to 6
Outputs:
- out_tokens: bfloat16 [16384, 768], P('dp', 'mp')
- grad_tokens: bfloat16 [16384, 768], P('dp', 'mp')
- grad_ln1_gain: float32 [768], replicated
- grad_ln1_shift: float32 [768], replicated
- grad_w_qkv: float32 [768, 3, 768], P(None, None, 'mp')
- grad_qv_bias: float32 [2, 768], P(None, 'mp')
- grad_rel_table: float32 [169, 24], P(None, 'mp')
- grad_w_out: float32 [768, 768], P('mp')
- grad_b_out: float32 [768], replicated
- grad_ln2_gain: float32 [768], replicated
- grad_ln2_shift: float32 [768], replicated
- grad_w_in: float32 [768, 3072], P(None, 'mp')
- grad_b_in: float32 [3072], P('mp')
- grad_w_back: float32 [3072, 768], P('mp')
- grad_b_back: float32 [768], replicated
The draws below stay inside these ranges and needn't reach their ends.
Inputs may be any that keep to these rules, and one draw needn't show every extreme that they name: Image i has crop_counts[i] crops; among every group's 6 images one has exactly 8. `crop_patches`: crop 0 of every image has 49 patches, crop 1 has 49 or 9, all later crops 9; entries past an image's crop count are not used.
All inputs are finite; a program needn't handle non-finite values.
Results may differ from the reference program's by a relative error of at most 0.019.
Values may be sent and summed in bfloat16 or wider, within the bound.
A program may use at most 256 MiB of HBM per device.

```python
from functools import partial
import jax
import jax.numpy as jnp
from jax import lax

D = 768
HEADS = 24
HEAD_DIM = 32
FF = 3072
SIDE = 7
LOCAL_SIDE = 3
CELLS = 49
LOCAL_CELLS = 9
OFFSETS = 169
CROP_MAX = 8
IMG_DEV = 6
TOK_DEV = 1024
TOKENS = 16384
IMAGES = 96
N_DP = 16


def draw_crop_counts(key, part):
    drawn = jax.random.randint(jax.random.fold_in(key, 11), (N_DP, IMG_DEV), 3, CROP_MAX + 1, dtype=jnp.int32)
    chosen = jax.random.randint(jax.random.fold_in(key, 12), (N_DP, 1), 0, IMG_DEV, dtype=jnp.int32)
    image_slot = jnp.arange(IMG_DEV, dtype=jnp.int32)[None, :]
    return jnp.where(image_slot == chosen, CROP_MAX, drawn).reshape(IMAGES).astype(jnp.int32)


def draw_crop_patches(key, part):
    global_count = jax.random.randint(jax.random.fold_in(key, 13), (IMAGES, 1), 1, 3, dtype=jnp.int32)
    crop_slot = jnp.arange(CROP_MAX, dtype=jnp.int32)[None, :]
    return jnp.where(crop_slot < global_count, CELLS, LOCAL_CELLS).astype(jnp.int32)


def with_ends(values, key, least, top_value):
    longest = values.shape.index(max(values.shape))
    spots = []
    for shift in (0, 1):
        where = [jax.random.randint(jax.random.fold_in(key, axis), (), 0, length) for axis, length in enumerate(values.shape)]
        where[longest] = (where[longest] + shift) % values.shape[longest]
        spots.append(tuple(where))
    return values.at[spots[0]].set(least).at[spots[1]].set(top_value)


def block_scale(key, extent, cuts, smallest, top_value):
    def one(axis_at, parts):
        steps = jax.random.uniform(jax.random.fold_in(jax.random.fold_in(key, 6), axis_at), (parts,), jnp.float32, smallest / len(cuts), top_value / len(cuts))
        return jnp.repeat(jnp.exp(steps), extent[axis_at] // parts).reshape((-1,) + (1,) * (len(extent) - axis_at - 1))

    loudness = one(*cuts[0])
    for cut in cuts[1:]:
        loudness = loudness * one(*cut)
    return loudness


def noise(rng, shape, width, reach, cuts=(), kind=jnp.bfloat16):
    values = jax.random.normal(rng, shape, jnp.float32) * width
    if len(cuts) > 0:
        values = block_scale(rng, shape, cuts, -0.22, 0.18) * values
    return jnp.clip(values, min=-reach, max=reach).astype(kind)


def setup_inputs(seed: int = 0) -> dict:
    splits = jax.random.split(jax.random.key(seed), 19)
    tokens = noise(splits[0], (TOKENS, D), 1.0, 6.0, ((0, 16), (1, 2)))
    crop_counts = draw_crop_counts(jax.random.fold_in(splits[18], 71), 0)
    crop_patches = draw_crop_patches(jax.random.fold_in(splits[18], 71), 0)
    rel_index = with_ends(jax.random.randint(splits[3], (CELLS, CELLS), 0, OFFSETS), jax.random.fold_in(splits[3], 1), 0, OFFSETS - 1).astype(jnp.int32)
    ln1_gain = jnp.clip(1.0 + 0.1 * jax.random.normal(splits[4], (D,), jnp.float32), 0.5, 1.5)
    ln1_shift = noise(splits[5], (D,), 0.3, 4.0, (), jnp.float32)
    w_qkv = noise(splits[6], (D, 3, D), D ** -0.5, 0.21875, ((2, 2),))
    qv_bias = noise(splits[7], (2, D), 0.3, 4.0, ((1, 2),), jnp.float32)
    rel_table = noise(splits[8], (OFFSETS, HEADS), 1.0, 6.0, ((1, 2),), jnp.float32)
    w_out = noise(splits[9], (D, D), (D // 16) ** -0.5, 0.875, ((0, 2),))
    b_out = noise(splits[10], (D,), 0.3, 4.0, (), jnp.float32)
    ln2_gain = jnp.clip(1.0 + 0.1 * jax.random.normal(splits[11], (D,), jnp.float32), 0.5, 1.5)
    ln2_shift = noise(splits[12], (D,), 0.3, 4.0, (), jnp.float32)
    w_in = noise(splits[13], (D, FF), D ** -0.5, 0.21875, ((1, 2),))
    b_in = noise(splits[14], (FF,), 0.3, 4.0, ((0, 2),), jnp.float32)
    w_back = noise(splits[15], (FF, D), FF ** -0.5, 0.109375, ((0, 2),))
    b_back = noise(splits[16], (D,), 0.3, 4.0, (), jnp.float32)
    cotangent = noise(splits[17], (TOKENS, D), 1.0, 6.0, ((0, 16), (1, 2)))
    return dict(tokens=tokens, crop_counts=crop_counts, crop_patches=crop_patches, rel_index=rel_index, ln1_gain=ln1_gain, ln1_shift=ln1_shift, w_qkv=w_qkv, qv_bias=qv_bias, rel_table=rel_table, w_out=w_out, b_out=b_out, ln2_gain=ln2_gain, ln2_shift=ln2_shift, w_in=w_in, b_in=b_in, w_back=w_back, b_back=b_back, cotangent=cotangent)


EPS = 1e-05
NEG = -1e+30

@jax.custom_vjp
def low(v):
    return lax.optimization_barrier(v.astype(jnp.bfloat16)).astype(jnp.float32)

@jax.custom_vjp
def low_back(v):
    return v

def low_keep(v):
    return (low(v), None)

def low_pass(kept, grad):
    return (grad,)

def back_keep(v):
    return (v, None)

def back_low(kept, grad):
    return (low(grad),)
low.defvjp(low_keep, low_pass)
low_back.defvjp(back_keep, back_low)

def layout(counts, patches, row_count):
    live_crop = jnp.arange(CROP_MAX, dtype=jnp.int32)[None, :] < counts[:, None]
    crop_rows = jnp.where(live_crop, patches, 0).reshape(-1).astype(jnp.int32)
    crop_ends = jnp.cumsum(crop_rows).astype(jnp.int32)
    used_rows = crop_ends[-1]
    row_ids = jnp.arange(row_count, dtype=jnp.int32)
    passed = crop_ends[None, :] <= row_ids[:, None]
    window = lax.optimization_barrier(jnp.sum(passed.astype(jnp.int32), axis=1)).astype(jnp.int32)
    starts = lax.optimization_barrier(jnp.max(jnp.where(passed, crop_ends[None, :], 0), axis=1)).astype(jnp.int32)
    finish = lax.optimization_barrier(jnp.min(jnp.where(passed, row_count + used_rows + 1, crop_ends[None, :]), axis=1)).astype(jnp.int32)
    length = finish - starts
    offset = row_ids - starts
    grid_side = jnp.where(length >= CELLS, SIDE, LOCAL_SIDE).astype(jnp.int32)
    cell_index = (offset // grid_side * SIDE + offset % grid_side).astype(jnp.int32)
    inside = row_ids < used_rows
    cell_ids = jnp.where(inside, cell_index, 0).astype(jnp.int32)
    windows = jnp.where(inside, window, crop_rows.shape[0] + row_ids - used_rows).astype(jnp.int32)
    return (cell_ids, windows)

def layer_norm(values, gain, shift):
    center = values - lax.optimization_barrier(jnp.mean(values, axis=-1, keepdims=True))
    spread = lax.optimization_barrier(jnp.mean(center * center, axis=-1, keepdims=True))
    return center * lax.rsqrt(spread + EPS) * gain + shift

def reference(tokens, crop_counts, crop_patches, rel_index, ln1_gain, ln1_shift, w_qkv, qv_bias, rel_table, w_out, b_out, ln2_gain, ln2_shift, w_in, b_in, w_back, b_back, cotangent):
    highest = lax.Precision.HIGHEST
    counts = crop_counts.reshape(N_DP, IMG_DEV)
    patches = crop_patches.reshape(N_DP, IMG_DEV, CROP_MAX)
    cell_ids, windows = jax.vmap(partial(layout, row_count=TOK_DEV))(counts, patches)
    floats = tuple((item.astype(jnp.float32) for item in (tokens, ln1_gain, ln1_shift, w_qkv, qv_bias, rel_table, w_out, b_out, ln2_gain, ln2_shift, w_in, b_in, w_back, b_back)))

    def forward(block_x, gain_one, shift_one, proj_qkv, bias_qv, table_f, proj_out, bias_out, gain_two, shift_two, proj_in, bias_in, proj_back, bias_back):

        def one_group(group_data):
            x_group, group_cells, group_windows = group_data
            mixer_in = low(layer_norm(x_group, gain_one, shift_one))
            projected = jnp.einsum('td,dcf->tcf', mixer_in, proj_qkv, precision=highest)
            queries = low_back(low(projected[:, 0] + bias_qv[0])).reshape(-1, HEADS, HEAD_DIM)
            key_proj = low_back(low(projected[:, 1])).reshape(-1, HEADS, HEAD_DIM)
            value_proj = low_back(low(projected[:, 2] + bias_qv[1])).reshape(-1, HEADS, HEAD_DIM)
            raw_scores = jnp.einsum('qhd,khd->hqk', queries, key_proj, precision=highest) * HEAD_DIM ** (-0.5)
            pair_bias = jnp.transpose(table_f[rel_index[group_cells[:, None], group_cells[None, :]]], (2, 0, 1))
            same_window = (group_windows[:, None] == group_windows[None, :])[None]
            scores = low_back(jnp.where(same_window, raw_scores + pair_bias, NEG))
            weights = low(jax.nn.softmax(scores, axis=-1))
            heads_out = low_back(low(jnp.einsum('hqk,khd->qhd', weights, value_proj, precision=highest).reshape(-1, D)))
            mixer_out = low_back(jnp.dot(heads_out, proj_out, precision=highest) + bias_out)
            residual = x_group + mixer_out
            hidden_in = low(layer_norm(residual, gain_two, shift_two))
            hidden_pre = low_back(jnp.dot(hidden_in, proj_in, precision=highest) + bias_in)
            activated = low(jax.nn.gelu(hidden_pre, approximate=False))
            return residual + low_back(jnp.dot(activated, proj_back, precision=highest) + bias_back)
        outputs = lax.map(jax.checkpoint(one_group), (block_x.reshape(N_DP, TOK_DEV, D), cell_ids, windows))
        return outputs.reshape(TOKENS, D)
    result, pull_back = jax.vjp(forward, *floats)
    grads = pull_back(cotangent.astype(jnp.float32))
    return (result.astype(jnp.bfloat16), grads[0].astype(jnp.bfloat16), grads[1], grads[2], grads[3], grads[4], grads[5], grads[6], grads[7], grads[8], grads[9], grads[10], grads[11], grads[12], grads[13])
```

```python
from functools import partial

import jax
import jax.numpy as jnp
from jax import lax
from jax.experimental import pallas as pl
from jax.experimental.pallas import tpu as pltpu
from jax.sharding import PartitionSpec as P

HEAD_DIM = 32
SIDE = 7
LOCAL_SIDE = 3
CELLS = 49
OFFSETS = 169
CROP_MAX = 8
QB = 128
HALO = 64
SPAN = QB + 2 * HALO
CP = 64
GROUP = 4
SCALE = HEAD_DIM ** (-0.5)
EPS = 1e-05
NEG = -1e30
F32 = jnp.float32
BF16 = jnp.bfloat16


def layout(counts, patches, row_count):
    live_crop = jnp.arange(CROP_MAX, dtype=jnp.int32)[None, :] < counts[:, None]
    crop_rows = jnp.where(live_crop, patches, 0).reshape(-1)
    crop_ends = jnp.cumsum(crop_rows)
    used_rows = crop_ends[-1]
    row_ids = jnp.arange(row_count, dtype=jnp.int32)
    passed = crop_ends[None, :] <= row_ids[:, None]
    window = jnp.sum(passed.astype(jnp.int32), axis=1)
    starts = jnp.max(jnp.where(passed, crop_ends[None, :], 0), axis=1)
    finish = jnp.min(jnp.where(passed, row_count + used_rows + 1, crop_ends[None, :]), axis=1)
    length = finish - starts
    offset = row_ids - starts
    grid_side = jnp.where(length >= CELLS, SIDE, LOCAL_SIDE).astype(jnp.int32)
    cell_index = offset // grid_side * SIDE + offset % grid_side
    inside = row_ids < used_rows
    cell_ids = jnp.where(inside, cell_index, 0)
    windows = jnp.where(inside, window, crop_rows.shape[0] + row_ids - used_rows)
    return (cell_ids, windows)


def layer_norm(values, gain, shift):
    center = values - jnp.mean(values, axis=-1, keepdims=True)
    spread = jnp.mean(center * center, axis=-1, keepdims=True)
    return center * lax.rsqrt(spread + EPS) * gain + shift


def dot(a, b):
    return jnp.dot(a, b, preferred_element_type=F32)


def dot_nt(a, b):
    return lax.dot_general(a, b, (((1,), (1,)), ((), ())), preferred_element_type=F32)


def stack_heads(rows_t):
    cols = []
    for j in range(GROUP):
        parts = []
        if j > 0:
            parts.append(jnp.zeros((HEAD_DIM * j, QB), BF16))
        parts.append(rows_t[HEAD_DIM * j : HEAD_DIM * (j + 1)])
        if j < GROUP - 1:
            parts.append(jnp.zeros((HEAD_DIM * (GROUP - 1 - j), QB), BF16))
        cols.append(jnp.concatenate(parts, axis=0))
    return jnp.concatenate(cols, axis=1)


def bias_rows(table, g, cells):
    tall = dot(table[2 * CP * GROUP * g : 2 * CP * GROUP * (g + 1), :], cells).astype(BF16)
    return jnp.concatenate([tall[2 * CP * j : 2 * CP * (j + 1)] for j in range(GROUP)], axis=1)


def attn_fwd_kernel(
    groups, tok, gain, shift, wt, qb_col, vb_col, vb_row, khot, qhott, table, kwin, qwin,
    a_out, qt, kx, kt, vx, o_out, lse, a_pad, vt,
):
    step = pl.program_id(0)
    rows_all = tok.shape[0]
    width = qt.shape[0]

    @pl.when(step == 0)
    def _():
        zero = jnp.zeros((HALO, tok.shape[1]), BF16)
        a_pad[:HALO, :] = zero
        a_pad[HALO + rows_all :, :] = zero

        def norm_rows(i, carry):
            at = pl.multiple_of(i * QB, QB)
            a = layer_norm(tok[pl.ds(at, QB), :].astype(F32), gain[...], shift[...]).astype(BF16)
            a_out[pl.ds(at, QB), :] = a
            a_pad[pl.ds(pl.multiple_of(at + HALO, HALO), QB), :] = a
            return carry

        lax.fori_loop(0, rows_all // QB, norm_rows, 0)
        a_all = a_pad[...]
        wk = wt[width : 2 * width, :]
        wv = wt[2 * width :, :]
        qt[...] = (dot_nt(wt[:width, :], a_out[...]) + qb_col[...]).astype(BF16)
        kx[...] = dot_nt(a_all, wk).astype(BF16)
        kt[...] = dot_nt(wk, a_all).astype(BF16)
        vx[...] = (dot_nt(a_all, wv) + vb_row[...]).astype(BF16)
        vt[...] = (dot_nt(wv, a_all) + vb_col[...]).astype(BF16)

    start = pl.multiple_of(step * QB, QB)
    span = pl.ds(start, SPAN)
    mask = jnp.where(kwin[span, :] == qwin[...], 0.0, NEG)
    hot = khot[span, :]
    cells = qhott[...]
    for g in range(groups):
        lanes = slice(128 * g, 128 * (g + 1))
        right = jnp.concatenate(
            [stack_heads(qt[lanes, pl.ds(start, QB)]), bias_rows(table, g, cells)], axis=0
        )
        scores = dot(jnp.concatenate([kx[span, lanes], hot], axis=1), right)
        outs = []
        for j in range(GROUP):
            h = GROUP * g + j
            s = scores[:, QB * j : QB * (j + 1)] * SCALE + mask
            peak = jnp.max(s, axis=0, keepdims=True)
            e = jnp.exp(s - peak)
            mass = jnp.sum(e, axis=0, keepdims=True)
            outs.append(dot(vt[HEAD_DIM * h : HEAD_DIM * (h + 1), span], e.astype(BF16)) / mass)
            lse[h : h + 1, :] = peak + jnp.log(mass)
        o_out[:, lanes] = jnp.concatenate(outs, axis=0).T.astype(BF16)


def whole(a):
    return pl.BlockSpec(a.shape, lambda i: (0,) * len(a.shape))


def same(*shape):
    return pl.BlockSpec(shape, lambda i: (0,) * len(shape))


def cols(n):
    return pl.BlockSpec((n, QB), lambda i: (0, i))


def attn_fwd(tok, gain, shift, wt, qb_col, vb_col, vb_row, khot, qhott, table, kwin, qwin):
    rows, model = tok.shape
    width = wt.shape[0] // 3
    heads = width // HEAD_DIM
    ext = rows + 2 * HALO
    shape = jax.ShapeDtypeStruct
    return pl.pallas_call(
        partial(attn_fwd_kernel, heads // GROUP),
        grid=(rows // QB,),
        in_specs=[whole(x) for x in (tok, gain, shift, wt, qb_col, vb_col, vb_row, khot)]
        + [cols(CP), whole(table), whole(kwin), cols(1)],
        out_specs=[
            same(rows, model), same(width, rows), same(ext, width), same(width, ext), same(ext, width),
            pl.BlockSpec((QB, width), lambda i: (i, 0)), cols(heads),
        ],
        out_shape=[
            shape((rows, model), BF16), shape((width, rows), BF16), shape((ext, width), BF16),
            shape((width, ext), BF16), shape((ext, width), BF16), shape((rows, width), BF16),
            shape((heads, rows), F32),
        ],
        scratch_shapes=[pltpu.VMEM((ext, model), BF16), pltpu.VMEM((width, ext), BF16)],
        name="attn_fwd",
    )(tok, gain, shift, wt, qb_col, vb_col, vb_row, khot, qhott, table, kwin, qwin)


def attn_bwd_kernel(
    groups, qt, kx, kt, vx, dot_t, khot, khott, qhott, qhot, table, kwin, qwin, lse,
    dq, dk, dv, gcell, dk_acc, dv_acc,
):
    step = pl.program_id(0)
    rows_all = dk.shape[0]

    @pl.when(step == 0)
    def _():
        dk_acc[...] = jnp.zeros_like(dk_acc)
        dv_acc[...] = jnp.zeros_like(dv_acc)
        gcell[...] = jnp.zeros_like(gcell)

    start = pl.multiple_of(step * QB, QB)
    span = pl.ds(start, SPAN)
    mask = jnp.where(kwin[span, :] == qwin[...], 0.0, NEG)
    hot = khot[span, :]
    hot_t = khott[:, span]
    cells = qhott[...]
    cells_r = qhot[...]
    for g in range(groups):
        lanes = slice(128 * g, 128 * (g + 1))
        q_stack = stack_heads(qt[lanes, :])
        do_stack = stack_heads(dot_t[lanes, :])
        right = jnp.concatenate([q_stack, bias_rows(table, g, cells)], axis=0)
        scores = dot(jnp.concatenate([kx[span, lanes], hot], axis=1), right)
        dprob = dot(vx[span, lanes], do_stack)
        ps, dss, dqs = [], [], []
        for j in range(GROUP):
            h = GROUP * g + j
            cut = slice(QB * j, QB * (j + 1))
            p = jnp.exp(scores[:, cut] * SCALE + mask - lse[h : h + 1, :])
            t = p * dprob[:, cut]
            inner = jnp.sum(t, axis=0, keepdims=True)
            ds = (t - p * inner).astype(BF16)
            ps.append(p.astype(BF16))
            dss.append(ds)
            both = dot(jnp.concatenate([kt[HEAD_DIM * h : HEAD_DIM * (h + 1), span], hot_t], axis=0), ds)
            dqs.append(both[:HEAD_DIM])
            gcell[CP * h : CP * (h + 1), :] += dot(both[HEAD_DIM:].astype(BF16), cells_r)
        dq[:, lanes] = (jnp.concatenate(dqs, axis=0) * SCALE).T.astype(BF16)
        dk_acc[span, lanes] += dot_nt(jnp.concatenate(dss, axis=1), q_stack)
        dv_acc[span, lanes] += dot_nt(jnp.concatenate(ps, axis=1), do_stack)

    @pl.when(step == pl.num_programs(0) - 1)
    def _():
        own = pl.ds(HALO, rows_all)
        dk[...] = (dk_acc[own, :] * SCALE).astype(BF16)
        dv[...] = dv_acc[own, :].astype(BF16)


def attn_bwd(qt, kx, kt, vx, dot_t, khot, khott, qhott, qhot, table, kwin, qwin, lse):
    width, rows = qt.shape
    heads = width // HEAD_DIM
    ext = rows + 2 * HALO
    shape = jax.ShapeDtypeStruct
    rblk = lambda n: pl.BlockSpec((QB, n), lambda i: (i, 0))
    return pl.pallas_call(
        partial(attn_bwd_kernel, heads // GROUP),
        grid=(rows // QB,),
        in_specs=[
            cols(width), whole(kx), whole(kt), whole(vx), cols(width), whole(khot), whole(khott),
            cols(CP), rblk(CP), whole(table), whole(kwin), cols(1), cols(heads),
        ],
        out_specs=[rblk(width), same(rows, width), same(rows, width), same(CP * heads, CP)],
        out_shape=[
            shape((rows, width), BF16), shape((rows, width), BF16), shape((rows, width), BF16),
            shape((CP * heads, CP), F32),
        ],
        scratch_shapes=[pltpu.VMEM((ext, width), F32), pltpu.VMEM((ext, width), F32)],
        name="attn_bwd",
    )(qt, kx, kt, vx, dot_t, khot, khott, qhott, qhot, table, kwin, qwin, lse)


def window_data(crop_counts, crop_patches, rel_index, rel_table, rows):
    highest = lax.Precision.HIGHEST
    heads = rel_table.shape[1]
    cells, wins = layout(crop_counts, crop_patches, rows)
    kcells = jnp.pad(cells, (HALO, HALO))
    kwin = jnp.pad(wins, (HALO, HALO), constant_values=-1)[:, None]
    span_cells = jnp.arange(CP, dtype=jnp.int32)
    wide_cells = jnp.arange(2 * CP, dtype=jnp.int32) % CP
    khot = (kcells[:, None] == wide_cells[None, :]).astype(BF16)
    khott = (span_cells[:, None] == kcells[None, :]).astype(BF16)
    qhott = (span_cells[:, None] == cells[None, :]).astype(BF16)
    qhot = (cells[:, None] == span_cells[None, :]).astype(BF16)
    rel_t = jnp.pad(rel_index.T, ((0, CP - CELLS), (0, CP - CELLS)), constant_values=-1).reshape(-1)
    offset_hot = (rel_t[:, None] == jnp.arange(OFFSETS, dtype=jnp.int32)[None, :]).astype(F32)
    bias = jnp.einsum("pm,mh->hp", offset_hot, rel_table, precision=highest) / SCALE
    high = bias.astype(BF16)
    rest = (bias - high.astype(F32)).astype(BF16)
    table = jnp.stack([high.reshape(heads, CP, CP), rest.reshape(heads, CP, CP)], axis=1)
    return (khot, khott, qhott, qhot, table.reshape(heads * 2 * CP, CP), kwin, wins[None, :], offset_hot)


def body(
    tokens,
    crop_counts,
    crop_patches,
    rel_index,
    ln1_gain,
    ln1_shift,
    w_qkv,
    qv_bias,
    rel_table,
    w_out,
    b_out,
    ln2_gain,
    ln2_shift,
    w_in,
    b_in,
    w_back,
    b_back,
    cotangent,
):
    highest = lax.Precision.HIGHEST
    rows, part_width = tokens.shape
    model = ln1_gain.shape[0]
    width = w_qkv.shape[2]
    heads = width // HEAD_DIM
    khot, khott, qhott, qhot, table, kwin, qwin, offset_hot = window_data(
        crop_counts, crop_patches, rel_index, rel_table, rows
    )
    column_start = lax.axis_index("mp") * part_width
    whole_in = lax.all_gather(tokens, "mp", axis=1, tiled=True)
    w_out_all = lax.all_gather(w_out, "mp", axis=0, tiled=True)
    whole_cot = lax.all_gather(cotangent, "mp", axis=1, tiled=True)
    wt = jnp.transpose(w_qkv, (1, 2, 0)).reshape(3 * width, model)
    mixer_in, qt, kx, kt, vx, heads_out, lse = attn_fwd(
        whole_in, ln1_gain[None, :], ln1_shift[None, :], wt, qv_bias[0][:, None], qv_bias[1][:, None],
        qv_bias[1][None, :], khot, qhott, table, kwin, qwin,
    )
    block_input = whole_in.astype(F32)
    heads_all = lax.all_gather(heads_out, "mp", axis=1, tiled=True)
    residual = block_input + dot(heads_all, w_out_all) + b_out
    hidden_in = layer_norm(residual, ln2_gain, ln2_shift).astype(BF16)
    hidden_pre = dot(hidden_in, w_in) + b_in
    activated = jax.nn.gelu(hidden_pre, approximate=False).astype(BF16)
    back_terms = dot(activated, w_back)
    grad_w_back = jnp.einsum("tf,td->fd", activated, whole_cot, preferred_element_type=F32)
    grad_act = jnp.einsum("td,fd->tf", whole_cot, w_back, preferred_element_type=F32)
    unused_gelu, gelu_pull = jax.vjp(partial(jax.nn.gelu, approximate=False), hidden_pre)
    grad_pre = gelu_pull(grad_act)[0].astype(BF16)
    hidden_terms = jnp.einsum("tf,df->td", grad_pre, w_in, preferred_element_type=F32)
    grad_normed_two = lax.psum(hidden_terms.astype(BF16), "mp").astype(F32)
    grad_b_back = jnp.sum(whole_cot.astype(F32), axis=0)
    grad_b_in = jnp.sum(grad_pre.astype(F32), axis=0)
    grad_w_in = jnp.einsum("td,tf->df", hidden_in, grad_pre, preferred_element_type=F32)
    unused_two, norm_two_pull = jax.vjp(layer_norm, residual, ln2_gain, ln2_shift)
    grad_resid_norm, grad_g2, grad_c2 = norm_two_pull(grad_normed_two)
    grad_resid = whole_cot.astype(F32) + grad_resid_norm
    grad_mixer = grad_resid.astype(BF16)
    grad_b_out = jnp.sum(grad_mixer.astype(F32), axis=0)
    grad_w_out = jnp.einsum("tf,td->fd", heads_out, grad_mixer, preferred_element_type=F32)
    grad_heads_t = jnp.einsum("fd,td->ft", w_out, grad_mixer, preferred_element_type=F32).astype(BF16)
    grad_query, grad_key, grad_value, gcell = attn_bwd(
        qt, kx, kt, vx, grad_heads_t, khot, khott, qhott, qhot, table, kwin, qwin, lse
    )
    grad_table = jnp.einsum(
        "pm,hp->mh", offset_hot, gcell.reshape(heads, CP * CP), precision=highest
    )
    grad_qkv = jnp.concatenate([grad_query, grad_key, grad_value], axis=1)
    mixer_terms = dot(grad_qkv, wt)
    grad_normed_one = lax.psum(mixer_terms.astype(BF16), "mp").astype(F32)
    grad_wt = jnp.einsum("tf,td->fd", grad_qkv, mixer_in, preferred_element_type=F32)
    grad_qv_bias = jnp.stack(
        [jnp.sum(grad_query.astype(F32), axis=0), jnp.sum(grad_value.astype(F32), axis=0)]
    )
    out_half = (
        lax.psum_scatter(back_terms.astype(BF16), "mp", scatter_dimension=1, tiled=True).astype(F32)
        + lax.dynamic_slice_in_dim(b_back, column_start, part_width, 0)
        + lax.dynamic_slice_in_dim(residual, column_start, part_width, 1)
    ).astype(BF16)
    unused_one, norm_one_pull = jax.vjp(layer_norm, block_input, ln1_gain, ln1_shift)
    grad_input_norm, grad_g1, grad_c1 = norm_one_pull(grad_normed_one)
    grad_input = grad_resid + grad_input_norm
    grad_half = lax.dynamic_slice_in_dim(grad_input, column_start, part_width, 1).astype(BF16)

    vectors = [grad_g1, grad_c1, grad_b_out, grad_g2, grad_c2, grad_b_back]
    packed = jnp.concatenate(
        [item.reshape(-1) for item in vectors + [grad_qv_bias, grad_b_in, grad_table]]
    )
    early = lax.psum((grad_w_in.astype(BF16), grad_w_back.astype(BF16)), "dp")
    early, late = lax.optimization_barrier(
        (early, (grad_wt.astype(BF16), grad_w_out.astype(BF16), packed.astype(BF16)))
    )
    late = lax.optimization_barrier(lax.psum(late, "dp"))
    grad_w_in, grad_w_back = (item.astype(F32) for item in early)
    grad_wt, grad_w_out, packed = (item.astype(F32) for item in late)
    grad_w_qkv = jnp.transpose(grad_wt.reshape(3, width, model), (2, 0, 1))
    at = 0
    outs = []
    for item in vectors + [grad_qv_bias, grad_b_in, grad_table]:
        outs.append(packed[at : at + item.size].reshape(item.shape))
        at += item.size
    grad_g1, grad_c1, grad_b_out, grad_g2, grad_c2, grad_b_back, grad_qv_bias, grad_b_in, grad_table = outs
    return (
        out_half,
        grad_half,
        grad_g1,
        grad_c1,
        grad_w_qkv,
        grad_qv_bias,
        grad_table,
        grad_w_out,
        grad_b_out,
        grad_g2,
        grad_c2,
        grad_w_in,
        grad_b_in,
        grad_w_back,
        grad_b_back,
    )


def solution(mesh):
    return jax.shard_map(
        body,
        mesh=mesh,
        in_specs=(
            P("dp", "mp"),
            P("dp"),
            P("dp", None),
            P(),
            P(),
            P(),
            P(None, None, "mp"),
            P(None, "mp"),
            P(None, "mp"),
            P("mp", None),
            P(),
            P(),
            P(),
            P(None, "mp"),
            P("mp"),
            P("mp", None),
            P(),
            P("dp", "mp"),
        ),
        out_specs=(
            P("dp", "mp"),
            P("dp", "mp"),
            P(),
            P(),
            P(None, None, "mp"),
            P(None, "mp"),
            P(None, "mp"),
            P("mp", None),
            P(),
            P(),
            P(),
            P(None, "mp"),
            P("mp"),
            P("mp", None),
            P(),
        ),
        check_vma=False,
    )
```

```python
from functools import partial

import jax
import jax.numpy as jnp
from jax import lax
from jax.experimental import pallas as pl
from jax.experimental.pallas import tpu as pltpu
from jax.sharding import PartitionSpec as P

HEAD_DIM = 32
SIDE = 7
LOCAL_SIDE = 3
CELLS = 49
OFFSETS = 169
CROP_MAX = 8
QB = 128
HALO = 64
SPAN = QB + 2 * HALO
CP = 64
GROUP = 4
SCALE = HEAD_DIM ** (-0.5)
EPS = 1e-05
NEG = -1e30
CHUNK = 256
MESH = pl.DeviceIdType.MESH
F32 = jnp.float32
BF16 = jnp.bfloat16


def layout(counts, patches, row_count):
    live_crop = jnp.arange(CROP_MAX, dtype=jnp.int32)[None, :] < counts[:, None]
    crop_rows = jnp.where(live_crop, patches, 0).reshape(-1)
    crop_ends = jnp.cumsum(crop_rows)
    used_rows = crop_ends[-1]
    row_ids = jnp.arange(row_count, dtype=jnp.int32)
    passed = crop_ends[None, :] <= row_ids[:, None]
    window = jnp.sum(passed.astype(jnp.int32), axis=1)
    starts = jnp.max(jnp.where(passed, crop_ends[None, :], 0), axis=1)
    finish = jnp.min(jnp.where(passed, row_count + used_rows + 1, crop_ends[None, :]), axis=1)
    length = finish - starts
    offset = row_ids - starts
    grid_side = jnp.where(length >= CELLS, SIDE, LOCAL_SIDE).astype(jnp.int32)
    cell_index = offset // grid_side * SIDE + offset % grid_side
    inside = row_ids < used_rows
    cell_ids = jnp.where(inside, cell_index, 0)
    windows = jnp.where(inside, window, crop_rows.shape[0] + row_ids - used_rows)
    return (cell_ids, windows)


def layer_norm(values, gain, shift):
    center = values - jnp.mean(values, axis=-1, keepdims=True)
    spread = jnp.mean(center * center, axis=-1, keepdims=True)
    return center * lax.rsqrt(spread + EPS) * gain + shift


def dot(a, b):
    return jnp.dot(a, b, preferred_element_type=F32)


def dot_nt(a, b):
    return lax.dot_general(a, b, (((1,), (1,)), ((), ())), preferred_element_type=F32)


def stack_heads(rows_t):
    cols = []
    for j in range(GROUP):
        parts = []
        if j > 0:
            parts.append(jnp.zeros((HEAD_DIM * j, QB), BF16))
        parts.append(rows_t[HEAD_DIM * j : HEAD_DIM * (j + 1)])
        if j < GROUP - 1:
            parts.append(jnp.zeros((HEAD_DIM * (GROUP - 1 - j), QB), BF16))
        cols.append(jnp.concatenate(parts, axis=0))
    return jnp.concatenate(cols, axis=1)


def bias_rows(table, g, cells):
    tall = dot(table[2 * CP * GROUP * g : 2 * CP * GROUP * (g + 1), :], cells).astype(BF16)
    return jnp.concatenate([tall[2 * CP * j : 2 * CP * (j + 1)] for j in range(GROUP)], axis=1)


def dot_tn(a, b):
    return lax.dot_general(a, b, (((0,), (0,)), ((), ())), preferred_element_type=F32)


def peer_of():
    return 1 - lax.axis_index("mp")


def greet():
    barrier = pltpu.get_barrier_semaphore()
    pl.semaphore_signal(barrier, inc=1, device_id={"mp": peer_of()}, device_id_type=MESH)
    pl.semaphore_wait(barrier, 1)


def to_peer(src, dst, send_sem, recv_sem):
    return pltpu.make_async_remote_copy(
        src_ref=src,
        dst_ref=dst,
        send_sem=send_sem,
        recv_sem=recv_sem,
        device_id={"mp": peer_of()},
        device_id_type=MESH,
    )


def rows_copy(src, dst, size, sems, i):
    at = pl.ds(pl.multiple_of(i * size, size), size)
    return to_peer(src.at[at], dst.at[at], sems[0].at[i], sems[1].at[i])


def half_lanes(index, half):
    return pl.ds(pl.multiple_of(index * half, 128), half)


def attn_fwd_kernel(
    groups, tok, gain, shift, wt, qb_col, vb_col, vb_row, khot, qhott, table, kwin, qwin,
    a_out, qt, kx, kt, vx, o_out, peer_out, lse, a_pad, vt, o_all, o_peer, send_sem, recv_sem,
):
    step = pl.program_id(0)
    last = tok.shape[0] // QB - 1
    rows_all = tok.shape[0]
    width = qt.shape[0]
    sems = (send_sem, recv_sem)

    @pl.when(step == 0)
    def _():
        greet()
        zero = jnp.zeros((HALO, tok.shape[1]), BF16)
        a_pad[:HALO, :] = zero
        a_pad[HALO + rows_all :, :] = zero

        def norm_rows(i, carry):
            at = pl.multiple_of(i * QB, QB)
            a = layer_norm(tok[pl.ds(at, QB), :].astype(F32), gain[...], shift[...]).astype(BF16)
            a_out[pl.ds(at, QB), :] = a
            a_pad[pl.ds(pl.multiple_of(at + HALO, HALO), QB), :] = a
            return carry

        lax.fori_loop(0, rows_all // QB, norm_rows, 0)
        a_all = a_pad[...]
        wk = wt[width : 2 * width, :]
        wv = wt[2 * width :, :]
        qt[...] = (dot_nt(wt[:width, :], a_out[...]) + qb_col[...]).astype(BF16)
        kx[...] = dot_nt(a_all, wk).astype(BF16)
        kt[...] = dot_nt(wk, a_all).astype(BF16)
        vx[...] = (dot_nt(a_all, wv) + vb_row[...]).astype(BF16)
        vt[...] = (dot_nt(wv, a_all) + vb_col[...]).astype(BF16)

    start = pl.multiple_of(step * QB, QB)
    span = pl.ds(start, SPAN)
    mask = jnp.where(kwin[span, :] == qwin[...], 0.0, NEG)
    hot = khot[span, :]
    cells = qhott[...]
    for g in range(groups):
        lanes = slice(128 * g, 128 * (g + 1))
        right = jnp.concatenate(
            [stack_heads(qt[lanes, pl.ds(start, QB)]), bias_rows(table, g, cells)], axis=0
        )
        scores = dot(jnp.concatenate([kx[span, lanes], hot], axis=1), right)
        outs = []
        for j in range(GROUP):
            h = GROUP * g + j
            s = scores[:, QB * j : QB * (j + 1)] * SCALE + mask
            peak = jnp.max(s, axis=0, keepdims=True)
            e = jnp.exp(s - peak)
            mass = jnp.sum(e, axis=0, keepdims=True)
            outs.append(dot(vt[HEAD_DIM * h : HEAD_DIM * (h + 1), span], e.astype(BF16)) / mass)
            lse[h : h + 1, :] = peak + jnp.log(mass)
        o_all[pl.ds(start, QB), lanes] = jnp.concatenate(outs, axis=0).T.astype(BF16)

    @pl.when(step > 0)
    def _():
        rows_copy(o_all, o_peer, QB, sems, step - 1).start()

    @pl.when(step == last)
    def _():
        o_out[...] = o_all[...]
        rows_copy(o_all, o_peer, QB, sems, last).start()

        def finish(i, carry):
            copy = rows_copy(o_all, o_peer, QB, sems, i)
            copy.wait()
            return carry

        lax.fori_loop(0, last + 1, finish, 0)
        peer_out[...] = o_peer[...]


def whole(a):
    return pl.BlockSpec(a.shape, lambda i: (0,) * len(a.shape))


def same(*shape):
    return pl.BlockSpec(shape, lambda i: (0,) * len(shape))


def cols(n):
    return pl.BlockSpec((n, QB), lambda i: (0, i))


def two_sems(n):
    return [pltpu.SemaphoreType.DMA((n,)), pltpu.SemaphoreType.DMA((n,))]


def attn_fwd(tok, gain, shift, wt, qb_col, vb_col, vb_row, khot, qhott, table, kwin, qwin):
    rows, model = tok.shape
    width = wt.shape[0] // 3
    heads = width // HEAD_DIM
    ext = rows + 2 * HALO
    shape = jax.ShapeDtypeStruct
    return pl.pallas_call(
        partial(attn_fwd_kernel, heads // GROUP),
        grid=(rows // QB,),
        in_specs=[whole(x) for x in (tok, gain, shift, wt, qb_col, vb_col, vb_row, khot)]
        + [cols(CP), whole(table), whole(kwin), cols(1)],
        out_specs=[
            same(rows, model), same(width, rows), same(ext, width), same(width, ext), same(ext, width),
            same(rows, width), same(rows, width), cols(heads),
        ],
        out_shape=[
            shape((rows, model), BF16), shape((width, rows), BF16), shape((ext, width), BF16),
            shape((width, ext), BF16), shape((ext, width), BF16), shape((rows, width), BF16),
            shape((rows, width), BF16), shape((heads, rows), F32),
        ],
        scratch_shapes=[
            pltpu.VMEM((ext, model), BF16), pltpu.VMEM((width, ext), BF16),
            pltpu.VMEM((rows, width), BF16), pltpu.VMEM((rows, width), BF16),
        ] + two_sems(rows // QB),
        compiler_params=pltpu.CompilerParams(collective_id=0, has_side_effects=True),
        name="attn_fwd",
    )(tok, gain, shift, wt, qb_col, vb_col, vb_row, khot, qhott, table, kwin, qwin)


def ffn_kernel(
    tok, o_own, o_peer, w_own, w_peer, bo, gain, shift, w_in, b_in, w_back, bb, cot,
    keep, give, gr, dot_t, g_out, g_in, g_back, vec, vec_in,
    n_s, r_s, h_s, z_s, du_s, gh_s, gh_p, go_s, wide_a, wide_b, send_sem, recv_sem,
):
    rows_all, model = tok.shape
    half = keep.shape[1]
    chunks = rows_all // CHUNK
    sems = (send_sem, recv_sem)
    me = lax.axis_index("mp")
    own = half_lanes(me, half)
    other = half_lanes(1 - me, half)
    greet()
    vec[...] = jnp.zeros_like(vec)
    vec_in[...] = jnp.zeros_like(vec_in)

    def forward(c, carry):
        at = pl.ds(pl.multiple_of(c * CHUNK, CHUNK), CHUNK)
        x1 = tok[at, :].astype(F32) + dot(o_own[at, :], w_own[...]) + dot(o_peer[at, :], w_peer[...])
        x1 = x1 + bo[...]
        center = x1 - jnp.mean(x1, axis=-1, keepdims=True)
        r = lax.rsqrt(jnp.mean(center * center, axis=-1, keepdims=True) + EPS)
        n = center * r
        h = (n * gain[...] + shift[...]).astype(BF16)
        wide_b[...] = x1
        n_s[at, :] = n
        r_s[at, :] = r
        h_s[at, :] = h
        u = dot(h, w_in[...]) + b_in[...]
        cdf = 0.5 * (1.0 + lax.erf(u * (0.5**0.5)))
        slope = cdf + u * (jnp.exp(-0.5 * u * u) * 0.3989422804014327)
        z = (u * cdf).astype(BF16)
        z_s[at, :] = z
        du = (dot_nt(cot[at, :], w_back[...]) * slope).astype(BF16)
        du_s[at, :] = du
        gh_s[at, :] = dot_nt(du, w_in[...]).astype(BF16)
        vec_in[...] += jnp.sum(du.astype(F32), axis=0, keepdims=True)
        wide_a[...] = dot(z, w_back[...])
        rows_copy(gh_s, gh_p, CHUNK, sems, c).start()
        keep[at, :] = wide_a[:, own] + wide_b[:, own] + bb[:, own]
        give[at, :] = wide_a[:, other].astype(BF16)
        return carry

    lax.fori_loop(0, chunks, forward, 0)

    def back_block(i, carry):
        at = pl.ds(pl.multiple_of(i * CHUNK, CHUNK), CHUNK)
        g_back[at, :] = dot_tn(z_s[:, at], cot[...]).astype(BF16)
        return carry

    lax.fori_loop(0, z_s.shape[1] // CHUNK, back_block, 0)

    def in_block(i, carry):
        at = pl.ds(pl.multiple_of(i * CHUNK, CHUNK), CHUNK)
        g_in[at, :] = dot_tn(h_s[:, at], du_s[...]).astype(BF16)
        return carry

    lax.fori_loop(0, model // CHUNK, in_block, 0)

    def backward(c, carry):
        at = pl.ds(pl.multiple_of(c * CHUNK, CHUNK), CHUNK)
        rows_copy(gh_s, gh_p, CHUNK, sems, c).wait()
        gh = gh_s[at, :].astype(F32) + gh_p[at, :].astype(F32)
        n = n_s[at, :]
        e = gh * gain[...]
        gy = cot[at, :].astype(F32)
        mean_e = jnp.mean(e, axis=-1, keepdims=True)
        mean_n = jnp.mean(e * n, axis=-1, keepdims=True)
        gx1 = gy + r_s[at, :] * (e - mean_e - n * mean_n)
        wide_a[...] = gx1
        go = gx1.astype(BF16)
        go_s[at, :] = go
        dot_t[:, at] = dot_nt(w_own[...], go).astype(BF16)
        vec[0:1, :] += jnp.sum(gh * n, axis=0, keepdims=True)
        vec[1:2, :] += jnp.sum(gh, axis=0, keepdims=True)
        vec[2:3, :] += jnp.sum(go.astype(F32), axis=0, keepdims=True)
        vec[3:4, :] += jnp.sum(gy, axis=0, keepdims=True)
        gr[at, :] = wide_a[:, own]
        return carry

    lax.fori_loop(0, chunks, backward, 0)
    g_out[...] = dot_tn(o_own[...], go_s[...]).astype(BF16)


def ffn(tok, o_own, o_peer, w_own, w_peer, bo, gain, shift, w_in, b_in, w_back, bb, cot):
    rows, model = tok.shape
    width = o_own.shape[1]
    hidden = w_in.shape[1]
    half = model // 2
    shape = jax.ShapeDtypeStruct
    vm = pltpu.VMEM
    return pl.pallas_call(
        ffn_kernel,
        in_specs=[pl.BlockSpec(memory_space=pltpu.VMEM)] * 13,
        out_specs=[pl.BlockSpec(memory_space=pltpu.VMEM)] * 9,
        out_shape=[
            shape((rows, half), F32), shape((rows, half), BF16), shape((rows, half), F32),
            shape((width, rows), BF16), shape((width, model), BF16), shape((model, hidden), BF16),
            shape((hidden, model), BF16), shape((8, model), F32), shape((1, hidden), F32),
        ],
        scratch_shapes=[
            vm((rows, model), F32), vm((rows, 1), F32), vm((rows, model), BF16), vm((rows, hidden), BF16),
            vm((rows, hidden), BF16), vm((rows, model), BF16), vm((rows, model), BF16),
            vm((rows, model), BF16), vm((CHUNK, model), F32), vm((CHUNK, model), F32),
        ] + two_sems(rows // CHUNK),
        compiler_params=pltpu.CompilerParams(collective_id=1, has_side_effects=True),
        name="ffn",
    )(tok, o_own, o_peer, w_own, w_peer, bo, gain, shift, w_in, b_in, w_back, bb, cot)


def attn_bwd_kernel(
    groups, keep, give, qt, kx, kt, vx, dot_t, khot, khott, qhott, qhot, table, kwin, qwin, lse,
    out, dq, dk, dv, gcell, dk_acc, dv_acc, got, send_sem, recv_sem,
):
    step = pl.program_id(0)
    rows_all = dk.shape[0]
    swap = to_peer(give, got, send_sem.at[0], recv_sem.at[0])

    @pl.when(step == 0)
    def _():
        greet()
        swap.start()
        dk_acc[...] = jnp.zeros_like(dk_acc)
        dv_acc[...] = jnp.zeros_like(dv_acc)
        gcell[...] = jnp.zeros_like(gcell)

    start = pl.multiple_of(step * QB, QB)
    span = pl.ds(start, SPAN)
    mask = jnp.where(kwin[span, :] == qwin[...], 0.0, NEG)
    hot = khot[span, :]
    hot_t = khott[:, span]
    cells = qhott[...]
    cells_r = qhot[...]
    for g in range(groups):
        lanes = slice(128 * g, 128 * (g + 1))
        q_stack = stack_heads(qt[lanes, :])
        do_stack = stack_heads(dot_t[lanes, :])
        right = jnp.concatenate([q_stack, bias_rows(table, g, cells)], axis=0)
        scores = dot(jnp.concatenate([kx[span, lanes], hot], axis=1), right)
        dprob = dot(vx[span, lanes], do_stack)
        ps, dss, dqs = [], [], []
        for j in range(GROUP):
            h = GROUP * g + j
            cut = slice(QB * j, QB * (j + 1))
            p = jnp.exp(scores[:, cut] * SCALE + mask - lse[h : h + 1, :])
            t = p * dprob[:, cut]
            inner = jnp.sum(t, axis=0, keepdims=True)
            ds = (t - p * inner).astype(BF16)
            ps.append(p.astype(BF16))
            dss.append(ds)
            both = dot(jnp.concatenate([kt[HEAD_DIM * h : HEAD_DIM * (h + 1), span], hot_t], axis=0), ds)
            dqs.append(both[:HEAD_DIM])
            gcell[CP * h : CP * (h + 1), :] += dot(both[HEAD_DIM:].astype(BF16), cells_r)
        dq[:, lanes] = (jnp.concatenate(dqs, axis=0) * SCALE).T.astype(BF16)
        dk_acc[span, lanes] += dot_nt(jnp.concatenate(dss, axis=1), q_stack)
        dv_acc[span, lanes] += dot_nt(jnp.concatenate(ps, axis=1), do_stack)

    @pl.when(step == rows_all // QB - 1)
    def _():
        inner_rows = pl.ds(HALO, rows_all)
        dk[...] = (dk_acc[inner_rows, :] * SCALE).astype(BF16)
        dv[...] = dv_acc[inner_rows, :].astype(BF16)
        swap.wait()
        out[...] = (keep[...] + got[...].astype(F32)).astype(BF16)


def attn_bwd(keep, give, qt, kx, kt, vx, dot_t, khot, khott, qhott, qhot, table, kwin, qwin, lse):
    width, rows = qt.shape
    heads = width // HEAD_DIM
    ext = rows + 2 * HALO
    half = keep.shape[1]
    shape = jax.ShapeDtypeStruct
    rblk = lambda n: pl.BlockSpec((QB, n), lambda i: (i, 0))
    return pl.pallas_call(
        partial(attn_bwd_kernel, heads // GROUP),
        grid=(rows // QB,),
        in_specs=[
            whole(keep), pl.BlockSpec(memory_space=pltpu.VMEM),
            cols(width), whole(kx), whole(kt), whole(vx), cols(width), whole(khot), whole(khott),
            cols(CP), rblk(CP), whole(table), whole(kwin), cols(1), cols(heads),
        ],
        out_specs=[
            same(rows, half), rblk(width), same(rows, width), same(rows, width), same(CP * heads, CP),
        ],
        out_shape=[
            shape((rows, half), BF16), shape((rows, width), BF16), shape((rows, width), BF16),
            shape((rows, width), BF16), shape((CP * heads, CP), F32),
        ],
        scratch_shapes=[
            pltpu.VMEM((ext, width), F32), pltpu.VMEM((ext, width), F32), pltpu.VMEM((rows, half), BF16),
        ] + two_sems(1),
        compiler_params=pltpu.CompilerParams(collective_id=2, has_side_effects=True),
        name="attn_bwd",
    )(keep, give, qt, kx, kt, vx, dot_t, khot, khott, qhott, qhot, table, kwin, qwin, lse)


def close_kernel(
    tok, a, dq, dk, dv, wt, gain, gr, out, g_wt, vec, vec_qv,
    ga_s, give, got, stat, stat_p, r_s, wide, vec_s, vec_p, send_sem, recv_sem,
):
    rows_all, model = tok.shape
    width = dq.shape[1]
    half = out.shape[1]
    chunks = rows_all // CHUNK
    me = lax.axis_index("mp")
    own = half_lanes(me, half)
    other = half_lanes(1 - me, half)
    greet()
    vec_s[...] = jnp.zeros_like(vec_s)
    main = lambda c: rows_copy(give, got, CHUNK, (send_sem.at[0], recv_sem.at[0]), c)
    side = lambda c: rows_copy(stat, stat_p, CHUNK, (send_sem.at[1], recv_sem.at[1]), c)
    lane = lax.broadcasted_iota(jnp.int32, (CHUNK, 128), 1)

    def norms(at):
        x = tok[at, :].astype(F32)
        center = x - jnp.mean(x, axis=-1, keepdims=True)
        r = lax.rsqrt(jnp.mean(center * center, axis=-1, keepdims=True) + EPS)
        return center * r, r

    def forward(c, carry):
        at = pl.ds(pl.multiple_of(c * CHUNK, CHUNK), CHUNK)
        ga = dot(dq[at, :], wt[:width, :]) + dot(dk[at, :], wt[width : 2 * width, :])
        ga = ga + dot(dv[at, :], wt[2 * width :, :])
        wide[...] = ga
        give[at, :] = wide[:, other].astype(BF16)
        ga_s[at, :] = wide[:, own]
        n, r = norms(at)
        e = ga * gain[...]
        first = jnp.mean(e, axis=-1, keepdims=True)
        second = jnp.mean(e * n, axis=-1, keepdims=True)
        stat[at, :] = jnp.where(lane == 0, first, jnp.where(lane == 1, second, 0.0))
        vec_s[0:1, :] += jnp.sum(ga * n, axis=0, keepdims=True)
        vec_s[1:2, :] += jnp.sum(ga, axis=0, keepdims=True)
        main(c).start()
        side(c).start()
        return carry

    lax.fori_loop(0, chunks, forward, 0)
    vectors = to_peer(vec_s, vec_p, send_sem.at[2, 0], recv_sem.at[2, 0])
    for k, item in enumerate((dq, dk, dv)):
        g_wt[width * k : width * (k + 1), :] = dot_tn(item[...], a[...]).astype(BF16)
    vectors.start()
    vec_qv[0:1, :] = jnp.sum(dq[...].astype(F32), axis=0, keepdims=True)
    vec_qv[1:2, :] = jnp.sum(dv[...].astype(F32), axis=0, keepdims=True)

    def backward(c, carry):
        at = pl.ds(pl.multiple_of(c * CHUNK, CHUNK), CHUNK)
        main(c).wait()
        side(c).wait()
        sums = stat[at, :] + stat_p[at, :]
        n, r = norms(at)
        wide[...] = n
        e = (ga_s[at, :] + got[at, :].astype(F32)) * gain[:, own]
        gx = gr[at, :] + r * (e - sums[:, 0:1] - wide[:, own] * sums[:, 1:2])
        out[at, :] = gx.astype(BF16)
        return carry

    lax.fori_loop(0, chunks, backward, 0)
    vectors.wait()
    vec[...] = vec_s[...] + vec_p[...]


def close(tok, a, dq, dk, dv, wt, gain, gr):
    rows, model = tok.shape
    width = dq.shape[1]
    half = gr.shape[1]
    chunks = rows // CHUNK
    shape = jax.ShapeDtypeStruct
    vm = pltpu.VMEM
    sems = pltpu.SemaphoreType.DMA((3, chunks))
    return pl.pallas_call(
        close_kernel,
        in_specs=[pl.BlockSpec(memory_space=pltpu.VMEM)] * 8,
        out_specs=[pl.BlockSpec(memory_space=pltpu.VMEM)] * 4,
        out_shape=[
            shape((rows, half), BF16), shape((3 * width, model), BF16), shape((8, model), F32),
            shape((8, width), F32),
        ],
        scratch_shapes=[
            vm((rows, half), F32), vm((rows, half), BF16), vm((rows, half), BF16), vm((rows, 128), F32),
            vm((rows, 128), F32), vm((rows, 1), F32), vm((CHUNK, model), F32), vm((8, model), F32),
            vm((8, model), F32), sems, sems,
        ],
        compiler_params=pltpu.CompilerParams(collective_id=3, has_side_effects=True),
        name="close",
    )(tok, a, dq, dk, dv, wt, gain, gr)


def window_data(crop_counts, crop_patches, rel_index, rel_table, rows):
    highest = lax.Precision.HIGHEST
    heads = rel_table.shape[1]
    cells, wins = layout(crop_counts, crop_patches, rows)
    kcells = jnp.pad(cells, (HALO, HALO))
    kwin = jnp.pad(wins, (HALO, HALO), constant_values=-1)[:, None]
    span_cells = jnp.arange(CP, dtype=jnp.int32)
    wide_cells = jnp.arange(2 * CP, dtype=jnp.int32) % CP
    khot = (kcells[:, None] == wide_cells[None, :]).astype(BF16)
    khott = (span_cells[:, None] == kcells[None, :]).astype(BF16)
    qhott = (span_cells[:, None] == cells[None, :]).astype(BF16)
    qhot = (cells[:, None] == span_cells[None, :]).astype(BF16)
    rel_t = jnp.pad(rel_index.T, ((0, CP - CELLS), (0, CP - CELLS)), constant_values=-1).reshape(-1)
    offset_hot = (rel_t[:, None] == jnp.arange(OFFSETS, dtype=jnp.int32)[None, :]).astype(F32)
    bias = jnp.einsum("pm,mh->hp", offset_hot, rel_table, precision=highest) / SCALE
    high = bias.astype(BF16)
    rest = (bias - high.astype(F32)).astype(BF16)
    table = jnp.stack([high.reshape(heads, CP, CP), rest.reshape(heads, CP, CP)], axis=1)
    return (khot, khott, qhott, qhot, table.reshape(heads * 2 * CP, CP), kwin, wins[None, :], offset_hot)


def body(
    tokens,
    crop_counts,
    crop_patches,
    rel_index,
    ln1_gain,
    ln1_shift,
    w_qkv,
    qv_bias,
    rel_table,
    w_out,
    b_out,
    ln2_gain,
    ln2_shift,
    w_in,
    b_in,
    w_back,
    b_back,
    cotangent,
):
    highest = lax.Precision.HIGHEST
    rows, part_width = tokens.shape
    model = ln1_gain.shape[0]
    width = w_qkv.shape[2]
    heads = width // HEAD_DIM
    khot, khott, qhott, qhot, table, kwin, qwin, offset_hot = window_data(
        crop_counts, crop_patches, rel_index, rel_table, rows
    )
    me = lax.axis_index("mp")
    whole_in = lax.all_gather(tokens, "mp", axis=1, tiled=True)
    w_out_all = lax.all_gather(w_out, "mp", axis=0, tiled=True)
    w_peer = lax.dynamic_slice_in_dim(w_out_all, (1 - me) * width, width, 0)
    whole_cot = lax.all_gather(cotangent, "mp", axis=1, tiled=True)
    wt = jnp.transpose(w_qkv, (1, 2, 0)).reshape(3 * width, model)
    mixer_in, qt, kx, kt, vx, heads_out, heads_peer, lse = attn_fwd(
        whole_in, ln1_gain[None, :], ln1_shift[None, :], wt, qv_bias[0][:, None], qv_bias[1][:, None],
        qv_bias[1][None, :], khot, qhott, table, kwin, qwin,
    )
    keep, give, gr, dot_t, grad_w_out, grad_w_in, grad_w_back, vec2, grad_b_in = ffn(
        whole_in, heads_out, heads_peer, w_out, w_peer, b_out[None, :], ln2_gain[None, :], ln2_shift[None, :],
        w_in, b_in[None, :], w_back, b_back[None, :], whole_cot,
    )
    early = lax.psum((grad_w_in, grad_w_back), "dp")
    out_half, grad_query, grad_key, grad_value, gcell = attn_bwd(
        keep, give, qt, kx, kt, vx, dot_t, khot, khott, qhott, qhot, table, kwin, qwin, lse
    )
    grad_table = jnp.einsum(
        "pm,hp->mh", offset_hot, gcell.reshape(heads, CP * CP), precision=highest
    )
    grad_half, grad_wt, vec1, vec_qv = close(
        whole_in, mixer_in, grad_query, grad_key, grad_value, wt, ln1_gain[None, :], gr
    )
    small = [vec1[0], vec1[1], vec2[2], vec2[0], vec2[1], vec2[3], vec_qv[:2], grad_b_in[0], grad_table]
    sizes = [item.shape for item in small]
    packed = jnp.concatenate([item.reshape(-1) for item in small])
    pad_rows = -(-packed.size // (16 * model)) * 16
    packed = jnp.pad(packed, (0, pad_rows * model - packed.size)).reshape(pad_rows, model).astype(BF16)
    early, late = lax.optimization_barrier((early, (grad_wt, grad_w_out, packed)))
    late = lax.optimization_barrier(lax.psum(late, "dp"))
    grad_w_in, grad_w_back = (item.astype(F32) for item in early)
    grad_wt, grad_w_out, packed = (item.astype(F32) for item in late)
    grad_w_qkv = jnp.transpose(grad_wt.reshape(3, width, model), (2, 0, 1))
    packed = packed.reshape(-1)
    at = 0
    outs = []
    for shape in sizes:
        size = 1
        for extent in shape:
            size *= extent
        outs.append(packed[at : at + size].reshape(shape))
        at += size
    grad_g1, grad_c1, grad_b_out, grad_g2, grad_c2, grad_b_back, grad_qv_bias, grad_b_in, grad_table = outs
    return (
        out_half,
        grad_half,
        grad_g1,
        grad_c1,
        grad_w_qkv,
        grad_qv_bias,
        grad_table,
        grad_w_out,
        grad_b_out,
        grad_g2,
        grad_c2,
        grad_w_in,
        grad_b_in,
        grad_w_back,
        grad_b_back,
    )


def solution(mesh):
    return jax.shard_map(
        body,
        mesh=mesh,
        in_specs=(
            P("dp", "mp"),
            P("dp"),
            P("dp", None),
            P(),
            P(),
            P(),
            P(None, None, "mp"),
            P(None, "mp"),
            P(None, "mp"),
            P("mp", None),
            P(),
            P(),
            P(),
            P(None, "mp"),
            P("mp"),
            P("mp", None),
            P(),
            P("dp", "mp"),
        ),
        out_specs=(
            P("dp", "mp"),
            P("dp", "mp"),
            P(),
            P(),
            P(None, None, "mp"),
            P(None, "mp"),
            P(None, "mp"),
            P("mp", None),
            P(),
            P(),
            P(),
            P(None, "mp"),
            P("mp"),
            P("mp", None),
            P(),
        ),
        check_vma=False,
    )
```

```python
from functools import partial

import jax
import jax.numpy as jnp
from jax import lax
from jax.experimental import pallas as pl
from jax.experimental.pallas import tpu as pltpu
from jax.sharding import PartitionSpec as P

HEAD_DIM = 32
SIDE = 7
LOCAL_SIDE = 3
CELLS = 49
OFFSETS = 169
CROP_MAX = 8
QB = 128
HALO = 64
SPAN = QB + 2 * HALO
CP = 64
GROUP = 4
SCALE = HEAD_DIM ** (-0.5)
EPS = 1e-05
NEG = -1e30
CHUNK = 256
SMALL = 16
MESH = pl.DeviceIdType.MESH
F32 = jnp.float32
BF16 = jnp.bfloat16


def layout(counts, patches, row_count):
    live_crop = jnp.arange(CROP_MAX, dtype=jnp.int32)[None, :] < counts[:, None]
    crop_rows = jnp.where(live_crop, patches, 0).reshape(-1)
    crop_ends = jnp.cumsum(crop_rows)
    used_rows = crop_ends[-1]
    row_ids = jnp.arange(row_count, dtype=jnp.int32)
    passed = crop_ends[None, :] <= row_ids[:, None]
    window = jnp.sum(passed.astype(jnp.int32), axis=1)
    starts = jnp.max(jnp.where(passed, crop_ends[None, :], 0), axis=1)
    finish = jnp.min(jnp.where(passed, row_count + used_rows + 1, crop_ends[None, :]), axis=1)
    length = finish - starts
    offset = row_ids - starts
    grid_side = jnp.where(length >= CELLS, SIDE, LOCAL_SIDE).astype(jnp.int32)
    cell_index = offset // grid_side * SIDE + offset % grid_side
    inside = row_ids < used_rows
    cell_ids = jnp.where(inside, cell_index, 0)
    windows = jnp.where(inside, window, crop_rows.shape[0] + row_ids - used_rows)
    return (cell_ids, windows)


def layer_norm(values, gain, shift):
    center = values - jnp.mean(values, axis=-1, keepdims=True)
    spread = jnp.mean(center * center, axis=-1, keepdims=True)
    return center * lax.rsqrt(spread + EPS) * gain + shift


def dot(a, b):
    return jnp.dot(a, b, preferred_element_type=F32)


def dot_nt(a, b):
    return lax.dot_general(a, b, (((1,), (1,)), ((), ())), preferred_element_type=F32)


def stack_heads(rows_t):
    cols = []
    for j in range(GROUP):
        parts = []
        if j > 0:
            parts.append(jnp.zeros((HEAD_DIM * j, QB), BF16))
        parts.append(rows_t[HEAD_DIM * j : HEAD_DIM * (j + 1)])
        if j < GROUP - 1:
            parts.append(jnp.zeros((HEAD_DIM * (GROUP - 1 - j), QB), BF16))
        cols.append(jnp.concatenate(parts, axis=0))
    return jnp.concatenate(cols, axis=1)


def bias_rows(table, g, cells):
    tall = dot(table[2 * CP * GROUP * g : 2 * CP * GROUP * (g + 1), :], cells).astype(BF16)
    return jnp.concatenate([tall[2 * CP * j : 2 * CP * (j + 1)] for j in range(GROUP)], axis=1)


def dot_tn(a, b):
    return lax.dot_general(a, b, (((0,), (0,)), ((), ())), preferred_element_type=F32)


def peer_of():
    return 1 - lax.axis_index("mp")


def greet():
    barrier = pltpu.get_barrier_semaphore()
    pl.semaphore_signal(barrier, inc=1, device_id={"mp": peer_of()}, device_id_type=MESH)
    pl.semaphore_wait(barrier, 1)


def to_peer(src, dst, send_sem, recv_sem):
    return pltpu.make_async_remote_copy(
        src_ref=src,
        dst_ref=dst,
        send_sem=send_sem,
        recv_sem=recv_sem,
        device_id={"mp": peer_of()},
        device_id_type=MESH,
    )


def rows_copy(src, dst, size, sems, i):
    at = pl.ds(pl.multiple_of(i * size, size), size)
    return to_peer(src.at[at], dst.at[at], sems[0].at[i], sems[1].at[i])


def half_lanes(index, half):
    return pl.ds(pl.multiple_of(index * half, 128), half)


def attn_fwd_kernel(
    groups, w_own, tok, gain, shift, wt, qb_col, vb_col, vb_row, khot, qhott, table, kwin, qwin,
    a_out, qt, kx, kt, vx, o_out, peer_out, w_out, lse, a_pad, vt, o_all, o_peer, w_got, send_sem, recv_sem,
):
    step = pl.program_id(0)
    last = tok.shape[0] // QB - 1
    rows_all = tok.shape[0]
    width = qt.shape[0]
    sems = (send_sem, recv_sem)
    weight = to_peer(w_own, w_got, send_sem.at[last + 1], recv_sem.at[last + 1])

    @pl.when(step == 0)
    def _():
        greet()
        weight.start()
        zero = jnp.zeros((HALO, tok.shape[1]), BF16)
        a_pad[:HALO, :] = zero
        a_pad[HALO + rows_all :, :] = zero

        def norm_rows(i, carry):
            at = pl.multiple_of(i * QB, QB)
            a = layer_norm(tok[pl.ds(at, QB), :].astype(F32), gain[...], shift[...]).astype(BF16)
            a_out[pl.ds(at, QB), :] = a
            a_pad[pl.ds(pl.multiple_of(at + HALO, HALO), QB), :] = a
            return carry

        lax.fori_loop(0, rows_all // QB, norm_rows, 0)
        a_all = a_pad[...]
        wk = wt[width : 2 * width, :]
        wv = wt[2 * width :, :]
        qt[...] = (dot_nt(wt[:width, :], a_out[...]) + qb_col[...]).astype(BF16)
        kx[...] = dot_nt(a_all, wk).astype(BF16)
        kt[...] = dot_nt(wk, a_all).astype(BF16)
        vx[...] = (dot_nt(a_all, wv) + vb_row[...]).astype(BF16)
        vt[...] = (dot_nt(wv, a_all) + vb_col[...]).astype(BF16)

    start = pl.multiple_of(step * QB, QB)
    span = pl.ds(start, SPAN)
    mask = jnp.where(kwin[span, :] == qwin[...], 0.0, NEG)
    hot = khot[span, :]
    cells = qhott[...]
    for g in range(groups):
        lanes = slice(128 * g, 128 * (g + 1))
        right = jnp.concatenate(
            [stack_heads(qt[lanes, pl.ds(start, QB)]), bias_rows(table, g, cells)], axis=0
        )
        scores = dot(jnp.concatenate([kx[span, lanes], hot], axis=1), right)
        outs = []
        for j in range(GROUP):
            h = GROUP * g + j
            s = scores[:, QB * j : QB * (j + 1)] * SCALE + mask
            peak = jnp.max(s, axis=0, keepdims=True)
            e = jnp.exp(s - peak)
            mass = jnp.sum(e, axis=0, keepdims=True)
            outs.append(dot(vt[HEAD_DIM * h : HEAD_DIM * (h + 1), span], e.astype(BF16)) / mass)
            lse[h : h + 1, :] = peak + jnp.log(mass)
        o_all[pl.ds(start, QB), lanes] = jnp.concatenate(outs, axis=0).T.astype(BF16)

    @pl.when(step > 0)
    def _():
        rows_copy(o_all, o_peer, QB, sems, step - 1).start()

    @pl.when(step == last)
    def _():
        o_out[...] = o_all[...]
        rows_copy(o_all, o_peer, QB, sems, last).start()

        def finish(i, carry):
            copy = rows_copy(o_all, o_peer, QB, sems, i)
            copy.wait()
            return carry

        lax.fori_loop(0, last + 1, finish, 0)
        weight.wait()
        w_out[...] = w_got[...]
        peer_out[...] = o_peer[...]


def whole(a):
    return pl.BlockSpec(a.shape, lambda i: (0,) * len(a.shape))


def same(*shape):
    return pl.BlockSpec(shape, lambda i: (0,) * len(shape))


def cols(n):
    return pl.BlockSpec((n, QB), lambda i: (0, i))


def two_sems(n):
    return [pltpu.SemaphoreType.DMA((n,)), pltpu.SemaphoreType.DMA((n,))]


def attn_fwd(w_own, tok, gain, shift, wt, qb_col, vb_col, vb_row, khot, qhott, table, kwin, qwin):
    rows, model = tok.shape
    width = wt.shape[0] // 3
    heads = width // HEAD_DIM
    ext = rows + 2 * HALO
    shape = jax.ShapeDtypeStruct
    return pl.pallas_call(
        partial(attn_fwd_kernel, heads // GROUP),
        grid=(rows // QB,),
        in_specs=[pl.BlockSpec(memory_space=pltpu.VMEM)]
        + [whole(x) for x in (tok, gain, shift, wt, qb_col, vb_col, vb_row, khot)]
        + [cols(CP), whole(table), whole(kwin), cols(1)],
        out_specs=[
            same(rows, model), same(width, rows), same(ext, width), same(width, ext), same(ext, width),
            same(rows, width), same(rows, width), same(width, model), cols(heads),
        ],
        out_shape=[
            shape((rows, model), BF16), shape((width, rows), BF16), shape((ext, width), BF16),
            shape((width, ext), BF16), shape((ext, width), BF16), shape((rows, width), BF16),
            shape((rows, width), BF16), shape((width, model), BF16), shape((heads, rows), F32),
        ],
        scratch_shapes=[
            pltpu.VMEM((ext, model), BF16), pltpu.VMEM((width, ext), BF16),
            pltpu.VMEM((rows, width), BF16), pltpu.VMEM((rows, width), BF16),
            pltpu.VMEM((width, model), BF16),
        ] + two_sems(rows // QB + 1),
        compiler_params=pltpu.CompilerParams(collective_id=0, has_side_effects=True),
        name="attn_fwd",
    )(w_own, tok, gain, shift, wt, qb_col, vb_col, vb_row, khot, qhott, table, kwin, qwin)


def ffn_kernel(
    tok, o_own, o_peer, w_own, w_peer, bo, gain, shift, w_in, b_in, w_back, bb, cot,
    keep, give, gr, dot_t, g_out, g_in, g_back, vec, vec_in,
    n_s, r_s, h_s, z_s, du_s, gh_s, gh_p, go_s, wide_a, wide_b, send_sem, recv_sem,
):
    rows_all, model = tok.shape
    half = keep.shape[1]
    chunks = rows_all // CHUNK
    sems = (send_sem, recv_sem)
    me = lax.axis_index("mp")
    own = half_lanes(me, half)
    other = half_lanes(1 - me, half)
    greet()
    vec[...] = jnp.zeros_like(vec)
    vec_in[...] = jnp.zeros_like(vec_in)

    def forward(c, carry):
        at = pl.ds(pl.multiple_of(c * CHUNK, CHUNK), CHUNK)
        x1 = tok[at, :].astype(F32) + dot(o_own[at, :], w_own[...]) + dot(o_peer[at, :], w_peer[...])
        x1 = x1 + bo[...]
        center = x1 - jnp.mean(x1, axis=-1, keepdims=True)
        r = lax.rsqrt(jnp.mean(center * center, axis=-1, keepdims=True) + EPS)
        n = center * r
        h = (n * gain[...] + shift[...]).astype(BF16)
        wide_b[...] = x1
        n_s[at, :] = n
        r_s[at, :] = r
        h_s[at, :] = h
        u = dot(h, w_in[...]) + b_in[...]
        cdf = 0.5 * (1.0 + lax.erf(u * (0.5**0.5)))
        slope = cdf + u * (jnp.exp(-0.5 * u * u) * 0.3989422804014327)
        z = (u * cdf).astype(BF16)
        z_s[at, :] = z
        du = (dot_nt(cot[at, :], w_back[...]) * slope).astype(BF16)
        du_s[at, :] = du
        gh_s[at, :] = dot_nt(du, w_in[...]).astype(BF16)
        vec_in[...] += jnp.sum(du.astype(F32), axis=0, keepdims=True)
        wide_a[...] = dot(z, w_back[...])
        rows_copy(gh_s, gh_p, CHUNK, sems, c).start()
        keep[at, :] = wide_a[:, own] + wide_b[:, own] + bb[:, own]
        give[at, :] = wide_a[:, other].astype(BF16)
        return carry

    lax.fori_loop(0, chunks, forward, 0)

    def back_block(i, carry):
        at = pl.ds(pl.multiple_of(i * CHUNK, CHUNK), CHUNK)
        g_back[at, :] = dot_tn(z_s[:, at], cot[...]).astype(BF16)
        return carry

    lax.fori_loop(0, z_s.shape[1] // CHUNK, back_block, 0)

    def in_block(i, carry):
        at = pl.ds(pl.multiple_of(i * CHUNK, CHUNK), CHUNK)
        g_in[at, :] = dot_tn(h_s[:, at], du_s[...]).astype(BF16)
        return carry

    lax.fori_loop(0, model // CHUNK, in_block, 0)

    def backward(c, carry):
        at = pl.ds(pl.multiple_of(c * CHUNK, CHUNK), CHUNK)
        rows_copy(gh_s, gh_p, CHUNK, sems, c).wait()
        gh = gh_s[at, :].astype(F32) + gh_p[at, :].astype(F32)
        n = n_s[at, :]
        e = gh * gain[...]
        gy = cot[at, :].astype(F32)
        mean_e = jnp.mean(e, axis=-1, keepdims=True)
        mean_n = jnp.mean(e * n, axis=-1, keepdims=True)
        gx1 = gy + r_s[at, :] * (e - mean_e - n * mean_n)
        wide_a[...] = gx1
        go = gx1.astype(BF16)
        go_s[at, :] = go
        dot_t[:, at] = dot_nt(w_own[...], go).astype(BF16)
        vec[0:1, :] += jnp.sum(gh * n, axis=0, keepdims=True)
        vec[1:2, :] += jnp.sum(gh, axis=0, keepdims=True)
        vec[2:3, :] += jnp.sum(go.astype(F32), axis=0, keepdims=True)
        vec[3:4, :] += jnp.sum(gy, axis=0, keepdims=True)
        gr[at, :] = wide_a[:, own]
        return carry

    lax.fori_loop(0, chunks, backward, 0)
    g_out[...] = dot_tn(o_own[...], go_s[...]).astype(BF16)


def ffn(tok, o_own, o_peer, w_own, w_peer, bo, gain, shift, w_in, b_in, w_back, bb, cot):
    rows, model = tok.shape
    width = o_own.shape[1]
    hidden = w_in.shape[1]
    half = model // 2
    shape = jax.ShapeDtypeStruct
    vm = pltpu.VMEM
    return pl.pallas_call(
        ffn_kernel,
        in_specs=[pl.BlockSpec(memory_space=pltpu.VMEM)] * 13,
        out_specs=[pl.BlockSpec(memory_space=pltpu.VMEM)] * 9,
        out_shape=[
            shape((rows, half), F32), shape((rows, half), BF16), shape((rows, half), F32),
            shape((width, rows), BF16), shape((width, model), BF16), shape((model, hidden), BF16),
            shape((hidden, model), BF16), shape((8, model), F32), shape((1, hidden), F32),
        ],
        scratch_shapes=[
            vm((rows, model), F32), vm((rows, 1), F32), vm((rows, model), BF16), vm((rows, hidden), BF16),
            vm((rows, hidden), BF16), vm((rows, model), BF16), vm((rows, model), BF16),
            vm((rows, model), BF16), vm((CHUNK, model), F32), vm((CHUNK, model), F32),
        ] + two_sems(rows // CHUNK),
        compiler_params=pltpu.CompilerParams(collective_id=1, has_side_effects=True),
        name="ffn",
    )(tok, o_own, o_peer, w_own, w_peer, bo, gain, shift, w_in, b_in, w_back, bb, cot)


def attn_bwd_kernel(
    groups, keep, give, qt, kx, kt, vx, dot_t, khot, khott, qhott, qhot, table, kwin, qwin, lse,
    out, dq, dk, dv, gcell, dk_acc, dv_acc, got, send_sem, recv_sem,
):
    step = pl.program_id(0)
    rows_all = dk.shape[0]
    swap = to_peer(give, got, send_sem.at[0], recv_sem.at[0])

    @pl.when(step == 0)
    def _():
        greet()
        swap.start()
        dk_acc[...] = jnp.zeros_like(dk_acc)
        dv_acc[...] = jnp.zeros_like(dv_acc)
        gcell[...] = jnp.zeros_like(gcell)

    start = pl.multiple_of(step * QB, QB)
    span = pl.ds(start, SPAN)
    mask = jnp.where(kwin[span, :] == qwin[...], 0.0, NEG)
    hot = khot[span, :]
    hot_t = khott[:, span]
    cells = qhott[...]
    cells_r = qhot[...]
    for g in range(groups):
        lanes = slice(128 * g, 128 * (g + 1))
        q_stack = stack_heads(qt[lanes, :])
        do_stack = stack_heads(dot_t[lanes, :])
        right = jnp.concatenate([q_stack, bias_rows(table, g, cells)], axis=0)
        scores = dot(jnp.concatenate([kx[span, lanes], hot], axis=1), right)
        dprob = dot(vx[span, lanes], do_stack)
        ps, dss, dqs = [], [], []
        for j in range(GROUP):
            h = GROUP * g + j
            cut = slice(QB * j, QB * (j + 1))
            p = jnp.exp(scores[:, cut] * SCALE + mask - lse[h : h + 1, :])
            t = p * dprob[:, cut]
            inner = jnp.sum(t, axis=0, keepdims=True)
            ds = (t - p * inner).astype(BF16)
            ps.append(p.astype(BF16))
            dss.append(ds)
            both = dot(jnp.concatenate([kt[HEAD_DIM * h : HEAD_DIM * (h + 1), span], hot_t], axis=0), ds)
            dqs.append(both[:HEAD_DIM])
            gcell[CP * h : CP * (h + 1), :] += dot(both[HEAD_DIM:].astype(BF16), cells_r)
        dq[:, lanes] = (jnp.concatenate(dqs, axis=0) * SCALE).T.astype(BF16)
        dk_acc[span, lanes] += dot_nt(jnp.concatenate(dss, axis=1), q_stack)
        dv_acc[span, lanes] += dot_nt(jnp.concatenate(ps, axis=1), do_stack)

    @pl.when(step == rows_all // QB - 1)
    def _():
        inner_rows = pl.ds(HALO, rows_all)
        dk[...] = (dk_acc[inner_rows, :] * SCALE).astype(BF16)
        dv[...] = dv_acc[inner_rows, :].astype(BF16)
        swap.wait()
        out[...] = (keep[...] + got[...].astype(F32)).astype(BF16)


def attn_bwd(keep, give, qt, kx, kt, vx, dot_t, khot, khott, qhott, qhot, table, kwin, qwin, lse):
    width, rows = qt.shape
    heads = width // HEAD_DIM
    ext = rows + 2 * HALO
    half = keep.shape[1]
    shape = jax.ShapeDtypeStruct
    rblk = lambda n: pl.BlockSpec((QB, n), lambda i: (i, 0))
    return pl.pallas_call(
        partial(attn_bwd_kernel, heads // GROUP),
        grid=(rows // QB,),
        in_specs=[
            whole(keep), pl.BlockSpec(memory_space=pltpu.VMEM),
            cols(width), whole(kx), whole(kt), whole(vx), cols(width), whole(khot), whole(khott),
            cols(CP), rblk(CP), whole(table), whole(kwin), cols(1), cols(heads),
        ],
        out_specs=[
            same(rows, half), rblk(width), same(rows, width), same(rows, width), same(CP * heads, CP),
        ],
        out_shape=[
            shape((rows, half), BF16), shape((rows, width), BF16), shape((rows, width), BF16),
            shape((rows, width), BF16), shape((CP * heads, CP), F32),
        ],
        scratch_shapes=[
            pltpu.VMEM((ext, width), F32), pltpu.VMEM((ext, width), F32), pltpu.VMEM((rows, half), BF16),
        ] + two_sems(1),
        compiler_params=pltpu.CompilerParams(collective_id=2, has_side_effects=True),
        name="attn_bwd",
    )(keep, give, qt, kx, kt, vx, dot_t, khot, khott, qhott, qhot, table, kwin, qwin, lse)


def close_kernel(
    tok, a, dq, dk, dv, wt, gain, gr, vec2, vec_in, table, out, late,
    ga_s, give, got, stat, stat_p, wide, vec_s, vec_p, send_sem, recv_sem,
):
    rows_all, model = tok.shape
    width = dq.shape[1]
    half = out.shape[1]
    chunks = rows_all // CHUNK
    me = lax.axis_index("mp")
    own = half_lanes(me, half)
    other = half_lanes(1 - me, half)
    greet()
    vec_s[...] = jnp.zeros_like(vec_s)
    main = lambda c: rows_copy(give, got, CHUNK, (send_sem.at[0], recv_sem.at[0]), c)
    side = lambda c: rows_copy(stat, stat_p, CHUNK, (send_sem.at[1], recv_sem.at[1]), c)
    lane = lax.broadcasted_iota(jnp.int32, (CHUNK, 128), 1)

    def norms(at):
        x = tok[at, :].astype(F32)
        center = x - jnp.mean(x, axis=-1, keepdims=True)
        r = lax.rsqrt(jnp.mean(center * center, axis=-1, keepdims=True) + EPS)
        return center * r, r

    def forward(c, carry):
        at = pl.ds(pl.multiple_of(c * CHUNK, CHUNK), CHUNK)
        ga = dot(dq[at, :], wt[:width, :]) + dot(dk[at, :], wt[width : 2 * width, :])
        ga = ga + dot(dv[at, :], wt[2 * width :, :])
        wide[...] = ga
        give[at, :] = wide[:, other].astype(BF16)
        ga_s[at, :] = wide[:, own]
        n, r = norms(at)
        e = ga * gain[...]
        first = jnp.mean(e, axis=-1, keepdims=True)
        second = jnp.mean(e * n, axis=-1, keepdims=True)
        stat[at, :] = jnp.where(lane == 0, first, jnp.where(lane == 1, second, 0.0))
        vec_s[0:1, :] += jnp.sum(ga * n, axis=0, keepdims=True)
        vec_s[1:2, :] += jnp.sum(ga, axis=0, keepdims=True)
        main(c).start()
        side(c).start()
        return carry

    lax.fori_loop(0, chunks, forward, 0)
    vectors = to_peer(vec_s, vec_p, send_sem.at[2, 0], recv_sem.at[2, 0])
    for k, item in enumerate((dq, dk, dv)):
        late[width * k : width * (k + 1), :] = dot_tn(item[...], a[...]).astype(BF16)
    vectors.start()
    qv = [jnp.sum(item[...].astype(F32), axis=0, keepdims=True) for item in (dq, dv)]

    def backward(c, carry):
        at = pl.ds(pl.multiple_of(c * CHUNK, CHUNK), CHUNK)
        main(c).wait()
        side(c).wait()
        sums = stat[at, :] + stat_p[at, :]
        n, r = norms(at)
        wide[...] = n
        e = (ga_s[at, :] + got[at, :].astype(F32)) * gain[:, own]
        gx = gr[at, :] + r * (e - sums[:, 0:1] - wide[:, own] * sums[:, 1:2])
        out[at, :] = gx.astype(BF16)
        return carry

    lax.fori_loop(0, chunks, backward, 0)
    vectors.wait()
    first = vec_s[0:2, :] + vec_p[0:2, :]
    parts = [first[0:1], first[1:2]] + [vec2[k : k + 1, :] for k in range(4)]
    parts.append(jnp.concatenate(qv, axis=1))
    parts += [vec_in[:, model * k : model * (k + 1)] for k in range(vec_in.shape[1] // model)]
    parts += [table[k : k + 1, :] for k in range(table.shape[0])]
    parts.append(jnp.zeros((SMALL - len(parts), model), F32))
    late[3 * width : 3 * width + SMALL, :] = jnp.concatenate(parts, axis=0).astype(BF16)
    spare = late.shape[0] - 3 * width - SMALL
    late[3 * width + SMALL :, :] = jnp.zeros((spare, model), BF16)


def close(late_rows, tok, a, dq, dk, dv, wt, gain, gr, vec2, vec_in, table):
    rows, model = tok.shape
    width = dq.shape[1]
    half = gr.shape[1]
    chunks = rows // CHUNK
    shape = jax.ShapeDtypeStruct
    vm = pltpu.VMEM
    sems = pltpu.SemaphoreType.DMA((3, chunks))
    return pl.pallas_call(
        close_kernel,
        in_specs=[pl.BlockSpec(memory_space=pltpu.VMEM)] * 11,
        out_specs=[pl.BlockSpec(memory_space=pltpu.VMEM)] * 2,
        out_shape=[shape((rows, half), BF16), shape((late_rows, model), BF16)],
        scratch_shapes=[
            vm((rows, half), F32), vm((rows, half), BF16), vm((rows, half), BF16), vm((rows, 128), F32),
            vm((rows, 128), F32), vm((CHUNK, model), F32), vm((8, model), F32), vm((8, model), F32),
            sems, sems,
        ],
        compiler_params=pltpu.CompilerParams(collective_id=3, has_side_effects=True),
        name="close",
    )(tok, a, dq, dk, dv, wt, gain, gr, vec2, vec_in, table)


def dp_copy(src, dst, partner, send_sem, recv_sem):
    return pltpu.make_async_remote_copy(
        src_ref=src,
        dst_ref=dst,
        send_sem=send_sem,
        recv_sem=recv_sem,
        device_id={"dp": partner},
        device_id_type=MESH,
    )


def dp_sum_kernel(orders, x, out, acc, got, send_sem, recv_sem):
    rows, wide = x.shape
    part = wide // len(orders)
    steps = len(orders[0])
    place = lax.axis_index("dp")

    def bit_of(b):
        return lax.rem(lax.div(place, 1 << b), 2)

    def partner_of(b):
        return place + (1 - 2 * bit_of(b)) * (1 << b)

    barrier = pltpu.get_barrier_semaphore()
    for b in range(steps):
        pl.semaphore_signal(barrier, inc=1, device_id={"dp": partner_of(b)}, device_id_type=MESH)
    pl.semaphore_wait(barrier, steps)

    state = [(x, 0)] * len(orders)
    kept = [[] for _ in orders]
    for s in range(steps):
        size = rows >> (s + 1)
        base = rows - (rows >> s)
        copies = []
        for k, order in enumerate(orders):
            src, low = state[k]
            lanes = pl.ds(part * k, part)
            bit = bit_of(order[s])
            mine = pl.multiple_of(low + bit * size, 16)
            theirs = pl.multiple_of(low + (1 - bit) * size, 16)
            copy = dp_copy(
                src.at[pl.ds(theirs, size), lanes],
                got.at[pl.ds(base, size), lanes],
                partner_of(order[s]),
                send_sem.at[k, s],
                recv_sem.at[k, s],
            )
            copy.start()
            copies.append(copy)
            kept[k].append(low)
            state[k] = (src, mine)
        for k, order in enumerate(orders):
            src, mine = state[k]
            lanes = slice(part * k, part * (k + 1))
            copies[k].wait()
            total = src[pl.ds(mine, size), lanes].astype(F32) + got[base : base + size, lanes].astype(F32)
            goal = out if s == steps - 1 else acc
            goal[pl.ds(mine, size), lanes] = total.astype(BF16)
            state[k] = (goal, mine)
    for s in reversed(range(steps)):
        size = rows >> (s + 1)
        copies = []
        for k, order in enumerate(orders):
            low = state[k][1]
            lanes = pl.ds(part * k, part)
            region = out.at[pl.ds(pl.multiple_of(low, 16), size), lanes]
            at = 2 * steps - 1 - s
            copy = dp_copy(region, region, partner_of(order[s]), send_sem.at[k, at], recv_sem.at[k, at])
            copy.start()
            copies.append(copy)
            state[k] = (out, kept[k][s])
        for copy in copies:
            copy.wait()


def dp_sum(ranks, x):
    rows, wide = x.shape
    steps = ranks.bit_length() - 1
    orders = [list(range(steps)), [0] + list(range(2, steps)) + [1]]
    vm = pltpu.VMEM
    sems = pltpu.SemaphoreType.DMA((2, 2 * steps))
    return pl.pallas_call(
        partial(dp_sum_kernel, orders),
        in_specs=[pl.BlockSpec(memory_space=pltpu.VMEM)],
        out_specs=pl.BlockSpec(memory_space=pltpu.VMEM),
        out_shape=jax.ShapeDtypeStruct((rows, wide), BF16),
        scratch_shapes=[vm((rows, wide), BF16), vm((rows, wide), BF16), sems, sems],
        compiler_params=pltpu.CompilerParams(collective_id=4, has_side_effects=True),
        name="dp_sum",
    )(x)


def window_data(crop_counts, crop_patches, rel_index, rel_table, rows):
    highest = lax.Precision.HIGHEST
    heads = rel_table.shape[1]
    cells, wins = layout(crop_counts, crop_patches, rows)
    kcells = jnp.pad(cells, (HALO, HALO))
    kwin = jnp.pad(wins, (HALO, HALO), constant_values=-1)[:, None]
    span_cells = jnp.arange(CP, dtype=jnp.int32)
    wide_cells = jnp.arange(2 * CP, dtype=jnp.int32) % CP
    khot = (kcells[:, None] == wide_cells[None, :]).astype(BF16)
    khott = (span_cells[:, None] == kcells[None, :]).astype(BF16)
    qhott = (span_cells[:, None] == cells[None, :]).astype(BF16)
    qhot = (cells[:, None] == span_cells[None, :]).astype(BF16)
    rel_t = jnp.pad(rel_index.T, ((0, CP - CELLS), (0, CP - CELLS)), constant_values=-1).reshape(-1)
    offset_hot = (rel_t[:, None] == jnp.arange(OFFSETS, dtype=jnp.int32)[None, :]).astype(F32)
    bias = jnp.einsum("pm,mh->hp", offset_hot, rel_table, precision=highest) / SCALE
    high = bias.astype(BF16)
    rest = (bias - high.astype(F32)).astype(BF16)
    table = jnp.stack([high.reshape(heads, CP, CP), rest.reshape(heads, CP, CP)], axis=1)
    return (khot, khott, qhott, qhot, table.reshape(heads * 2 * CP, CP), kwin, wins[None, :], offset_hot)


def body(
    tokens,
    crop_counts,
    crop_patches,
    rel_index,
    ln1_gain,
    ln1_shift,
    w_qkv,
    qv_bias,
    rel_table,
    w_out,
    b_out,
    ln2_gain,
    ln2_shift,
    w_in,
    b_in,
    w_back,
    b_back,
    cotangent,
):
    highest = lax.Precision.HIGHEST
    rows, part_width = tokens.shape
    model = ln1_gain.shape[0]
    width = w_qkv.shape[2]
    heads = width // HEAD_DIM
    khot, khott, qhott, qhot, table, kwin, qwin, offset_hot = window_data(
        crop_counts, crop_patches, rel_index, rel_table, rows
    )
    whole_in = lax.all_gather(tokens, "mp", axis=1, tiled=True)
    whole_cot = lax.all_gather(cotangent, "mp", axis=1, tiled=True)
    wt = jnp.transpose(w_qkv, (1, 2, 0)).reshape(3 * width, model)
    mixer_in, qt, kx, kt, vx, heads_out, heads_peer, w_peer, lse = attn_fwd(
        w_out,
        whole_in, ln1_gain[None, :], ln1_shift[None, :], wt, qv_bias[0][:, None], qv_bias[1][:, None],
        qv_bias[1][None, :], khot, qhott, table, kwin, qwin,
    )
    keep, give, gr, dot_t, grad_w_out, grad_w_in, grad_w_back, vec2, grad_b_in = ffn(
        whole_in, heads_out, heads_peer, w_out, w_peer, b_out[None, :], ln2_gain[None, :], ln2_shift[None, :],
        w_in, b_in[None, :], w_back, b_back[None, :], whole_cot,
    )
    early = lax.psum((grad_w_in, grad_w_back, grad_w_out), "dp")
    out_half, grad_query, grad_key, grad_value, gcell = attn_bwd(
        keep, give, qt, kx, kt, vx, dot_t, khot, khott, qhott, qhot, table, kwin, qwin, lse
    )
    grad_table = jnp.einsum(
        "pm,hp->mh", offset_hot, gcell.reshape(heads, CP * CP), precision=highest
    )
    table_rows = -(-grad_table.size // model)
    table_flat = jnp.pad(grad_table.reshape(-1), (0, table_rows * model - grad_table.size))
    ranks = lax.axis_size("dp")
    late_rows = -(-(3 * width + SMALL) // (16 * ranks)) * 16 * ranks
    grad_half, late = close(
        late_rows, whole_in, mixer_in, grad_query, grad_key, grad_value, wt, ln1_gain[None, :], gr,
        vec2, grad_b_in, table_flat.reshape(table_rows, model),
    )
    late = dp_sum(ranks, late)
    early, late = lax.optimization_barrier((early, late))
    grad_w_in, grad_w_back, grad_w_out = (item.astype(F32) for item in early)
    late = late[: 3 * width + SMALL].astype(F32)
    grad_w_qkv = jnp.transpose(late[: 3 * width].reshape(3, width, model), (2, 0, 1))
    small = late[3 * width :]
    grad_g1, grad_c1, grad_g2, grad_c2, grad_b_out, grad_b_back = (small[k] for k in range(6))
    grad_qv_bias = small[6].reshape(2, width)
    hidden_rows = w_in.shape[1] // model
    grad_b_in = small[7 : 7 + hidden_rows].reshape(-1)
    flat = small[7 + hidden_rows : 7 + hidden_rows + table_rows].reshape(-1)
    grad_table = flat[: grad_table.size].reshape(grad_table.shape)
    return (
        out_half,
        grad_half,
        grad_g1,
        grad_c1,
        grad_w_qkv,
        grad_qv_bias,
        grad_table,
        grad_w_out,
        grad_b_out,
        grad_g2,
        grad_c2,
        grad_w_in,
        grad_b_in,
        grad_w_back,
        grad_b_back,
    )


def solution(mesh):
    return jax.shard_map(
        body,
        mesh=mesh,
        in_specs=(
            P("dp", "mp"),
            P("dp"),
            P("dp", None),
            P(),
            P(),
            P(),
            P(None, None, "mp"),
            P(None, "mp"),
            P(None, "mp"),
            P("mp", None),
            P(),
            P(),
            P(),
            P(None, "mp"),
            P("mp"),
            P("mp", None),
            P(),
            P("dp", "mp"),
        ),
        out_specs=(
            P("dp", "mp"),
            P("dp", "mp"),
            P(),
            P(),
            P(None, None, "mp"),
            P(None, "mp"),
            P(None, "mp"),
            P("mp", None),
            P(),
            P(),
            P(),
            P(None, "mp"),
            P("mp"),
            P("mp", None),
            P(),
        ),
        check_vma=False,
    )
```

```python
from functools import partial

import jax
import jax.numpy as jnp
from jax import lax
from jax.experimental import pallas as pl
from jax.experimental.pallas import tpu as pltpu
from jax.sharding import PartitionSpec as P

HEAD_DIM = 32
SIDE = 7
LOCAL_SIDE = 3
CELLS = 49
OFFSETS = 169
CROP_MAX = 8
QB = 128
HALO = 64
SPAN = QB + 2 * HALO
CP = 64
GROUP = 4
SCALE = HEAD_DIM ** (-0.5)
EPS = 1e-05
NEG = -1e30
CHUNK = 256
SMALL = 16
MESH = pl.DeviceIdType.MESH
F32 = jnp.float32
BF16 = jnp.bfloat16


def layout(counts, patches, row_count):
    live_crop = jnp.arange(CROP_MAX, dtype=jnp.int32)[None, :] < counts[:, None]
    crop_rows = jnp.where(live_crop, patches, 0).reshape(-1)
    crop_ends = jnp.cumsum(crop_rows)
    used_rows = crop_ends[-1]
    row_ids = jnp.arange(row_count, dtype=jnp.int32)
    passed = crop_ends[None, :] <= row_ids[:, None]
    window = jnp.sum(passed.astype(jnp.int32), axis=1)
    starts = jnp.max(jnp.where(passed, crop_ends[None, :], 0), axis=1)
    finish = jnp.min(jnp.where(passed, row_count + used_rows + 1, crop_ends[None, :]), axis=1)
    length = finish - starts
    offset = row_ids - starts
    grid_side = jnp.where(length >= CELLS, SIDE, LOCAL_SIDE).astype(jnp.int32)
    cell_index = offset // grid_side * SIDE + offset % grid_side
    inside = row_ids < used_rows
    cell_ids = jnp.where(inside, cell_index, 0)
    windows = jnp.where(inside, window, crop_rows.shape[0] + row_ids - used_rows)
    return (cell_ids, windows)


def layer_norm(values, gain, shift):
    center = values - jnp.mean(values, axis=-1, keepdims=True)
    spread = jnp.mean(center * center, axis=-1, keepdims=True)
    return center * lax.rsqrt(spread + EPS) * gain + shift


def dot(a, b):
    return jnp.dot(a, b, preferred_element_type=F32)


def dot_nt(a, b):
    return lax.dot_general(a, b, (((1,), (1,)), ((), ())), preferred_element_type=F32)


def stack_heads(rows_t):
    cols = []
    for j in range(GROUP):
        parts = []
        if j > 0:
            parts.append(jnp.zeros((HEAD_DIM * j, QB), BF16))
        parts.append(rows_t[HEAD_DIM * j : HEAD_DIM * (j + 1)])
        if j < GROUP - 1:
            parts.append(jnp.zeros((HEAD_DIM * (GROUP - 1 - j), QB), BF16))
        cols.append(jnp.concatenate(parts, axis=0))
    return jnp.concatenate(cols, axis=1)


def bias_rows(table, g, cells):
    tall = dot(table[2 * CP * GROUP * g : 2 * CP * GROUP * (g + 1), :], cells).astype(BF16)
    return jnp.concatenate([tall[2 * CP * j : 2 * CP * (j + 1)] for j in range(GROUP)], axis=1)


def dot_tn(a, b):
    return lax.dot_general(a, b, (((0,), (0,)), ((), ())), preferred_element_type=F32)


def peer_of():
    return 1 - lax.axis_index("mp")


def greet():
    barrier = pltpu.get_barrier_semaphore()
    pl.semaphore_signal(barrier, inc=1, device_id={"mp": peer_of()}, device_id_type=MESH)
    pl.semaphore_wait(barrier, 1)


def to_peer(src, dst, send_sem, recv_sem):
    return pltpu.make_async_remote_copy(
        src_ref=src,
        dst_ref=dst,
        send_sem=send_sem,
        recv_sem=recv_sem,
        device_id={"mp": peer_of()},
        device_id_type=MESH,
    )


def rows_copy(src, dst, size, sems, i):
    at = pl.ds(pl.multiple_of(i * size, size), size)
    return to_peer(src.at[at], dst.at[at], sems[0].at[i], sems[1].at[i])


def half_lanes(index, half):
    return pl.ds(pl.multiple_of(index * half, 128), half)


def attn_fwd_kernel(
    groups, w_own, tok, gain, shift, wt, qb_col, vb_col, vb_row, khot, qhott, table, kwin, qwin,
    a_out, qt, kx, kt, vx, o_out, peer_out, w_out, lse, a_pad, vt, o_all, o_peer, w_got, send_sem, recv_sem,
):
    step = pl.program_id(0)
    last = tok.shape[0] // QB - 1
    rows_all = tok.shape[0]
    width = qt.shape[0]
    sems = (send_sem, recv_sem)
    weight = to_peer(w_own, w_got, send_sem.at[last + 1], recv_sem.at[last + 1])

    @pl.when(step == 0)
    def _():
        greet()
        weight.start()
        zero = jnp.zeros((HALO, tok.shape[1]), BF16)
        a_pad[:HALO, :] = zero
        a_pad[HALO + rows_all :, :] = zero

        def norm_rows(i, carry):
            at = pl.multiple_of(i * QB, QB)
            a = layer_norm(tok[pl.ds(at, QB), :].astype(F32), gain[...], shift[...]).astype(BF16)
            a_out[pl.ds(at, QB), :] = a
            a_pad[pl.ds(pl.multiple_of(at + HALO, HALO), QB), :] = a
            return carry

        lax.fori_loop(0, rows_all // QB, norm_rows, 0)
        a_all = a_pad[...]
        wk = wt[width : 2 * width, :]
        wv = wt[2 * width :, :]
        qt[...] = (dot_nt(wt[:width, :], a_out[...]) + qb_col[...]).astype(BF16)
        kx[...] = dot_nt(a_all, wk).astype(BF16)
        kt[...] = dot_nt(wk, a_all).astype(BF16)
        vx[...] = (dot_nt(a_all, wv) + vb_row[...]).astype(BF16)
        vt[...] = (dot_nt(wv, a_all) + vb_col[...]).astype(BF16)

    start = pl.multiple_of(step * QB, QB)
    span = pl.ds(start, SPAN)
    mask = jnp.where(kwin[span, :] == qwin[...], 0.0, NEG)
    hot = khot[span, :]
    cells = qhott[...]
    for g in range(groups):
        lanes = slice(128 * g, 128 * (g + 1))
        right = jnp.concatenate(
            [stack_heads(qt[lanes, pl.ds(start, QB)]), bias_rows(table, g, cells)], axis=0
        )
        scores = dot(jnp.concatenate([kx[span, lanes], hot], axis=1), right)
        outs = []
        for j in range(GROUP):
            h = GROUP * g + j
            s = scores[:, QB * j : QB * (j + 1)] * SCALE + mask
            peak = jnp.max(s, axis=0, keepdims=True)
            e = jnp.exp(s - peak)
            mass = jnp.sum(e, axis=0, keepdims=True)
            outs.append(dot(vt[HEAD_DIM * h : HEAD_DIM * (h + 1), span], e.astype(BF16)) / mass)
            lse[h : h + 1, :] = peak + jnp.log(mass)
        o_all[pl.ds(start, QB), lanes] = jnp.concatenate(outs, axis=0).T.astype(BF16)

    @pl.when(step > 0)
    def _():
        rows_copy(o_all, o_peer, QB, sems, step - 1).start()

    @pl.when(step == last)
    def _():
        o_out[...] = o_all[...]
        rows_copy(o_all, o_peer, QB, sems, last).start()

        def finish(i, carry):
            copy = rows_copy(o_all, o_peer, QB, sems, i)
            copy.wait()
            return carry

        lax.fori_loop(0, last + 1, finish, 0)
        weight.wait()
        w_out[...] = w_got[...]
        peer_out[...] = o_peer[...]


def whole(a):
    return pl.BlockSpec(a.shape, lambda i: (0,) * len(a.shape))


def same(*shape):
    return pl.BlockSpec(shape, lambda i: (0,) * len(shape))


def cols(n):
    return pl.BlockSpec((n, QB), lambda i: (0, i))


def two_sems(n):
    return [pltpu.SemaphoreType.DMA((n,)), pltpu.SemaphoreType.DMA((n,))]


def attn_fwd(w_own, tok, gain, shift, wt, qb_col, vb_col, vb_row, khot, qhott, table, kwin, qwin):
    rows, model = tok.shape
    width = wt.shape[0] // 3
    heads = width // HEAD_DIM
    ext = rows + 2 * HALO
    shape = jax.ShapeDtypeStruct
    return pl.pallas_call(
        partial(attn_fwd_kernel, heads // GROUP),
        grid=(rows // QB,),
        in_specs=[pl.BlockSpec(memory_space=pltpu.VMEM)]
        + [whole(x) for x in (tok, gain, shift, wt, qb_col, vb_col, vb_row, khot)]
        + [cols(CP), whole(table), whole(kwin), cols(1)],
        out_specs=[
            same(rows, model), same(width, rows), same(ext, width), same(width, ext), same(ext, width),
            same(rows, width), same(rows, width), same(width, model), cols(heads),
        ],
        out_shape=[
            shape((rows, model), BF16), shape((width, rows), BF16), shape((ext, width), BF16),
            shape((width, ext), BF16), shape((ext, width), BF16), shape((rows, width), BF16),
            shape((rows, width), BF16), shape((width, model), BF16), shape((heads, rows), F32),
        ],
        scratch_shapes=[
            pltpu.VMEM((ext, model), BF16), pltpu.VMEM((width, ext), BF16),
            pltpu.VMEM((rows, width), BF16), pltpu.VMEM((rows, width), BF16),
            pltpu.VMEM((width, model), BF16),
        ] + two_sems(rows // QB + 1),
        compiler_params=pltpu.CompilerParams(collective_id=0, has_side_effects=True),
        name="attn_fwd",
    )(w_own, tok, gain, shift, wt, qb_col, vb_col, vb_row, khot, qhott, table, kwin, qwin)


def ffn_fwd_kernel(
    tok, o_own, o_peer, w_own, w_peer, bo, gain, shift, w_in, b_in, w_back, bb, cot_own,
    keep, give, n_out, r_out, h_out, slope_out, cot, g_back, z_s, cot_got, wide_a, wide_b, send_sem, recv_sem,
):
    rows_all, model = tok.shape
    half = keep.shape[1]
    chunks = rows_all // CHUNK
    me = lax.axis_index("mp")
    own = half_lanes(me, half)
    other = half_lanes(1 - me, half)
    greet()
    swap = to_peer(cot_own, cot_got, send_sem.at[0], recv_sem.at[0])
    swap.start()
    cot[:, own] = cot_own[...]

    def forward(c, carry):
        at = pl.ds(pl.multiple_of(c * CHUNK, CHUNK), CHUNK)
        x1 = tok[at, :].astype(F32) + dot(o_own[at, :], w_own[...]) + dot(o_peer[at, :], w_peer[...])
        x1 = x1 + bo[...]
        center = x1 - jnp.mean(x1, axis=-1, keepdims=True)
        r = lax.rsqrt(jnp.mean(center * center, axis=-1, keepdims=True) + EPS)
        n = center * r
        h = (n * gain[...] + shift[...]).astype(BF16)
        wide_b[...] = x1
        n_out[at, :] = n.astype(BF16)
        r_out[at, :] = r
        h_out[at, :] = h
        u = dot(h, w_in[...]) + b_in[...]
        cdf = 0.5 * (1.0 + lax.erf(u * (0.5**0.5)))
        slope = cdf + u * (jnp.exp(-0.5 * u * u) * 0.3989422804014327)
        slope_out[at, :] = slope.astype(BF16)
        z = (u * cdf).astype(BF16)
        z_s[at, :] = z
        wide_a[...] = dot(z, w_back[...])
        keep[at, :] = wide_a[:, own] + wide_b[:, own] + bb[:, own]
        give[at, :] = wide_a[:, other].astype(BF16)
        return carry

    lax.fori_loop(0, chunks, forward, 0)
    swap.wait()
    cot[:, other] = cot_got[...]

    def back_block(i, carry):
        at = pl.ds(pl.multiple_of(i * CHUNK, CHUNK), CHUNK)
        g_back[at, :] = dot_tn(z_s[:, at], cot[...]).astype(BF16)
        return carry

    lax.fori_loop(0, z_s.shape[1] // CHUNK, back_block, 0)


def ffn_fwd(tok, o_own, o_peer, w_own, w_peer, bo, gain, shift, w_in, b_in, w_back, bb, cot_own):
    rows, model = tok.shape
    hidden = w_in.shape[1]
    half = cot_own.shape[1]
    shape = jax.ShapeDtypeStruct
    vm = pltpu.VMEM
    return pl.pallas_call(
        ffn_fwd_kernel,
        in_specs=[pl.BlockSpec(memory_space=pltpu.VMEM)] * 13,
        out_specs=[pl.BlockSpec(memory_space=pltpu.VMEM)] * 8,
        out_shape=[
            shape((rows, half), F32), shape((rows, half), BF16), shape((rows, model), BF16),
            shape((rows, 1), F32), shape((rows, model), BF16), shape((rows, hidden), BF16),
            shape((rows, model), BF16), shape((hidden, model), BF16),
        ],
        scratch_shapes=[
            vm((rows, hidden), BF16), vm((rows, half), BF16), vm((CHUNK, model), F32), vm((CHUNK, model), F32),
        ] + two_sems(1),
        compiler_params=pltpu.CompilerParams(collective_id=1, has_side_effects=True),
        name="ffn_fwd",
    )(tok, o_own, o_peer, w_own, w_peer, bo, gain, shift, w_in, b_in, w_back, bb, cot_own)


def ffn_bwd_kernel(
    n_in, r_in, h_in, slope, cot, w_in, w_back, w_own, gain, o_own,
    gr, dot_t, g_out, g_in, vec, vec_in, du_s, gh_s, gh_p, go_s, wide_a, send_sem, recv_sem,
):
    rows_all, model = n_in.shape
    half = gr.shape[1]
    chunks = rows_all // CHUNK
    sems = (send_sem, recv_sem)
    own = half_lanes(lax.axis_index("mp"), half)
    greet()
    vec[...] = jnp.zeros_like(vec)
    vec_in[...] = jnp.zeros_like(vec_in)

    def forward(c, carry):
        at = pl.ds(pl.multiple_of(c * CHUNK, CHUNK), CHUNK)
        du = (dot_nt(cot[at, :], w_back[...]) * slope[at, :].astype(F32)).astype(BF16)
        du_s[at, :] = du
        gh_s[at, :] = dot_nt(du, w_in[...]).astype(BF16)
        vec_in[...] += jnp.sum(du.astype(F32), axis=0, keepdims=True)
        rows_copy(gh_s, gh_p, CHUNK, sems, c).start()
        return carry

    lax.fori_loop(0, chunks, forward, 0)

    def in_block(i, carry):
        at = pl.ds(pl.multiple_of(i * CHUNK, CHUNK), CHUNK)
        g_in[at, :] = dot_tn(h_in[:, at], du_s[...]).astype(BF16)
        return carry

    lax.fori_loop(0, model // CHUNK, in_block, 0)

    def backward(c, carry):
        at = pl.ds(pl.multiple_of(c * CHUNK, CHUNK), CHUNK)
        rows_copy(gh_s, gh_p, CHUNK, sems, c).wait()
        gh = gh_s[at, :].astype(F32) + gh_p[at, :].astype(F32)
        n = n_in[at, :].astype(F32)
        e = gh * gain[...]
        gy = cot[at, :].astype(F32)
        mean_e = jnp.mean(e, axis=-1, keepdims=True)
        mean_n = jnp.mean(e * n, axis=-1, keepdims=True)
        gx1 = gy + r_in[at, :] * (e - mean_e - n * mean_n)
        wide_a[...] = gx1
        go = gx1.astype(BF16)
        go_s[at, :] = go
        dot_t[:, at] = dot_nt(w_own[...], go).astype(BF16)
        vec[0:1, :] += jnp.sum(gh * n, axis=0, keepdims=True)
        vec[1:2, :] += jnp.sum(gh, axis=0, keepdims=True)
        vec[2:3, :] += jnp.sum(go.astype(F32), axis=0, keepdims=True)
        vec[3:4, :] += jnp.sum(gy, axis=0, keepdims=True)
        gr[at, :] = wide_a[:, own]
        return carry

    lax.fori_loop(0, chunks, backward, 0)
    g_out[...] = dot_tn(o_own[...], go_s[...]).astype(BF16)


def ffn_bwd(n_in, r_in, h_in, slope, cot, w_in, w_back, w_own, gain, o_own):
    rows, model = n_in.shape
    width = o_own.shape[1]
    hidden = w_in.shape[1]
    half = model // 2
    shape = jax.ShapeDtypeStruct
    vm = pltpu.VMEM
    return pl.pallas_call(
        ffn_bwd_kernel,
        in_specs=[pl.BlockSpec(memory_space=pltpu.VMEM)] * 10,
        out_specs=[pl.BlockSpec(memory_space=pltpu.VMEM)] * 6,
        out_shape=[
            shape((rows, half), F32), shape((width, rows), BF16), shape((width, model), BF16),
            shape((model, hidden), BF16), shape((8, model), F32), shape((1, hidden), F32),
        ],
        scratch_shapes=[
            vm((rows, hidden), BF16), vm((rows, model), BF16), vm((rows, model), BF16),
            vm((rows, model), BF16), vm((CHUNK, model), F32),
        ] + two_sems(rows // CHUNK),
        compiler_params=pltpu.CompilerParams(collective_id=5, has_side_effects=True),
        name="ffn_bwd",
    )(n_in, r_in, h_in, slope, cot, w_in, w_back, w_own, gain, o_own)


def attn_bwd_kernel(
    groups, keep, give, qt, kx, kt, vx, dot_t, khot, khott, qhott, qhot, table, kwin, qwin, lse,
    out, dq, dk, dv, gcell, dk_acc, dv_acc, got, send_sem, recv_sem,
):
    step = pl.program_id(0)
    rows_all = dk.shape[0]
    swap = to_peer(give, got, send_sem.at[0], recv_sem.at[0])

    @pl.when(step == 0)
    def _():
        greet()
        swap.start()
        dk_acc[...] = jnp.zeros_like(dk_acc)
        dv_acc[...] = jnp.zeros_like(dv_acc)
        gcell[...] = jnp.zeros_like(gcell)

    start = pl.multiple_of(step * QB, QB)
    span = pl.ds(start, SPAN)
    mask = jnp.where(kwin[span, :] == qwin[...], 0.0, NEG)
    hot = khot[span, :]
    hot_t = khott[:, span]
    cells = qhott[...]
    cells_r = qhot[...]
    for g in range(groups):
        lanes = slice(128 * g, 128 * (g + 1))
        q_stack = stack_heads(qt[lanes, :])
        do_stack = stack_heads(dot_t[lanes, :])
        right = jnp.concatenate([q_stack, bias_rows(table, g, cells)], axis=0)
        scores = dot(jnp.concatenate([kx[span, lanes], hot], axis=1), right)
        dprob = dot(vx[span, lanes], do_stack)
        ps, dss, dqs = [], [], []
        for j in range(GROUP):
            h = GROUP * g + j
            cut = slice(QB * j, QB * (j + 1))
            p = jnp.exp(scores[:, cut] * SCALE + mask - lse[h : h + 1, :])
            t = p * dprob[:, cut]
            inner = jnp.sum(t, axis=0, keepdims=True)
            ds = (t - p * inner).astype(BF16)
            ps.append(p.astype(BF16))
            dss.append(ds)
            both = dot(jnp.concatenate([kt[HEAD_DIM * h : HEAD_DIM * (h + 1), span], hot_t], axis=0), ds)
            dqs.append(both[:HEAD_DIM])
            gcell[CP * h : CP * (h + 1), :] += dot(both[HEAD_DIM:].astype(BF16), cells_r)
        dq[:, lanes] = (jnp.concatenate(dqs, axis=0) * SCALE).T.astype(BF16)
        dk_acc[span, lanes] += dot_nt(jnp.concatenate(dss, axis=1), q_stack)
        dv_acc[span, lanes] += dot_nt(jnp.concatenate(ps, axis=1), do_stack)

    @pl.when(step == rows_all // QB - 1)
    def _():
        inner_rows = pl.ds(HALO, rows_all)
        dk[...] = (dk_acc[inner_rows, :] * SCALE).astype(BF16)
        dv[...] = dv_acc[inner_rows, :].astype(BF16)
        swap.wait()
        out[...] = (keep[...] + got[...].astype(F32)).astype(BF16)


def attn_bwd(keep, give, qt, kx, kt, vx, dot_t, khot, khott, qhott, qhot, table, kwin, qwin, lse):
    width, rows = qt.shape
    heads = width // HEAD_DIM
    ext = rows + 2 * HALO
    half = keep.shape[1]
    shape = jax.ShapeDtypeStruct
    rblk = lambda n: pl.BlockSpec((QB, n), lambda i: (i, 0))
    return pl.pallas_call(
        partial(attn_bwd_kernel, heads // GROUP),
        grid=(rows // QB,),
        in_specs=[
            whole(keep), pl.BlockSpec(memory_space=pltpu.VMEM),
            cols(width), whole(kx), whole(kt), whole(vx), cols(width), whole(khot), whole(khott),
            cols(CP), rblk(CP), whole(table), whole(kwin), cols(1), cols(heads),
        ],
        out_specs=[
            same(rows, half), rblk(width), same(rows, width), same(rows, width), same(CP * heads, CP),
        ],
        out_shape=[
            shape((rows, half), BF16), shape((rows, width), BF16), shape((rows, width), BF16),
            shape((rows, width), BF16), shape((CP * heads, CP), F32),
        ],
        scratch_shapes=[
            pltpu.VMEM((ext, width), F32), pltpu.VMEM((ext, width), F32), pltpu.VMEM((rows, half), BF16),
        ] + two_sems(1),
        compiler_params=pltpu.CompilerParams(collective_id=2, has_side_effects=True),
        name="attn_bwd",
    )(keep, give, qt, kx, kt, vx, dot_t, khot, khott, qhott, qhot, table, kwin, qwin, lse)


def close_kernel(
    tok, a, dq, dk, dv, wt, gain, gr, vec2, vec_in, table, out, late,
    ga_s, give, got, stat, stat_p, wide, vec_s, vec_p, send_sem, recv_sem,
):
    rows_all, model = tok.shape
    width = dq.shape[1]
    half = out.shape[1]
    chunks = rows_all // CHUNK
    me = lax.axis_index("mp")
    own = half_lanes(me, half)
    other = half_lanes(1 - me, half)
    greet()
    vec_s[...] = jnp.zeros_like(vec_s)
    main = lambda c: rows_copy(give, got, CHUNK, (send_sem.at[0], recv_sem.at[0]), c)
    side = lambda c: rows_copy(stat, stat_p, CHUNK, (send_sem.at[1], recv_sem.at[1]), c)
    lane = lax.broadcasted_iota(jnp.int32, (CHUNK, 128), 1)

    def norms(at):
        x = tok[at, :].astype(F32)
        center = x - jnp.mean(x, axis=-1, keepdims=True)
        r = lax.rsqrt(jnp.mean(center * center, axis=-1, keepdims=True) + EPS)
        return center * r, r

    def forward(c, carry):
        at = pl.ds(pl.multiple_of(c * CHUNK, CHUNK), CHUNK)
        ga = dot(dq[at, :], wt[:width, :]) + dot(dk[at, :], wt[width : 2 * width, :])
        ga = ga + dot(dv[at, :], wt[2 * width :, :])
        wide[...] = ga
        give[at, :] = wide[:, other].astype(BF16)
        ga_s[at, :] = wide[:, own]
        n, r = norms(at)
        e = ga * gain[...]
        first = jnp.mean(e, axis=-1, keepdims=True)
        second = jnp.mean(e * n, axis=-1, keepdims=True)
        stat[at, :] = jnp.where(lane == 0, first, jnp.where(lane == 1, second, 0.0))
        vec_s[0:1, :] += jnp.sum(ga * n, axis=0, keepdims=True)
        vec_s[1:2, :] += jnp.sum(ga, axis=0, keepdims=True)
        main(c).start()
        side(c).start()
        return carry

    lax.fori_loop(0, chunks, forward, 0)
    vectors = to_peer(vec_s, vec_p, send_sem.at[2, 0], recv_sem.at[2, 0])
    for k, item in enumerate((dq, dk, dv)):
        late[width * k : width * (k + 1), :] = dot_tn(item[...], a[...]).astype(BF16)
    vectors.start()
    qv = [jnp.sum(item[...].astype(F32), axis=0, keepdims=True) for item in (dq, dv)]

    def backward(c, carry):
        at = pl.ds(pl.multiple_of(c * CHUNK, CHUNK), CHUNK)
        main(c).wait()
        side(c).wait()
        sums = stat[at, :] + stat_p[at, :]
        n, r = norms(at)
        wide[...] = n
        e = (ga_s[at, :] + got[at, :].astype(F32)) * gain[:, own]
        gx = gr[at, :] + r * (e - sums[:, 0:1] - wide[:, own] * sums[:, 1:2])
        out[at, :] = gx.astype(BF16)
        return carry

    lax.fori_loop(0, chunks, backward, 0)
    vectors.wait()
    first = vec_s[0:2, :] + vec_p[0:2, :]
    parts = [first[0:1], first[1:2]] + [vec2[k : k + 1, :] for k in range(4)]
    parts.append(jnp.concatenate(qv, axis=1))
    parts += [vec_in[:, model * k : model * (k + 1)] for k in range(vec_in.shape[1] // model)]
    parts += [table[k : k + 1, :] for k in range(table.shape[0])]
    parts.append(jnp.zeros((SMALL - len(parts), model), F32))
    late[3 * width : 3 * width + SMALL, :] = jnp.concatenate(parts, axis=0).astype(BF16)
    spare = late.shape[0] - 3 * width - SMALL
    late[3 * width + SMALL :, :] = jnp.zeros((spare, model), BF16)


def close(late_rows, tok, a, dq, dk, dv, wt, gain, gr, vec2, vec_in, table):
    rows, model = tok.shape
    width = dq.shape[1]
    half = gr.shape[1]
    chunks = rows // CHUNK
    shape = jax.ShapeDtypeStruct
    vm = pltpu.VMEM
    sems = pltpu.SemaphoreType.DMA((3, chunks))
    return pl.pallas_call(
        close_kernel,
        in_specs=[pl.BlockSpec(memory_space=pltpu.VMEM)] * 11,
        out_specs=[pl.BlockSpec(memory_space=pltpu.VMEM)] * 2,
        out_shape=[shape((rows, half), BF16), shape((late_rows, model), BF16)],
        scratch_shapes=[
            vm((rows, half), F32), vm((rows, half), BF16), vm((rows, half), BF16), vm((rows, 128), F32),
            vm((rows, 128), F32), vm((CHUNK, model), F32), vm((8, model), F32), vm((8, model), F32),
            sems, sems,
        ],
        compiler_params=pltpu.CompilerParams(collective_id=3, has_side_effects=True),
        name="close",
    )(tok, a, dq, dk, dv, wt, gain, gr, vec2, vec_in, table)


def dp_copy(src, dst, partner, send_sem, recv_sem):
    return pltpu.make_async_remote_copy(
        src_ref=src,
        dst_ref=dst,
        send_sem=send_sem,
        recv_sem=recv_sem,
        device_id={"dp": partner},
        device_id_type=MESH,
    )


def dp_sum_kernel(orders, x, out, acc, got, send_sem, recv_sem):
    rows, wide = x.shape
    part = wide // len(orders)
    steps = len(orders[0])
    place = lax.axis_index("dp")

    def bit_of(b):
        return lax.rem(lax.div(place, 1 << b), 2)

    def partner_of(b):
        return place + (1 - 2 * bit_of(b)) * (1 << b)

    barrier = pltpu.get_barrier_semaphore()
    for b in range(steps):
        pl.semaphore_signal(barrier, inc=1, device_id={"dp": partner_of(b)}, device_id_type=MESH)
    pl.semaphore_wait(barrier, steps)

    state = [(x, 0)] * len(orders)
    kept = [[] for _ in orders]
    for s in range(steps):
        size = rows >> (s + 1)
        base = rows - (rows >> s)
        copies = []
        for k, order in enumerate(orders):
            src, low = state[k]
            lanes = pl.ds(part * k, part)
            bit = bit_of(order[s])
            mine = pl.multiple_of(low + bit * size, 16)
            theirs = pl.multiple_of(low + (1 - bit) * size, 16)
            copy = dp_copy(
                src.at[pl.ds(theirs, size), lanes],
                got.at[pl.ds(base, size), lanes],
                partner_of(order[s]),
                send_sem.at[k, s],
                recv_sem.at[k, s],
            )
            copy.start()
            copies.append(copy)
            kept[k].append(low)
            state[k] = (src, mine)
        for k, order in enumerate(orders):
            src, mine = state[k]
            lanes = slice(part * k, part * (k + 1))
            copies[k].wait()
            total = src[pl.ds(mine, size), lanes].astype(F32) + got[base : base + size, lanes].astype(F32)
            goal = out if s == steps - 1 else acc
            goal[pl.ds(mine, size), lanes] = total.astype(BF16)
            state[k] = (goal, mine)
    for s in reversed(range(steps)):
        size = rows >> (s + 1)
        copies = []
        for k, order in enumerate(orders):
            low = state[k][1]
            lanes = pl.ds(part * k, part)
            region = out.at[pl.ds(pl.multiple_of(low, 16), size), lanes]
            at = 2 * steps - 1 - s
            copy = dp_copy(region, region, partner_of(order[s]), send_sem.at[k, at], recv_sem.at[k, at])
            copy.start()
            copies.append(copy)
            state[k] = (out, kept[k][s])
        for copy in copies:
            copy.wait()


def dp_sum(ranks, x):
    rows, wide = x.shape
    steps = ranks.bit_length() - 1
    orders = [list(range(steps)), [0] + list(range(2, steps)) + [1]]
    vm = pltpu.VMEM
    sems = pltpu.SemaphoreType.DMA((2, 2 * steps))
    return pl.pallas_call(
        partial(dp_sum_kernel, orders),
        in_specs=[pl.BlockSpec(memory_space=pltpu.VMEM)],
        out_specs=pl.BlockSpec(memory_space=pltpu.VMEM),
        out_shape=jax.ShapeDtypeStruct((rows, wide), BF16),
        scratch_shapes=[vm((rows, wide), BF16), vm((rows, wide), BF16), sems, sems],
        compiler_params=pltpu.CompilerParams(collective_id=4, has_side_effects=True),
        name="dp_sum",
    )(x)


def window_data(crop_counts, crop_patches, rel_index, rel_table, rows):
    highest = lax.Precision.HIGHEST
    heads = rel_table.shape[1]
    cells, wins = layout(crop_counts, crop_patches, rows)
    kcells = jnp.pad(cells, (HALO, HALO))
    kwin = jnp.pad(wins, (HALO, HALO), constant_values=-1)[:, None]
    span_cells = jnp.arange(CP, dtype=jnp.int32)
    wide_cells = jnp.arange(2 * CP, dtype=jnp.int32) % CP
    khot = (kcells[:, None] == wide_cells[None, :]).astype(BF16)
    khott = (span_cells[:, None] == kcells[None, :]).astype(BF16)
    qhott = (span_cells[:, None] == cells[None, :]).astype(BF16)
    qhot = (cells[:, None] == span_cells[None, :]).astype(BF16)
    rel_t = jnp.pad(rel_index.T, ((0, CP - CELLS), (0, CP - CELLS)), constant_values=-1).reshape(-1)
    offset_hot = (rel_t[:, None] == jnp.arange(OFFSETS, dtype=jnp.int32)[None, :]).astype(F32)
    bias = jnp.einsum("pm,mh->hp", offset_hot, rel_table, precision=highest) / SCALE
    high = bias.astype(BF16)
    rest = (bias - high.astype(F32)).astype(BF16)
    table = jnp.stack([high.reshape(heads, CP, CP), rest.reshape(heads, CP, CP)], axis=1)
    return (khot, khott, qhott, qhot, table.reshape(heads * 2 * CP, CP), kwin, wins[None, :], offset_hot)


def body(
    tokens,
    crop_counts,
    crop_patches,
    rel_index,
    ln1_gain,
    ln1_shift,
    w_qkv,
    qv_bias,
    rel_table,
    w_out,
    b_out,
    ln2_gain,
    ln2_shift,
    w_in,
    b_in,
    w_back,
    b_back,
    cotangent,
):
    highest = lax.Precision.HIGHEST
    rows, part_width = tokens.shape
    model = ln1_gain.shape[0]
    width = w_qkv.shape[2]
    heads = width // HEAD_DIM
    khot, khott, qhott, qhot, table, kwin, qwin, offset_hot = window_data(
        crop_counts, crop_patches, rel_index, rel_table, rows
    )
    whole_in = lax.all_gather(tokens, "mp", axis=1, tiled=True)
    wt = jnp.transpose(w_qkv, (1, 2, 0)).reshape(3 * width, model)
    mixer_in, qt, kx, kt, vx, heads_out, heads_peer, w_peer, lse = attn_fwd(
        w_out,
        whole_in, ln1_gain[None, :], ln1_shift[None, :], wt, qv_bias[0][:, None], qv_bias[1][:, None],
        qv_bias[1][None, :], khot, qhott, table, kwin, qwin,
    )
    keep, give, normed, spread, hidden_in, slope, whole_cot, grad_w_back = ffn_fwd(
        whole_in, heads_out, heads_peer, w_out, w_peer, b_out[None, :], ln2_gain[None, :], ln2_shift[None, :],
        w_in, b_in[None, :], w_back, b_back[None, :], cotangent,
    )
    ranks = lax.axis_size("dp")
    grad_w_back = lax.psum(grad_w_back, "dp", axis_index_groups=[list(range(ranks))[::-1]])
    gr, dot_t, grad_w_out, grad_w_in, vec2, grad_b_in = ffn_bwd(
        normed, spread, hidden_in, slope, whole_cot, w_in, w_back, w_out, ln2_gain[None, :], heads_out
    )
    early = lax.psum((grad_w_in, grad_w_out), "dp")
    out_half, grad_query, grad_key, grad_value, gcell = attn_bwd(
        keep, give, qt, kx, kt, vx, dot_t, khot, khott, qhott, qhot, table, kwin, qwin, lse
    )
    grad_table = jnp.einsum(
        "pm,hp->mh", offset_hot, gcell.reshape(heads, CP * CP), precision=highest
    )
    table_rows = -(-grad_table.size // model)
    table_flat = jnp.pad(grad_table.reshape(-1), (0, table_rows * model - grad_table.size))
    late_rows = -(-(3 * width + SMALL) // (16 * ranks)) * 16 * ranks
    grad_half, late = close(
        late_rows, whole_in, mixer_in, grad_query, grad_key, grad_value, wt, ln1_gain[None, :], gr,
        vec2, grad_b_in, table_flat.reshape(table_rows, model),
    )
    late = dp_sum(ranks, late)
    grad_w_back, early, late = lax.optimization_barrier((grad_w_back, early, late))
    grad_w_back = grad_w_back.astype(F32)
    grad_w_in, grad_w_out = (item.astype(F32) for item in early)
    late = late[: 3 * width + SMALL].astype(F32)
    grad_w_qkv = jnp.transpose(late[: 3 * width].reshape(3, width, model), (2, 0, 1))
    small = late[3 * width :]
    grad_g1, grad_c1, grad_g2, grad_c2, grad_b_out, grad_b_back = (small[k] for k in range(6))
    grad_qv_bias = small[6].reshape(2, width)
    hidden_rows = w_in.shape[1] // model
    grad_b_in = small[7 : 7 + hidden_rows].reshape(-1)
    flat = small[7 + hidden_rows : 7 + hidden_rows + table_rows].reshape(-1)
    grad_table = flat[: grad_table.size].reshape(grad_table.shape)
    return (
        out_half,
        grad_half,
        grad_g1,
        grad_c1,
        grad_w_qkv,
        grad_qv_bias,
        grad_table,
        grad_w_out,
        grad_b_out,
        grad_g2,
        grad_c2,
        grad_w_in,
        grad_b_in,
        grad_w_back,
        grad_b_back,
    )


def solution(mesh):
    return jax.shard_map(
        body,
        mesh=mesh,
        in_specs=(
            P("dp", "mp"),
            P("dp"),
            P("dp", None),
            P(),
            P(),
            P(),
            P(None, None, "mp"),
            P(None, "mp"),
            P(None, "mp"),
            P("mp", None),
            P(),
            P(),
            P(),
            P(None, "mp"),
            P("mp"),
            P("mp", None),
            P(),
            P("dp", "mp"),
        ),
        out_specs=(
            P("dp", "mp"),
            P("dp", "mp"),
            P(),
            P(),
            P(None, None, "mp"),
            P(None, "mp"),
            P(None, "mp"),
            P("mp", None),
            P(),
            P(),
            P(),
            P(None, "mp"),
            P("mp"),
            P("mp", None),
            P(),
        ),
        check_vma=False,
    )
```

```python
from functools import partial

import jax
import jax.numpy as jnp
from jax import lax
from jax.experimental import pallas as pl
from jax.experimental.pallas import tpu as pltpu
from jax.sharding import PartitionSpec as P

HEAD_DIM = 32
SIDE = 7
LOCAL_SIDE = 3
CELLS = 49
OFFSETS = 169
CROP_MAX = 8
QB = 128
HALO = 64
SPAN = QB + 2 * HALO
CP = 64
GROUP = 4
SCALE = HEAD_DIM ** (-0.5)
EPS = 1e-05
NEG = -1e30
CHUNK = 256
SMALL = 16
MESH = pl.DeviceIdType.MESH
F32 = jnp.float32
BF16 = jnp.bfloat16


def layout(counts, patches, row_count):
    live_crop = jnp.arange(CROP_MAX, dtype=jnp.int32)[None, :] < counts[:, None]
    crop_rows = jnp.where(live_crop, patches, 0).reshape(-1)
    crop_ends = jnp.cumsum(crop_rows)
    used_rows = crop_ends[-1]
    row_ids = jnp.arange(row_count, dtype=jnp.int32)
    passed = crop_ends[None, :] <= row_ids[:, None]
    window = jnp.sum(passed.astype(jnp.int32), axis=1)
    starts = jnp.max(jnp.where(passed, crop_ends[None, :], 0), axis=1)
    finish = jnp.min(jnp.where(passed, row_count + used_rows + 1, crop_ends[None, :]), axis=1)
    length = finish - starts
    offset = row_ids - starts
    grid_side = jnp.where(length >= CELLS, SIDE, LOCAL_SIDE).astype(jnp.int32)
    cell_index = offset // grid_side * SIDE + offset % grid_side
    inside = row_ids < used_rows
    cell_ids = jnp.where(inside, cell_index, 0)
    windows = jnp.where(inside, window, crop_rows.shape[0] + row_ids - used_rows)
    return (cell_ids, windows)


def layer_norm(values, gain, shift):
    center = values - jnp.mean(values, axis=-1, keepdims=True)
    spread = jnp.mean(center * center, axis=-1, keepdims=True)
    return center * lax.rsqrt(spread + EPS) * gain + shift


def dot(a, b):
    return jnp.dot(a, b, preferred_element_type=F32)


def dot_nt(a, b):
    return lax.dot_general(a, b, (((1,), (1,)), ((), ())), preferred_element_type=F32)


def stack_heads(rows_t):
    cols = []
    for j in range(GROUP):
        parts = []
        if j > 0:
            parts.append(jnp.zeros((HEAD_DIM * j, QB), BF16))
        parts.append(rows_t[HEAD_DIM * j : HEAD_DIM * (j + 1)])
        if j < GROUP - 1:
            parts.append(jnp.zeros((HEAD_DIM * (GROUP - 1 - j), QB), BF16))
        cols.append(jnp.concatenate(parts, axis=0))
    return jnp.concatenate(cols, axis=1)


def bias_rows(table, g, cells):
    tall = dot(table[2 * CP * GROUP * g : 2 * CP * GROUP * (g + 1), :], cells).astype(BF16)
    return jnp.concatenate([tall[2 * CP * j : 2 * CP * (j + 1)] for j in range(GROUP)], axis=1)


def dot_tn(a, b):
    return lax.dot_general(a, b, (((0,), (0,)), ((), ())), preferred_element_type=F32)


def peer_of():
    return 1 - lax.axis_index("mp")


def greet():
    barrier = pltpu.get_barrier_semaphore()
    pl.semaphore_signal(barrier, inc=1, device_id={"mp": peer_of()}, device_id_type=MESH)
    pl.semaphore_wait(barrier, 1)


def to_peer(src, dst, send_sem, recv_sem):
    return pltpu.make_async_remote_copy(
        src_ref=src,
        dst_ref=dst,
        send_sem=send_sem,
        recv_sem=recv_sem,
        device_id={"mp": peer_of()},
        device_id_type=MESH,
    )


def rows_copy(src, dst, size, sems, i):
    at = pl.ds(pl.multiple_of(i * size, size), size)
    return to_peer(src.at[at], dst.at[at], sems[0].at[i], sems[1].at[i])


def half_lanes(index, half):
    return pl.ds(pl.multiple_of(index * half, 128), half)


def attn_fwd_kernel(
    groups, w_own, tok, gain, shift, wt, qb_col, vb_col, vb_row, khot, qhott, table, kwin, qwin,
    a_out, qt, kx, kt, vx, o_out, peer_out, w_out, lse, a_pad, vt, o_all, o_peer, w_got, send_sem, recv_sem,
):
    step = pl.program_id(0)
    last = tok.shape[0] // QB - 1
    rows_all = tok.shape[0]
    width = qt.shape[0]
    sems = (send_sem, recv_sem)
    place = lax.axis_index("dp")
    core = lax.rem(place, 2)
    mate = place + 1 - 2 * core
    fetched = w_own.shape[0] // 2
    part = pl.ds(pl.multiple_of(core * fetched, 16), fetched)
    weight = to_peer(w_own.at[part], w_got.at[part], send_sem.at[last + 1], recv_sem.at[last + 1])
    handed = dp_copy(w_got.at[part], w_got.at[part], mate, send_sem.at[last + 2], recv_sem.at[last + 2])

    @pl.when(step == 0)
    def _():
        barrier = pltpu.get_barrier_semaphore()
        pl.semaphore_signal(barrier, inc=1, device_id={"mp": peer_of()}, device_id_type=MESH)
        pl.semaphore_signal(barrier, inc=1, device_id={"dp": mate}, device_id_type=MESH)
        pl.semaphore_wait(barrier, 2)
        weight.start()
        zero = jnp.zeros((HALO, tok.shape[1]), BF16)
        a_pad[:HALO, :] = zero
        a_pad[HALO + rows_all :, :] = zero

        def norm_rows(i, carry):
            at = pl.multiple_of(i * QB, QB)
            a = layer_norm(tok[pl.ds(at, QB), :].astype(F32), gain[...], shift[...]).astype(BF16)
            a_out[pl.ds(at, QB), :] = a
            a_pad[pl.ds(pl.multiple_of(at + HALO, HALO), QB), :] = a
            return carry

        lax.fori_loop(0, rows_all // QB, norm_rows, 0)
        a_all = a_pad[...]
        wk = wt[width : 2 * width, :]
        wv = wt[2 * width :, :]
        qt[...] = (dot_nt(wt[:width, :], a_out[...]) + qb_col[...]).astype(BF16)
        kx[...] = dot_nt(a_all, wk).astype(BF16)
        kt[...] = dot_nt(wk, a_all).astype(BF16)
        vx[...] = (dot_nt(a_all, wv) + vb_row[...]).astype(BF16)
        vt[...] = (dot_nt(wv, a_all) + vb_col[...]).astype(BF16)

    start = pl.multiple_of(step * QB, QB)
    span = pl.ds(start, SPAN)
    mask = jnp.where(kwin[span, :] == qwin[...], 0.0, NEG)
    hot = khot[span, :]
    cells = qhott[...]
    for g in range(groups):
        lanes = slice(128 * g, 128 * (g + 1))
        right = jnp.concatenate(
            [stack_heads(qt[lanes, pl.ds(start, QB)]), bias_rows(table, g, cells)], axis=0
        )
        scores = dot(jnp.concatenate([kx[span, lanes], hot], axis=1), right)
        outs = []
        for j in range(GROUP):
            h = GROUP * g + j
            s = scores[:, QB * j : QB * (j + 1)] * SCALE + mask
            peak = jnp.max(s, axis=0, keepdims=True)
            e = jnp.exp(s - peak)
            mass = jnp.sum(e, axis=0, keepdims=True)
            outs.append(dot(vt[HEAD_DIM * h : HEAD_DIM * (h + 1), span], e.astype(BF16)) / mass)
            lse[h : h + 1, :] = peak + jnp.log(mass)
        o_all[pl.ds(start, QB), lanes] = jnp.concatenate(outs, axis=0).T.astype(BF16)

    @pl.when(step > 0)
    def _():
        rows_copy(o_all, o_peer, QB, sems, step - 1).start()

    @pl.when(step == last - 2)
    def _():
        weight.wait()
        handed.start()

    @pl.when(step == last)
    def _():
        o_out[...] = o_all[...]
        rows_copy(o_all, o_peer, QB, sems, last).start()

        def finish(i, carry):
            copy = rows_copy(o_all, o_peer, QB, sems, i)
            copy.wait()
            return carry

        lax.fori_loop(0, last + 1, finish, 0)
        handed.wait()
        w_out[...] = w_got[...]
        peer_out[...] = o_peer[...]


def whole(a):
    return pl.BlockSpec(a.shape, lambda i: (0,) * len(a.shape))


def same(*shape):
    return pl.BlockSpec(shape, lambda i: (0,) * len(shape))


def cols(n):
    return pl.BlockSpec((n, QB), lambda i: (0, i))


def two_sems(n):
    return [pltpu.SemaphoreType.DMA((n,)), pltpu.SemaphoreType.DMA((n,))]


def attn_fwd(w_own, tok, gain, shift, wt, qb_col, vb_col, vb_row, khot, qhott, table, kwin, qwin):
    rows, model = tok.shape
    width = wt.shape[0] // 3
    heads = width // HEAD_DIM
    ext = rows + 2 * HALO
    shape = jax.ShapeDtypeStruct
    return pl.pallas_call(
        partial(attn_fwd_kernel, heads // GROUP),
        grid=(rows // QB,),
        in_specs=[pl.BlockSpec(memory_space=pltpu.VMEM)]
        + [whole(x) for x in (tok, gain, shift, wt, qb_col, vb_col, vb_row, khot)]
        + [cols(CP), whole(table), whole(kwin), cols(1)],
        out_specs=[
            same(rows, model), same(width, rows), same(ext, width), same(width, ext), same(ext, width),
            same(rows, width), same(rows, width), same(width, model), cols(heads),
        ],
        out_shape=[
            shape((rows, model), BF16), shape((width, rows), BF16), shape((ext, width), BF16),
            shape((width, ext), BF16), shape((ext, width), BF16), shape((rows, width), BF16),
            shape((rows, width), BF16), shape((width, model), BF16), shape((heads, rows), F32),
        ],
        scratch_shapes=[
            pltpu.VMEM((ext, model), BF16), pltpu.VMEM((width, ext), BF16),
            pltpu.VMEM((rows, width), BF16), pltpu.VMEM((rows, width), BF16),
            pltpu.VMEM((width, model), BF16),
        ] + two_sems(rows // QB + 2),
        compiler_params=pltpu.CompilerParams(collective_id=0, has_side_effects=True),
        name="attn_fwd",
    )(w_own, tok, gain, shift, wt, qb_col, vb_col, vb_row, khot, qhott, table, kwin, qwin)


def ffn_kernel(
    tok, o_own, o_peer, w_own, w_peer, bo, gain, shift, w_in, b_in, w_back, bb, cot,
    keep, give, gr, dot_t, g_out, g_in, g_back, vec, vec_in,
    n_s, r_s, h_s, z_s, du_s, gh_s, gh_p, g_acc, wide_a, wide_b, send_sem, recv_sem,
):
    rows_all, model = tok.shape
    half = keep.shape[1]
    chunks = rows_all // CHUNK
    sems = (send_sem, recv_sem)
    me = lax.axis_index("mp")
    own = half_lanes(me, half)
    other = half_lanes(1 - me, half)
    greet()
    vec[...] = jnp.zeros_like(vec)
    vec_in[...] = jnp.zeros_like(vec_in)

    def forward(c, carry):
        at = pl.ds(pl.multiple_of(c * CHUNK, CHUNK), CHUNK)
        x1 = tok[at, :].astype(F32) + dot(o_own[at, :], w_own[...]) + dot(o_peer[at, :], w_peer[...])
        x1 = x1 + bo[...]
        center = x1 - jnp.mean(x1, axis=-1, keepdims=True)
        r = lax.rsqrt(jnp.mean(center * center, axis=-1, keepdims=True) + EPS)
        n = center * r
        h = (n * gain[...] + shift[...]).astype(BF16)
        wide_b[...] = x1
        n_s[at, :] = n
        r_s[at, :] = r
        h_s[at, :] = h
        u = dot(h, w_in[...]) + b_in[...]
        cdf = 0.5 * (1.0 + lax.erf(u * (0.5**0.5)))
        slope = cdf + u * (jnp.exp(-0.5 * u * u) * 0.3989422804014327)
        z = (u * cdf).astype(BF16)
        z_s[at, :] = z
        du = (dot_nt(cot[at, :], w_back[...]) * slope).astype(BF16)
        du_s[at, :] = du
        gh_s[at, :] = dot_nt(du, w_in[...]).astype(BF16)
        vec_in[...] += jnp.sum(du.astype(F32), axis=0, keepdims=True)
        keep[at, :] = wide_b[:, own] + bb[:, own]
        rows_copy(gh_s, gh_p, CHUNK, sems, c).start()
        return carry

    lax.fori_loop(0, chunks, forward, 0)

    def output(c, carry):
        at = pl.ds(pl.multiple_of(c * CHUNK, CHUNK), CHUNK)
        wide_a[...] = dot(z_s[at, :], w_back[...])
        keep[at, :] += wide_a[:, own]
        give[at, :] = wide_a[:, other].astype(BF16)
        return carry

    lax.fori_loop(0, chunks, output, 0)
    g_acc[...] = jnp.zeros_like(g_acc)

    def back_block(i, carry):
        at = pl.ds(pl.multiple_of(i * CHUNK, CHUNK), CHUNK)
        g_back[at, :] = dot_tn(z_s[:, at], cot[...]).astype(BF16)
        return carry

    lax.fori_loop(0, z_s.shape[1] // CHUNK, back_block, 0)

    def in_block(i, carry):
        at = pl.ds(pl.multiple_of(i * CHUNK, CHUNK), CHUNK)
        g_in[at, :] = dot_tn(h_s[:, at], du_s[...]).astype(BF16)
        return carry

    lax.fori_loop(0, model // CHUNK, in_block, 0)

    def backward(c, carry):
        at = pl.ds(pl.multiple_of(c * CHUNK, CHUNK), CHUNK)
        rows_copy(gh_s, gh_p, CHUNK, sems, c).wait()
        gh = gh_s[at, :].astype(F32) + gh_p[at, :].astype(F32)
        n = n_s[at, :]
        e = gh * gain[...]
        gy = cot[at, :].astype(F32)
        mean_e = jnp.mean(e, axis=-1, keepdims=True)
        mean_n = jnp.mean(e * n, axis=-1, keepdims=True)
        gx1 = gy + r_s[at, :] * (e - mean_e - n * mean_n)
        wide_a[...] = gx1
        go = gx1.astype(BF16)
        g_acc[...] += dot_tn(o_own[at, :], go)
        dot_t[:, at] = dot_nt(w_own[...], go).astype(BF16)
        vec[0:1, :] += jnp.sum(gh * n, axis=0, keepdims=True)
        vec[1:2, :] += jnp.sum(gh, axis=0, keepdims=True)
        vec[2:3, :] += jnp.sum(go.astype(F32), axis=0, keepdims=True)
        vec[3:4, :] += jnp.sum(gy, axis=0, keepdims=True)
        gr[at, :] = wide_a[:, own]
        return carry

    lax.fori_loop(0, chunks, backward, 0)
    g_out[...] = g_acc[...].astype(BF16)


def ffn(tok, o_own, o_peer, w_own, w_peer, bo, gain, shift, w_in, b_in, w_back, bb, cot):
    rows, model = tok.shape
    width = o_own.shape[1]
    hidden = w_in.shape[1]
    half = model // 2
    shape = jax.ShapeDtypeStruct
    vm = pltpu.VMEM
    return pl.pallas_call(
        ffn_kernel,
        in_specs=[pl.BlockSpec(memory_space=pltpu.VMEM)] * 13,
        out_specs=[pl.BlockSpec(memory_space=pltpu.VMEM)] * 9,
        out_shape=[
            shape((rows, half), F32), shape((rows, half), BF16), shape((rows, half), F32),
            shape((width, rows), BF16), shape((width, model), BF16), shape((model, hidden), BF16),
            shape((hidden, model), BF16), shape((8, model), F32), shape((1, hidden), F32),
        ],
        scratch_shapes=[
            vm((rows, model), F32), vm((rows, 1), F32), vm((rows, model), BF16), vm((rows, hidden), BF16),
            vm((rows, hidden), BF16), vm((rows, model), BF16), vm((rows, model), BF16),
            vm((width, model), F32), vm((CHUNK, model), F32), vm((CHUNK, model), F32),
        ] + two_sems(rows // CHUNK),
        compiler_params=pltpu.CompilerParams(collective_id=1, has_side_effects=True),
        name="ffn",
    )(tok, o_own, o_peer, w_own, w_peer, bo, gain, shift, w_in, b_in, w_back, bb, cot)


def attn_bwd_kernel(
    groups, keep, give, qt, kx, kt, vx, dot_t, khot, khott, qhott, qhot, table, kwin, qwin, lse,
    out, dq, dk, dv, gcell, dk_acc, dv_acc, got, send_sem, recv_sem,
):
    step = pl.program_id(0)
    rows_all = dk.shape[0]
    swap = to_peer(give, got, send_sem.at[0], recv_sem.at[0])

    @pl.when(step == 0)
    def _():
        greet()
        swap.start()
        dk_acc[...] = jnp.zeros_like(dk_acc)
        dv_acc[...] = jnp.zeros_like(dv_acc)
        gcell[...] = jnp.zeros_like(gcell)

    start = pl.multiple_of(step * QB, QB)
    span = pl.ds(start, SPAN)
    mask = jnp.where(kwin[span, :] == qwin[...], 0.0, NEG)
    hot = khot[span, :]
    hot_t = khott[:, span]
    cells = qhott[...]
    cells_r = qhot[...]
    for g in range(groups):
        lanes = slice(128 * g, 128 * (g + 1))
        q_stack = stack_heads(qt[lanes, :])
        do_stack = stack_heads(dot_t[lanes, :])
        right = jnp.concatenate([q_stack, bias_rows(table, g, cells)], axis=0)
        scores = dot(jnp.concatenate([kx[span, lanes], hot], axis=1), right)
        dprob = dot(vx[span, lanes], do_stack)
        ps, dss, dqs = [], [], []
        for j in range(GROUP):
            h = GROUP * g + j
            cut = slice(QB * j, QB * (j + 1))
            p = jnp.exp(scores[:, cut] * SCALE + mask - lse[h : h + 1, :])
            t = p * dprob[:, cut]
            inner = jnp.sum(t, axis=0, keepdims=True)
            ds = (t - p * inner).astype(BF16)
            ps.append(p.astype(BF16))
            dss.append(ds)
            both = dot(jnp.concatenate([kt[HEAD_DIM * h : HEAD_DIM * (h + 1), span], hot_t], axis=0), ds)
            dqs.append(both[:HEAD_DIM])
            gcell[CP * h : CP * (h + 1), :] += dot(both[HEAD_DIM:].astype(BF16), cells_r)
        dq[:, lanes] = (jnp.concatenate(dqs, axis=0) * SCALE).T.astype(BF16)
        dk_acc[span, lanes] += dot_nt(jnp.concatenate(dss, axis=1), q_stack)
        dv_acc[span, lanes] += dot_nt(jnp.concatenate(ps, axis=1), do_stack)

    @pl.when(step == rows_all // QB - 1)
    def _():
        inner_rows = pl.ds(HALO, rows_all)
        dk[...] = (dk_acc[inner_rows, :] * SCALE).astype(BF16)
        dv[...] = dv_acc[inner_rows, :].astype(BF16)
        swap.wait()
        out[...] = (keep[...] + got[...].astype(F32)).astype(BF16)


def attn_bwd(keep, give, qt, kx, kt, vx, dot_t, khot, khott, qhott, qhot, table, kwin, qwin, lse):
    width, rows = qt.shape
    heads = width // HEAD_DIM
    ext = rows + 2 * HALO
    half = keep.shape[1]
    shape = jax.ShapeDtypeStruct
    rblk = lambda n: pl.BlockSpec((QB, n), lambda i: (i, 0))
    return pl.pallas_call(
        partial(attn_bwd_kernel, heads // GROUP),
        grid=(rows // QB,),
        in_specs=[
            whole(keep), pl.BlockSpec(memory_space=pltpu.VMEM),
            cols(width), whole(kx), whole(kt), whole(vx), cols(width), whole(khot), whole(khott),
            cols(CP), rblk(CP), whole(table), whole(kwin), cols(1), cols(heads),
        ],
        out_specs=[
            same(rows, half), rblk(width), same(rows, width), same(rows, width), same(CP * heads, CP),
        ],
        out_shape=[
            shape((rows, half), BF16), shape((rows, width), BF16), shape((rows, width), BF16),
            shape((rows, width), BF16), shape((CP * heads, CP), F32),
        ],
        scratch_shapes=[
            pltpu.VMEM((ext, width), F32), pltpu.VMEM((ext, width), F32), pltpu.VMEM((rows, half), BF16),
        ] + two_sems(1),
        compiler_params=pltpu.CompilerParams(collective_id=2, has_side_effects=True),
        name="attn_bwd",
    )(keep, give, qt, kx, kt, vx, dot_t, khot, khott, qhott, qhot, table, kwin, qwin, lse)


def close_kernel(
    tok, a, dq, dk, dv, wt, gain, gr, vec2, vec_in, table, out, late,
    ga_s, give, got, stat, stat_p, wide, vec_s, vec_p, send_sem, recv_sem,
):
    rows_all, model = tok.shape
    width = dq.shape[1]
    half = out.shape[1]
    chunks = rows_all // CHUNK
    me = lax.axis_index("mp")
    own = half_lanes(me, half)
    other = half_lanes(1 - me, half)
    greet()
    vec_s[...] = jnp.zeros_like(vec_s)
    main = lambda c: rows_copy(give, got, CHUNK, (send_sem.at[0], recv_sem.at[0]), c)
    side = lambda c: rows_copy(stat, stat_p, CHUNK, (send_sem.at[1], recv_sem.at[1]), c)
    lane = lax.broadcasted_iota(jnp.int32, (CHUNK, 128), 1)

    def norms(at):
        x = tok[at, :].astype(F32)
        center = x - jnp.mean(x, axis=-1, keepdims=True)
        r = lax.rsqrt(jnp.mean(center * center, axis=-1, keepdims=True) + EPS)
        return center * r, r

    def forward(c, carry):
        at = pl.ds(pl.multiple_of(c * CHUNK, CHUNK), CHUNK)
        ga = dot(dq[at, :], wt[:width, :]) + dot(dk[at, :], wt[width : 2 * width, :])
        ga = ga + dot(dv[at, :], wt[2 * width :, :])
        wide[...] = ga
        give[at, :] = wide[:, other].astype(BF16)
        ga_s[at, :] = wide[:, own]
        n, r = norms(at)
        e = ga * gain[...]
        first = jnp.mean(e, axis=-1, keepdims=True)
        second = jnp.mean(e * n, axis=-1, keepdims=True)
        stat[at, :] = jnp.where(lane == 0, first, jnp.where(lane == 1, second, 0.0))
        vec_s[0:1, :] += jnp.sum(ga * n, axis=0, keepdims=True)
        vec_s[1:2, :] += jnp.sum(ga, axis=0, keepdims=True)
        main(c).start()
        side(c).start()
        return carry

    lax.fori_loop(0, chunks, forward, 0)
    vectors = to_peer(vec_s, vec_p, send_sem.at[2, 0], recv_sem.at[2, 0])
    grads = jnp.concatenate([dq[...], dk[...], dv[...]], axis=1)
    for b in range(2):
        block = dot_tn(a[:, width * b : width * (b + 1)], grads).astype(BF16)
        for c in range(3):
            k = 2 * c + b
            goal = (width * (k % 3), width * (k // 3))
            late[goal[0] : goal[0] + width, goal[1] : goal[1] + width] = block[:, width * c : width * (c + 1)]
    vectors.start()
    qv = [jnp.sum(item[...].astype(F32), axis=0, keepdims=True) for item in (dq, dv)]

    def backward(c, carry):
        at = pl.ds(pl.multiple_of(c * CHUNK, CHUNK), CHUNK)
        main(c).wait()
        side(c).wait()
        sums = stat[at, :] + stat_p[at, :]
        n, r = norms(at)
        wide[...] = n
        e = (ga_s[at, :] + got[at, :].astype(F32)) * gain[:, own]
        gx = gr[at, :] + r * (e - sums[:, 0:1] - wide[:, own] * sums[:, 1:2])
        out[at, :] = gx.astype(BF16)
        return carry

    lax.fori_loop(0, chunks, backward, 0)
    vectors.wait()
    first = vec_s[0:2, :] + vec_p[0:2, :]
    parts = [first[0:1], first[1:2]] + [vec2[k : k + 1, :] for k in range(4)]
    parts.append(jnp.concatenate(qv, axis=1))
    parts += [vec_in[:, model * k : model * (k + 1)] for k in range(vec_in.shape[1] // model)]
    parts += [table[k : k + 1, :] for k in range(table.shape[0])]
    parts.append(jnp.zeros((SMALL - len(parts), model), F32))
    late[3 * width : 3 * width + SMALL, :] = jnp.concatenate(parts, axis=0).astype(BF16)
    spare = late.shape[0] - 3 * width - SMALL
    late[3 * width + SMALL :, :] = jnp.zeros((spare, model), BF16)


def close(late_rows, tok, a, dq, dk, dv, wt, gain, gr, vec2, vec_in, table):
    rows, model = tok.shape
    width = dq.shape[1]
    half = gr.shape[1]
    chunks = rows // CHUNK
    shape = jax.ShapeDtypeStruct
    vm = pltpu.VMEM
    sems = pltpu.SemaphoreType.DMA((3, chunks))
    return pl.pallas_call(
        close_kernel,
        in_specs=[pl.BlockSpec(memory_space=pltpu.VMEM)] * 11,
        out_specs=[pl.BlockSpec(memory_space=pltpu.VMEM)] * 2,
        out_shape=[shape((rows, half), BF16), shape((late_rows, model), BF16)],
        scratch_shapes=[
            vm((rows, half), F32), vm((rows, half), BF16), vm((rows, half), BF16), vm((rows, 128), F32),
            vm((rows, 128), F32), vm((CHUNK, model), F32), vm((8, model), F32), vm((8, model), F32),
            sems, sems,
        ],
        compiler_params=pltpu.CompilerParams(collective_id=3, has_side_effects=True),
        name="close",
    )(tok, a, dq, dk, dv, wt, gain, gr, vec2, vec_in, table)


def dp_copy(src, dst, partner, send_sem, recv_sem):
    return pltpu.make_async_remote_copy(
        src_ref=src,
        dst_ref=dst,
        send_sem=send_sem,
        recv_sem=recv_sem,
        device_id={"dp": partner},
        device_id_type=MESH,
    )


def dp_sum_kernel(orders, x, big, small, out, acc, got, send_sem, recv_sem):
    rows, wide = x.shape
    part = wide // len(orders)
    steps = len(orders[0])
    place = lax.axis_index("dp")

    def bit_of(b):
        return lax.rem(lax.div(place, 1 << b), 2)

    def partner_of(b):
        return place + (1 - 2 * bit_of(b)) * (1 << b)

    barrier = pltpu.get_barrier_semaphore()
    for b in range(steps):
        pl.semaphore_signal(barrier, inc=1, device_id={"dp": partner_of(b)}, device_id_type=MESH)
    pl.semaphore_wait(barrier, steps)

    state = [(x, 0)] * len(orders)
    kept = [[] for _ in orders]
    for s in range(steps):
        size = rows >> (s + 1)
        base = rows - (rows >> s)
        copies = []
        for k, order in enumerate(orders):
            src, low = state[k]
            lanes = pl.ds(part * k, part)
            bit = bit_of(order[s])
            mine = pl.multiple_of(low + bit * size, 16)
            theirs = pl.multiple_of(low + (1 - bit) * size, 16)
            copy = dp_copy(
                src.at[pl.ds(theirs, size), lanes],
                got.at[pl.ds(base, size), lanes],
                partner_of(order[s]),
                send_sem.at[k, s],
                recv_sem.at[k, s],
            )
            copy.start()
            copies.append(copy)
            kept[k].append(low)
            state[k] = (src, mine)
        for k, order in enumerate(orders):
            src, mine = state[k]
            lanes = slice(part * k, part * (k + 1))
            copies[k].wait()
            total = src[pl.ds(mine, size), lanes].astype(F32) + got[base : base + size, lanes].astype(F32)
            goal = out if s == steps - 1 else acc
            goal[pl.ds(mine, size), lanes] = total.astype(BF16)
            state[k] = (goal, mine)
    for s in reversed(range(steps)):
        size = rows >> (s + 1)
        copies = []
        for k, order in enumerate(orders):
            low = state[k][1]
            lanes = pl.ds(part * k, part)
            region = out.at[pl.ds(pl.multiple_of(low, 16), size), lanes]
            at = 2 * steps - 1 - s
            copy = dp_copy(region, region, partner_of(order[s]), send_sem.at[k, at], recv_sem.at[k, at])
            copy.start()
            copies.append(copy)
            state[k] = (out, kept[k][s])
        for copy in copies:
            copy.wait()
    tall = big.shape[0] // 2
    for k in range(2):
        big[tall * k : tall * (k + 1), :] = out[:tall, big.shape[1] * k : big.shape[1] * (k + 1)]
    small[...] = out[tall : tall + small.shape[0], :].astype(F32)


def dp_sum(ranks, big_shape, x):
    rows, wide = x.shape
    steps = ranks.bit_length() - 1
    orders = [list(range(steps)), [0] + list(range(2, steps)) + [1]]
    vm = pltpu.VMEM
    sems = pltpu.SemaphoreType.DMA((2, 2 * steps))
    return pl.pallas_call(
        partial(dp_sum_kernel, orders),
        in_specs=[pl.BlockSpec(memory_space=pltpu.VMEM)],
        out_specs=[pl.BlockSpec(memory_space=pltpu.VMEM)] * 2,
        out_shape=[jax.ShapeDtypeStruct(big_shape, BF16), jax.ShapeDtypeStruct((SMALL, wide), F32)],
        scratch_shapes=[vm((rows, wide), BF16)] * 3 + [sems, sems],
        compiler_params=pltpu.CompilerParams(collective_id=4, has_side_effects=True),
        name="dp_sum",
    )(x)


def window_data(crop_counts, crop_patches, rel_index, rel_table, rows):
    highest = lax.Precision.HIGHEST
    heads = rel_table.shape[1]
    cells, wins = layout(crop_counts, crop_patches, rows)
    kcells = jnp.pad(cells, (HALO, HALO))
    kwin = jnp.pad(wins, (HALO, HALO), constant_values=-1)[:, None]
    span_cells = jnp.arange(CP, dtype=jnp.int32)
    wide_cells = jnp.arange(2 * CP, dtype=jnp.int32) % CP
    khot = (kcells[:, None] == wide_cells[None, :]).astype(BF16)
    khott = (span_cells[:, None] == kcells[None, :]).astype(BF16)
    qhott = (span_cells[:, None] == cells[None, :]).astype(BF16)
    qhot = (cells[:, None] == span_cells[None, :]).astype(BF16)
    rel_t = jnp.pad(rel_index.T, ((0, CP - CELLS), (0, CP - CELLS)), constant_values=-1).reshape(-1)
    offset_hot = (rel_t[:, None] == jnp.arange(OFFSETS, dtype=jnp.int32)[None, :]).astype(F32)
    bias = jnp.einsum("pm,mh->hp", offset_hot, rel_table, precision=highest) / SCALE
    high = bias.astype(BF16)
    rest = (bias - high.astype(F32)).astype(BF16)
    table = jnp.stack([high.reshape(heads, CP, CP), rest.reshape(heads, CP, CP)], axis=1)
    return (khot, khott, qhott, qhot, table.reshape(heads * 2 * CP, CP), kwin, wins[None, :], offset_hot)


def body(
    tokens,
    crop_counts,
    crop_patches,
    rel_index,
    ln1_gain,
    ln1_shift,
    w_qkv,
    qv_bias,
    rel_table,
    w_out,
    b_out,
    ln2_gain,
    ln2_shift,
    w_in,
    b_in,
    w_back,
    b_back,
    cotangent,
):
    highest = lax.Precision.HIGHEST
    rows, part_width = tokens.shape
    model = ln1_gain.shape[0]
    width = w_qkv.shape[2]
    heads = width // HEAD_DIM
    khot, khott, qhott, qhot, table, kwin, qwin, offset_hot = window_data(
        crop_counts, crop_patches, rel_index, rel_table, rows
    )
    whole_in = lax.all_gather(tokens, "mp", axis=1, tiled=True)
    whole_cot = lax.all_gather(cotangent, "mp", axis=1, tiled=True)
    wt = jnp.transpose(w_qkv, (1, 2, 0)).reshape(3 * width, model)
    mixer_in, qt, kx, kt, vx, heads_out, heads_peer, w_peer, lse = attn_fwd(
        w_out,
        whole_in, ln1_gain[None, :], ln1_shift[None, :], wt, qv_bias[0][:, None], qv_bias[1][:, None],
        qv_bias[1][None, :], khot, qhott, table, kwin, qwin,
    )
    keep, give, gr, dot_t, grad_w_out, grad_w_in, grad_w_back, vec2, grad_b_in = ffn(
        whole_in, heads_out, heads_peer, w_out, w_peer, b_out[None, :], ln2_gain[None, :], ln2_shift[None, :],
        w_in, b_in[None, :], w_back, b_back[None, :], whole_cot,
    )
    early = lax.psum((grad_w_in, grad_w_back, grad_w_out), "dp")
    out_half, grad_query, grad_key, grad_value, gcell = attn_bwd(
        keep, give, qt, kx, kt, vx, dot_t, khot, khott, qhott, qhot, table, kwin, qwin, lse
    )
    grad_table = jnp.einsum(
        "pm,hp->mh", offset_hot, gcell.reshape(heads, CP * CP), precision=highest
    )
    table_rows = -(-grad_table.size // model)
    table_flat = jnp.pad(grad_table.reshape(-1), (0, table_rows * model - grad_table.size))
    ranks = lax.axis_size("dp")
    late_rows = -(-(3 * width + SMALL) // (16 * ranks)) * 16 * ranks
    grad_half, late = close(
        late_rows, whole_in, mixer_in, grad_query, grad_key, grad_value, wt, ln1_gain[None, :], gr,
        vec2, grad_b_in, table_flat.reshape(table_rows, model),
    )
    big, small = dp_sum(ranks, (3 * model, width), late)
    early, big = lax.optimization_barrier((early, big))
    grad_w_in, grad_w_back, grad_w_out = (item.astype(F32) for item in early)
    grad_w_qkv = jnp.transpose(big.astype(F32).reshape(3, model, width), (1, 0, 2))
    grad_g1, grad_c1, grad_g2, grad_c2, grad_b_out, grad_b_back = (small[k] for k in range(6))
    grad_qv_bias = small[6].reshape(2, width)
    hidden_rows = w_in.shape[1] // model
    grad_b_in = small[7 : 7 + hidden_rows].reshape(-1)
    flat = small[7 + hidden_rows : 7 + hidden_rows + table_rows].reshape(-1)
    grad_table = flat[: grad_table.size].reshape(grad_table.shape)
    return (
        out_half,
        grad_half,
        grad_g1,
        grad_c1,
        grad_w_qkv,
        grad_qv_bias,
        grad_table,
        grad_w_out,
        grad_b_out,
        grad_g2,
        grad_c2,
        grad_w_in,
        grad_b_in,
        grad_w_back,
        grad_b_back,
    )


def solution(mesh):
    return jax.shard_map(
        body,
        mesh=mesh,
        in_specs=(
            P("dp", "mp"),
            P("dp"),
            P("dp", None),
            P(),
            P(),
            P(),
            P(None, None, "mp"),
            P(None, "mp"),
            P(None, "mp"),
            P("mp", None),
            P(),
            P(),
            P(),
            P(None, "mp"),
            P("mp"),
            P("mp", None),
            P(),
            P("dp", "mp"),
        ),
        out_specs=(
            P("dp", "mp"),
            P("dp", "mp"),
            P(),
            P(),
            P(None, None, "mp"),
            P(None, "mp"),
            P(None, "mp"),
            P("mp", None),
            P(),
            P(),
            P(),
            P(None, "mp"),
            P("mp"),
            P("mp", None),
            P(),
        ),
        check_vma=False,
    )
```

```python
from functools import partial

import jax
import jax.numpy as jnp
from jax import lax
from jax.experimental import pallas as pl
from jax.experimental.pallas import tpu as pltpu
from jax.sharding import PartitionSpec as P

HEAD_DIM = 32
SIDE = 7
LOCAL_SIDE = 3
CELLS = 49
OFFSETS = 169
CROP_MAX = 8
QB = 128
HALO = 64
SPAN = QB + 2 * HALO
CP = 64
GROUP = 4
SCALE = HEAD_DIM ** (-0.5)
EPS = 1e-05
NEG = -1e30
BLOCK = 256
FFN_ROWS = 128
CLOSE_ROWS = 128
SMALL = 16
MESH = pl.DeviceIdType.MESH
F32 = jnp.float32
BF16 = jnp.bfloat16


def layout(counts, patches, row_count):
    live_crop = jnp.arange(CROP_MAX, dtype=jnp.int32)[None, :] < counts[:, None]
    crop_rows = jnp.where(live_crop, patches, 0).reshape(-1)
    crop_ends = jnp.cumsum(crop_rows)
    used_rows = crop_ends[-1]
    row_ids = jnp.arange(row_count, dtype=jnp.int32)
    passed = crop_ends[None, :] <= row_ids[:, None]
    window = jnp.sum(passed.astype(jnp.int32), axis=1)
    starts = jnp.max(jnp.where(passed, crop_ends[None, :], 0), axis=1)
    finish = jnp.min(jnp.where(passed, row_count + used_rows + 1, crop_ends[None, :]), axis=1)
    length = finish - starts
    offset = row_ids - starts
    grid_side = jnp.where(length >= CELLS, SIDE, LOCAL_SIDE).astype(jnp.int32)
    cell_index = offset // grid_side * SIDE + offset % grid_side
    inside = row_ids < used_rows
    cell_ids = jnp.where(inside, cell_index, 0)
    windows = jnp.where(inside, window, crop_rows.shape[0] + row_ids - used_rows)
    return (cell_ids, windows)


def layer_norm(values, gain, shift):
    center = values - jnp.mean(values, axis=-1, keepdims=True)
    spread = jnp.mean(center * center, axis=-1, keepdims=True)
    return center * lax.rsqrt(spread + EPS) * gain + shift


def dot(a, b):
    return jnp.dot(a, b, preferred_element_type=F32)


def dot_nt(a, b):
    return lax.dot_general(a, b, (((1,), (1,)), ((), ())), preferred_element_type=F32)


def stack_heads(rows_t):
    cols = []
    for j in range(GROUP):
        parts = []
        if j > 0:
            parts.append(jnp.zeros((HEAD_DIM * j, QB), BF16))
        parts.append(rows_t[HEAD_DIM * j : HEAD_DIM * (j + 1)])
        if j < GROUP - 1:
            parts.append(jnp.zeros((HEAD_DIM * (GROUP - 1 - j), QB), BF16))
        cols.append(jnp.concatenate(parts, axis=0))
    return jnp.concatenate(cols, axis=1)


def bias_rows(table, g, cells):
    tall = dot(table[2 * CP * GROUP * g : 2 * CP * GROUP * (g + 1), :], cells).astype(BF16)
    return jnp.concatenate([tall[2 * CP * j : 2 * CP * (j + 1)] for j in range(GROUP)], axis=1)


def dot_tn(a, b):
    return lax.dot_general(a, b, (((0,), (0,)), ((), ())), preferred_element_type=F32)


def peer_of():
    return 1 - lax.axis_index("mp")


def greet():
    barrier = pltpu.get_barrier_semaphore()
    pl.semaphore_signal(barrier, inc=1, device_id={"mp": peer_of()}, device_id_type=MESH)
    pl.semaphore_wait(barrier, 1)


def to_peer(src, dst, send_sem, recv_sem):
    return pltpu.make_async_remote_copy(
        src_ref=src,
        dst_ref=dst,
        send_sem=send_sem,
        recv_sem=recv_sem,
        device_id={"mp": peer_of()},
        device_id_type=MESH,
    )


def rows_copy(src, dst, size, sems, i):
    at = pl.ds(pl.multiple_of(i * size, size), size)
    return to_peer(src.at[at], dst.at[at], sems[0].at[i], sems[1].at[i])


def half_lanes(index, half):
    return pl.ds(pl.multiple_of(index * half, 128), half)


def attn_fwd_kernel(
    groups, w_own, cot_own, tok, gain, shift, wt, qb_col, vb_col, vb_row, khot, qhott, table, kwin, qwin,
    a_out, qt, kx, kt, vx, o_out, peer_out, w_out, cot, lse,
    a_pad, vt, o_all, o_peer, w_got, cot_got, send_sem, recv_sem,
):
    step = pl.program_id(0)
    last = tok.shape[0] // QB - 1
    rows_all = tok.shape[0]
    width = qt.shape[0]
    sems = (send_sem, recv_sem)
    place = lax.axis_index("dp")
    core = lax.rem(place, 2)
    mate = place + 1 - 2 * core
    fetched = w_own.shape[0] // 2
    part = pl.ds(pl.multiple_of(core * fetched, 16), fetched)
    weight = to_peer(w_own.at[part], w_got.at[part], send_sem.at[last + 1], recv_sem.at[last + 1])
    swap = to_peer(cot_own, cot_got, send_sem.at[last + 3], recv_sem.at[last + 3])
    handed = dp_copy(w_got.at[part], w_got.at[part], mate, send_sem.at[last + 2], recv_sem.at[last + 2])

    @pl.when(step == 0)
    def _():
        barrier = pltpu.get_barrier_semaphore()
        pl.semaphore_signal(barrier, inc=1, device_id={"mp": peer_of()}, device_id_type=MESH)
        pl.semaphore_signal(barrier, inc=1, device_id={"dp": mate}, device_id_type=MESH)
        pl.semaphore_wait(barrier, 2)
        weight.start()
        swap.start()
        zero = jnp.zeros((HALO, tok.shape[1]), BF16)
        a_pad[:HALO, :] = zero
        a_pad[HALO + rows_all :, :] = zero

        def norm_rows(i, carry):
            at = pl.multiple_of(i * QB, QB)
            a = layer_norm(tok[pl.ds(at, QB), :].astype(F32), gain[...], shift[...]).astype(BF16)
            a_out[pl.ds(at, QB), :] = a
            a_pad[pl.ds(pl.multiple_of(at + HALO, HALO), QB), :] = a
            return carry

        lax.fori_loop(0, rows_all // QB, norm_rows, 0)
        a_all = a_pad[...]
        wk = wt[width : 2 * width, :]
        wv = wt[2 * width :, :]
        qt[...] = (dot_nt(wt[:width, :], a_out[...]) + qb_col[...]).astype(BF16)
        kx[...] = dot_nt(a_all, wk).astype(BF16)
        kt[...] = dot_nt(wk, a_all).astype(BF16)
        vx[...] = (dot_nt(a_all, wv) + vb_row[...]).astype(BF16)
        vt[...] = (dot_nt(wv, a_all) + vb_col[...]).astype(BF16)

    start = pl.multiple_of(step * QB, QB)
    span = pl.ds(start, SPAN)
    mask = jnp.where(kwin[span, :] == qwin[...], 0.0, NEG)
    hot = khot[span, :]
    cells = qhott[...]
    for g in range(groups):
        lanes = slice(128 * g, 128 * (g + 1))
        right = jnp.concatenate(
            [stack_heads(qt[lanes, pl.ds(start, QB)]), bias_rows(table, g, cells)], axis=0
        )
        scores = dot(jnp.concatenate([kx[span, lanes], hot], axis=1), right)
        outs = []
        for j in range(GROUP):
            h = GROUP * g + j
            s = scores[:, QB * j : QB * (j + 1)] * SCALE + mask
            peak = jnp.max(s, axis=0, keepdims=True)
            e = jnp.exp(s - peak)
            mass = jnp.sum(e, axis=0, keepdims=True)
            outs.append(dot(vt[HEAD_DIM * h : HEAD_DIM * (h + 1), span], e.astype(BF16)) / mass)
            lse[h : h + 1, :] = peak + jnp.log(mass)
        o_all[pl.ds(start, QB), lanes] = jnp.concatenate(outs, axis=0).T.astype(BF16)

    @pl.when(step > 0)
    def _():
        rows_copy(o_all, o_peer, QB, sems, step - 1).start()

    @pl.when(step == last - 2)
    def _():
        weight.wait()
        handed.start()

    @pl.when(step == last)
    def _():
        o_out[...] = o_all[...]
        half = cot_own.shape[1]
        me = lax.axis_index("mp")
        cot[:, half_lanes(me, half)] = cot_own[...]
        swap.wait()
        cot[:, half_lanes(1 - me, half)] = cot_got[...]
        rows_copy(o_all, o_peer, QB, sems, last).start()

        def finish(i, carry):
            copy = rows_copy(o_all, o_peer, QB, sems, i)
            copy.wait()
            return carry

        lax.fori_loop(0, last + 1, finish, 0)
        handed.wait()
        w_out[...] = w_got[...]
        peer_out[...] = o_peer[...]


def whole(a):
    return pl.BlockSpec(a.shape, lambda i: (0,) * len(a.shape))


def same(*shape):
    return pl.BlockSpec(shape, lambda i: (0,) * len(shape))


def cols(n):
    return pl.BlockSpec((n, QB), lambda i: (0, i))


def two_sems(n):
    return [pltpu.SemaphoreType.DMA((n,)), pltpu.SemaphoreType.DMA((n,))]


def attn_fwd(w_own, cot_own, tok, gain, shift, wt, qb_col, vb_col, vb_row, khot, qhott, table, kwin, qwin):
    rows, model = tok.shape
    width = wt.shape[0] // 3
    heads = width // HEAD_DIM
    ext = rows + 2 * HALO
    shape = jax.ShapeDtypeStruct
    return pl.pallas_call(
        partial(attn_fwd_kernel, heads // GROUP),
        grid=(rows // QB,),
        in_specs=[pl.BlockSpec(memory_space=pltpu.VMEM)] * 2
        + [whole(x) for x in (tok, gain, shift, wt, qb_col, vb_col, vb_row, khot)]
        + [cols(CP), whole(table), whole(kwin), cols(1)],
        out_specs=[
            same(rows, model), same(width, rows), same(ext, width), same(width, ext), same(ext, width),
            same(rows, width), same(rows, width), same(width, model), same(rows, model),
            cols(heads),
        ],
        out_shape=[
            shape((rows, model), BF16), shape((width, rows), BF16), shape((ext, width), BF16),
            shape((width, ext), BF16), shape((ext, width), BF16), shape((rows, width), BF16),
            shape((rows, width), BF16), shape((width, model), BF16), shape((rows, model), BF16),
            shape((heads, rows), F32),
        ],
        scratch_shapes=[
            pltpu.VMEM((ext, model), BF16), pltpu.VMEM((width, ext), BF16),
            pltpu.VMEM((rows, width), BF16), pltpu.VMEM((rows, width), BF16),
            pltpu.VMEM((width, model), BF16), pltpu.VMEM(cot_own.shape, BF16),
        ] + two_sems(rows // QB + 3),
        compiler_params=pltpu.CompilerParams(collective_id=0, has_side_effects=True),
        name="attn_fwd",
    )(w_own, cot_own, tok, gain, shift, wt, qb_col, vb_col, vb_row, khot, qhott, table, kwin, qwin)


def ffn_kernel(
    tok, o_own, o_peer, w_own, w_peer, bo, gain, shift, w_in, b_in, w_back, bb, cot,
    keep, give, gr, dot_t, g_out, g_in, g_back, vec, vec_in,
    n_s, r_s, h_s, z_s, du_s, gh_s, gh_p, g_acc, wide_a, wide_b, send_sem, recv_sem,
):
    rows_all, model = tok.shape
    half = keep.shape[1]
    chunks = rows_all // FFN_ROWS
    sems = (send_sem, recv_sem)
    me = lax.axis_index("mp")
    own = half_lanes(me, half)
    other = half_lanes(1 - me, half)
    greet()
    vec[...] = jnp.zeros_like(vec)
    vec_in[...] = jnp.zeros_like(vec_in)

    def forward(c, carry):
        at = pl.ds(pl.multiple_of(c * FFN_ROWS, FFN_ROWS), FFN_ROWS)
        x1 = tok[at, :].astype(F32) + dot(o_own[at, :], w_own[...]) + dot(o_peer[at, :], w_peer[...])
        x1 = x1 + bo[...]
        center = x1 - jnp.mean(x1, axis=-1, keepdims=True)
        r = lax.rsqrt(jnp.mean(center * center, axis=-1, keepdims=True) + EPS)
        n = center * r
        h = (n * gain[...] + shift[...]).astype(BF16)
        wide_b[...] = x1
        n_s[at, :] = n
        r_s[at, :] = r
        h_s[at, :] = h
        u = dot(h, w_in[...]) + b_in[...]
        cdf = 0.5 * (1.0 + lax.erf(u * (0.5**0.5)))
        slope = cdf + u * (jnp.exp(-0.5 * u * u) * 0.3989422804014327)
        z = (u * cdf).astype(BF16)
        z_s[at, :] = z
        du = (dot_nt(cot[at, :], w_back[...]) * slope).astype(BF16)
        du_s[at, :] = du
        gh_s[at, :] = dot_nt(du, w_in[...]).astype(BF16)
        vec_in[...] += jnp.sum(du.astype(F32), axis=0, keepdims=True)
        keep[at, :] = wide_b[:, own] + bb[:, own]
        rows_copy(gh_s, gh_p, FFN_ROWS, sems, c).start()
        return carry

    lax.fori_loop(0, chunks, forward, 0)

    def output(c, carry):
        at = pl.ds(pl.multiple_of(c * FFN_ROWS, FFN_ROWS), FFN_ROWS)
        wide_a[...] = dot(z_s[at, :], w_back[...])
        keep[at, :] += wide_a[:, own]
        give[at, :] = wide_a[:, other].astype(BF16)
        return carry

    lax.fori_loop(0, chunks, output, 0)
    g_acc[...] = jnp.zeros_like(g_acc)

    def back_block(i, carry):
        at = pl.ds(pl.multiple_of(i * BLOCK, BLOCK), BLOCK)
        g_back[at, :] = dot_tn(z_s[:, at], cot[...]).astype(BF16)
        return carry

    lax.fori_loop(0, z_s.shape[1] // BLOCK, back_block, 0)

    def in_block(i, carry):
        at = pl.ds(pl.multiple_of(i * BLOCK, BLOCK), BLOCK)
        g_in[at, :] = dot_tn(h_s[:, at], du_s[...]).astype(BF16)
        return carry

    lax.fori_loop(0, model // BLOCK, in_block, 0)

    def backward(c, carry):
        at = pl.ds(pl.multiple_of(c * FFN_ROWS, FFN_ROWS), FFN_ROWS)
        rows_copy(gh_s, gh_p, FFN_ROWS, sems, c).wait()
        gh = gh_s[at, :].astype(F32) + gh_p[at, :].astype(F32)
        n = n_s[at, :]
        e = gh * gain[...]
        gy = cot[at, :].astype(F32)
        mean_e = jnp.mean(e, axis=-1, keepdims=True)
        mean_n = jnp.mean(e * n, axis=-1, keepdims=True)
        gx1 = gy + r_s[at, :] * (e - mean_e - n * mean_n)
        wide_a[...] = gx1
        go = gx1.astype(BF16)
        g_acc[...] += dot_tn(o_own[at, :], go)
        dot_t[:, at] = dot_nt(w_own[...], go).astype(BF16)
        vec[0:1, :] += jnp.sum(gh * n, axis=0, keepdims=True)
        vec[1:2, :] += jnp.sum(gh, axis=0, keepdims=True)
        vec[2:3, :] += jnp.sum(go.astype(F32), axis=0, keepdims=True)
        vec[3:4, :] += jnp.sum(gy, axis=0, keepdims=True)
        gr[at, :] = wide_a[:, own]
        return carry

    lax.fori_loop(0, chunks, backward, 0)
    g_out[...] = g_acc[...].astype(BF16)


def ffn(tok, o_own, o_peer, w_own, w_peer, bo, gain, shift, w_in, b_in, w_back, bb, cot):
    rows, model = tok.shape
    width = o_own.shape[1]
    hidden = w_in.shape[1]
    half = model // 2
    shape = jax.ShapeDtypeStruct
    vm = pltpu.VMEM
    return pl.pallas_call(
        ffn_kernel,
        in_specs=[pl.BlockSpec(memory_space=pltpu.VMEM)] * 13,
        out_specs=[pl.BlockSpec(memory_space=pltpu.VMEM)] * 9,
        out_shape=[
            shape((rows, half), F32), shape((rows, half), BF16), shape((rows, half), F32),
            shape((width, rows), BF16), shape((width, model), BF16), shape((model, hidden), BF16),
            shape((hidden, model), BF16), shape((8, model), F32), shape((1, hidden), F32),
        ],
        scratch_shapes=[
            vm((rows, model), F32), vm((rows, 1), F32), vm((rows, model), BF16), vm((rows, hidden), BF16),
            vm((rows, hidden), BF16), vm((rows, model), BF16), vm((rows, model), BF16),
            vm((width, model), F32), vm((FFN_ROWS, model), F32), vm((FFN_ROWS, model), F32),
        ] + two_sems(rows // FFN_ROWS),
        compiler_params=pltpu.CompilerParams(collective_id=1, has_side_effects=True),
        name="ffn",
    )(tok, o_own, o_peer, w_own, w_peer, bo, gain, shift, w_in, b_in, w_back, bb, cot)


def attn_bwd_kernel(
    groups, keep, give, qt, kx, kt, vx, dot_t, khot, khott, qhott, qhot, table, kwin, qwin, lse,
    out, dq, dk, dv, gcell, dk_acc, dv_acc, got, send_sem, recv_sem,
):
    step = pl.program_id(0)
    rows_all = dk.shape[0]
    swap = to_peer(give, got, send_sem.at[0], recv_sem.at[0])

    @pl.when(step == 0)
    def _():
        greet()
        swap.start()
        dk_acc[...] = jnp.zeros_like(dk_acc)
        dv_acc[...] = jnp.zeros_like(dv_acc)
        gcell[...] = jnp.zeros_like(gcell)

    start = pl.multiple_of(step * QB, QB)
    span = pl.ds(start, SPAN)
    mask = jnp.where(kwin[span, :] == qwin[...], 0.0, NEG)
    hot = khot[span, :]
    hot_t = khott[:, span]
    cells = qhott[...]
    cells_r = qhot[...]
    for g in range(groups):
        lanes = slice(128 * g, 128 * (g + 1))
        q_stack = stack_heads(qt[lanes, :])
        do_stack = stack_heads(dot_t[lanes, :])
        right = jnp.concatenate([q_stack, bias_rows(table, g, cells)], axis=0)
        scores = dot(jnp.concatenate([kx[span, lanes], hot], axis=1), right)
        dprob = dot(vx[span, lanes], do_stack)
        ps, dss, dqs = [], [], []
        for j in range(GROUP):
            h = GROUP * g + j
            cut = slice(QB * j, QB * (j + 1))
            p = jnp.exp(scores[:, cut] * SCALE + mask - lse[h : h + 1, :])
            t = p * dprob[:, cut]
            inner = jnp.sum(t, axis=0, keepdims=True)
            ds = (t - p * inner).astype(BF16)
            ps.append(p.astype(BF16))
            dss.append(ds)
            both = dot(jnp.concatenate([kt[HEAD_DIM * h : HEAD_DIM * (h + 1), span], hot_t], axis=0), ds)
            dqs.append(both[:HEAD_DIM])
            gcell[CP * h : CP * (h + 1), :] += dot(both[HEAD_DIM:].astype(BF16), cells_r)
        dq[:, lanes] = (jnp.concatenate(dqs, axis=0) * SCALE).T.astype(BF16)
        dk_acc[span, lanes] += dot_nt(jnp.concatenate(dss, axis=1), q_stack)
        dv_acc[span, lanes] += dot_nt(jnp.concatenate(ps, axis=1), do_stack)

    @pl.when(step == rows_all // QB - 1)
    def _():
        inner_rows = pl.ds(HALO, rows_all)
        dk[...] = (dk_acc[inner_rows, :] * SCALE).astype(BF16)
        dv[...] = dv_acc[inner_rows, :].astype(BF16)
        swap.wait()
        out[...] = (keep[...] + got[...].astype(F32)).astype(BF16)


def attn_bwd(keep, give, qt, kx, kt, vx, dot_t, khot, khott, qhott, qhot, table, kwin, qwin, lse):
    width, rows = qt.shape
    heads = width // HEAD_DIM
    ext = rows + 2 * HALO
    half = keep.shape[1]
    shape = jax.ShapeDtypeStruct
    rblk = lambda n: pl.BlockSpec((QB, n), lambda i: (i, 0))
    return pl.pallas_call(
        partial(attn_bwd_kernel, heads // GROUP),
        grid=(rows // QB,),
        in_specs=[
            whole(keep), pl.BlockSpec(memory_space=pltpu.VMEM),
            cols(width), whole(kx), whole(kt), whole(vx), cols(width), whole(khot), whole(khott),
            cols(CP), rblk(CP), whole(table), whole(kwin), cols(1), cols(heads),
        ],
        out_specs=[
            same(rows, half), rblk(width), same(rows, width), same(rows, width), same(CP * heads, CP),
        ],
        out_shape=[
            shape((rows, half), BF16), shape((rows, width), BF16), shape((rows, width), BF16),
            shape((rows, width), BF16), shape((CP * heads, CP), F32),
        ],
        scratch_shapes=[
            pltpu.VMEM((ext, width), F32), pltpu.VMEM((ext, width), F32), pltpu.VMEM((rows, half), BF16),
        ] + two_sems(1),
        compiler_params=pltpu.CompilerParams(collective_id=2, has_side_effects=True),
        name="attn_bwd",
    )(keep, give, qt, kx, kt, vx, dot_t, khot, khott, qhott, qhot, table, kwin, qwin, lse)


def close_kernel(
    tok, a, dq, dk, dv, wt, gain, gr, vec2, vec_in, table, out, late,
    ga_s, give, got, stat, stat_p, wide, vec_s, vec_p, send_sem, recv_sem,
):
    rows_all, model = tok.shape
    width = dq.shape[1]
    half = out.shape[1]
    chunks = rows_all // CLOSE_ROWS
    me = lax.axis_index("mp")
    own = half_lanes(me, half)
    other = half_lanes(1 - me, half)
    greet()
    vec_s[...] = jnp.zeros_like(vec_s)
    main = lambda c: rows_copy(give, got, CLOSE_ROWS, (send_sem.at[0], recv_sem.at[0]), c)
    side = lambda c: rows_copy(stat, stat_p, CLOSE_ROWS, (send_sem.at[1], recv_sem.at[1]), c)
    lane = lax.broadcasted_iota(jnp.int32, (CLOSE_ROWS, 128), 1)

    def norms(at):
        x = tok[at, :].astype(F32)
        center = x - jnp.mean(x, axis=-1, keepdims=True)
        r = lax.rsqrt(jnp.mean(center * center, axis=-1, keepdims=True) + EPS)
        return center * r, r

    def forward(c, carry):
        at = pl.ds(pl.multiple_of(c * CLOSE_ROWS, CLOSE_ROWS), CLOSE_ROWS)
        ga = dot(dq[at, :], wt[:width, :]) + dot(dk[at, :], wt[width : 2 * width, :])
        ga = ga + dot(dv[at, :], wt[2 * width :, :])
        wide[...] = ga
        give[at, :] = wide[:, other].astype(BF16)
        ga_s[at, :] = wide[:, own]
        n, r = norms(at)
        e = ga * gain[...]
        first = jnp.mean(e, axis=-1, keepdims=True)
        second = jnp.mean(e * n, axis=-1, keepdims=True)
        stat[at, :] = jnp.where(lane == 0, first, jnp.where(lane == 1, second, 0.0))
        vec_s[0:1, :] += jnp.sum(ga * n, axis=0, keepdims=True)
        vec_s[1:2, :] += jnp.sum(ga, axis=0, keepdims=True)
        main(c).start()
        side(c).start()
        return carry

    lax.fori_loop(0, chunks, forward, 0)
    vectors = to_peer(vec_s, vec_p, send_sem.at[2, 0], recv_sem.at[2, 0])
    grads = jnp.concatenate([dq[...], dk[...], dv[...]], axis=1)
    for b in range(2):
        block = dot_tn(a[:, width * b : width * (b + 1)], grads).astype(BF16)
        for c in range(3):
            k = 2 * c + b
            goal = (width * (k % 3), width * (k // 3))
            late[goal[0] : goal[0] + width, goal[1] : goal[1] + width] = block[:, width * c : width * (c + 1)]
    vectors.start()
    qv = [jnp.sum(item[...].astype(F32), axis=0, keepdims=True) for item in (dq, dv)]

    def backward(c, carry):
        at = pl.ds(pl.multiple_of(c * CLOSE_ROWS, CLOSE_ROWS), CLOSE_ROWS)
        main(c).wait()
        side(c).wait()
        sums = stat[at, :] + stat_p[at, :]
        n, r = norms(at)
        wide[...] = n
        e = (ga_s[at, :] + got[at, :].astype(F32)) * gain[:, own]
        gx = gr[at, :] + r * (e - sums[:, 0:1] - wide[:, own] * sums[:, 1:2])
        out[at, :] = gx.astype(BF16)
        return carry

    lax.fori_loop(0, chunks, backward, 0)
    vectors.wait()
    first = vec_s[0:2, :] + vec_p[0:2, :]
    parts = [first[0:1], first[1:2]] + [vec2[k : k + 1, :] for k in range(4)]
    parts.append(jnp.concatenate(qv, axis=1))
    parts += [vec_in[:, model * k : model * (k + 1)] for k in range(vec_in.shape[1] // model)]
    parts += [table[k : k + 1, :] for k in range(table.shape[0])]
    parts.append(jnp.zeros((SMALL - len(parts), model), F32))
    late[3 * width : 3 * width + SMALL, :] = jnp.concatenate(parts, axis=0).astype(BF16)
    spare = late.shape[0] - 3 * width - SMALL
    late[3 * width + SMALL :, :] = jnp.zeros((spare, model), BF16)


def close(late_rows, tok, a, dq, dk, dv, wt, gain, gr, vec2, vec_in, table):
    rows, model = tok.shape
    width = dq.shape[1]
    half = gr.shape[1]
    chunks = rows // CLOSE_ROWS
    shape = jax.ShapeDtypeStruct
    vm = pltpu.VMEM
    sems = pltpu.SemaphoreType.DMA((3, chunks))
    return pl.pallas_call(
        close_kernel,
        in_specs=[pl.BlockSpec(memory_space=pltpu.VMEM)] * 11,
        out_specs=[pl.BlockSpec(memory_space=pltpu.VMEM)] * 2,
        out_shape=[shape((rows, half), BF16), shape((late_rows, model), BF16)],
        scratch_shapes=[
            vm((rows, half), F32), vm((rows, half), BF16), vm((rows, half), BF16), vm((rows, 128), F32),
            vm((rows, 128), F32), vm((CLOSE_ROWS, model), F32), vm((8, model), F32), vm((8, model), F32),
            sems, sems,
        ],
        compiler_params=pltpu.CompilerParams(collective_id=3, has_side_effects=True),
        name="close",
    )(tok, a, dq, dk, dv, wt, gain, gr, vec2, vec_in, table)


def dp_copy(src, dst, partner, send_sem, recv_sem):
    return pltpu.make_async_remote_copy(
        src_ref=src,
        dst_ref=dst,
        send_sem=send_sem,
        recv_sem=recv_sem,
        device_id={"dp": partner},
        device_id_type=MESH,
    )


def dp_sum_kernel(flows, x, big, small, out, acc, got, send_sem, recv_sem):
    rows = x.shape[0]
    steps = len(flows[0][0])
    place = lax.axis_index("dp")

    def bit_of(b):
        return lax.rem(lax.div(place, 1 << b), 2)

    def partner_of(b):
        return place + (1 - 2 * bit_of(b)) * (1 << b)

    barrier = pltpu.get_barrier_semaphore()
    for b in range(steps):
        pl.semaphore_signal(barrier, inc=1, device_id={"dp": partner_of(b)}, device_id_type=MESH)
    pl.semaphore_wait(barrier, steps)

    lows = [[0] for _ in flows]
    for k, (order, _, _) in enumerate(flows):
        for s in range(steps):
            lows[k].append(lows[k][s] + bit_of(order[s]) * (rows >> (s + 1)))

    def halve(k, s):
        order, lane, count = flows[k]
        size = rows >> (s + 1)
        lanes = pl.ds(lane, count)
        theirs = pl.multiple_of(lows[k][s] + (1 - bit_of(order[s])) * size, 16)
        copy = dp_copy(
            (x if s == 0 else acc).at[pl.ds(theirs, size), lanes],
            got.at[pl.ds(rows - (rows >> s), size), lanes],
            partner_of(order[s]),
            send_sem.at[k, s],
            recv_sem.at[k, s],
        )
        copy.start()
        return copy

    def add(k, s):
        _, lane, count = flows[k]
        size = rows >> (s + 1)
        base = rows - (rows >> s)
        lanes = slice(lane, lane + count)
        mine = pl.ds(pl.multiple_of(lows[k][s + 1], 16), size)
        total = (x if s == 0 else acc)[mine, lanes].astype(F32) + got[base : base + size, lanes].astype(F32)
        (out if s == steps - 1 else acc)[mine, lanes] = total.astype(BF16)

    def double(k, s):
        order, lane, count = flows[k]
        at = 2 * steps - 1 - s
        region = out.at[pl.ds(pl.multiple_of(lows[k][s + 1], 16), rows >> (s + 1)), pl.ds(lane, count)]
        copy = dp_copy(region, region, partner_of(order[s]), send_sem.at[k, at], recv_sem.at[k, at])
        copy.start()
        return copy

    copies = [halve(k, 0) for k in range(len(flows))]
    for s in range(steps):
        for k in range(len(flows)):
            copies[k].wait()
            add(k, s)
            copies[k] = halve(k, s + 1) if s + 1 < steps else double(k, s)
    for s in reversed(range(steps)):
        for k in range(len(flows)):
            copies[k].wait()
            if s > 0:
                copies[k] = double(k, s - 1)
    tall = big.shape[0] // 2
    for k in range(2):
        big[tall * k : tall * (k + 1), :] = out[:tall, big.shape[1] * k : big.shape[1] * (k + 1)]
    small[...] = out[tall : tall + small.shape[0], :].astype(F32)


def dp_sum(ranks, big_shape, x):
    rows, wide = x.shape
    steps = ranks.bit_length() - 1
    first, second = list(range(steps)), [0] + list(range(2, steps)) + [1]
    flows = [(first, 0, 256), (second, 256, 256), (first, 512, 128), (second, 640, 128)]
    vm = pltpu.VMEM
    sems = pltpu.SemaphoreType.DMA((len(flows), 2 * steps))
    return pl.pallas_call(
        partial(dp_sum_kernel, flows),
        in_specs=[pl.BlockSpec(memory_space=pltpu.VMEM)],
        out_specs=[pl.BlockSpec(memory_space=pltpu.VMEM)] * 2,
        out_shape=[jax.ShapeDtypeStruct(big_shape, BF16), jax.ShapeDtypeStruct((SMALL, wide), F32)],
        scratch_shapes=[vm((rows, wide), BF16)] * 3 + [sems, sems],
        compiler_params=pltpu.CompilerParams(collective_id=4, has_side_effects=True),
        name="dp_sum",
    )(x)


def window_data(crop_counts, crop_patches, rel_index, rel_table, rows):
    highest = lax.Precision.HIGHEST
    heads = rel_table.shape[1]
    cells, wins = layout(crop_counts, crop_patches, rows)
    kcells = jnp.pad(cells, (HALO, HALO))
    kwin = jnp.pad(wins, (HALO, HALO), constant_values=-1)[:, None]
    span_cells = jnp.arange(CP, dtype=jnp.int32)
    wide_cells = jnp.arange(2 * CP, dtype=jnp.int32) % CP
    khot = (kcells[:, None] == wide_cells[None, :]).astype(BF16)
    khott = (span_cells[:, None] == kcells[None, :]).astype(BF16)
    qhott = (span_cells[:, None] == cells[None, :]).astype(BF16)
    qhot = (cells[:, None] == span_cells[None, :]).astype(BF16)
    rel_t = jnp.pad(rel_index.T, ((0, CP - CELLS), (0, CP - CELLS)), constant_values=-1).reshape(-1)
    offset_hot = (rel_t[:, None] == jnp.arange(OFFSETS, dtype=jnp.int32)[None, :]).astype(F32)
    bias = jnp.einsum("pm,mh->hp", offset_hot, rel_table, precision=highest) / SCALE
    high = bias.astype(BF16)
    rest = (bias - high.astype(F32)).astype(BF16)
    table = jnp.stack([high.reshape(heads, CP, CP), rest.reshape(heads, CP, CP)], axis=1)
    return (khot, khott, qhott, qhot, table.reshape(heads * 2 * CP, CP), kwin, wins[None, :], offset_hot)


def body(
    tokens,
    crop_counts,
    crop_patches,
    rel_index,
    ln1_gain,
    ln1_shift,
    w_qkv,
    qv_bias,
    rel_table,
    w_out,
    b_out,
    ln2_gain,
    ln2_shift,
    w_in,
    b_in,
    w_back,
    b_back,
    cotangent,
):
    highest = lax.Precision.HIGHEST
    rows, part_width = tokens.shape
    model = ln1_gain.shape[0]
    width = w_qkv.shape[2]
    heads = width // HEAD_DIM
    khot, khott, qhott, qhot, table, kwin, qwin, offset_hot = window_data(
        crop_counts, crop_patches, rel_index, rel_table, rows
    )
    whole_in = lax.all_gather(tokens, "mp", axis=1, tiled=True)
    wt = jnp.transpose(w_qkv, (1, 2, 0)).reshape(3 * width, model)
    mixer_in, qt, kx, kt, vx, heads_out, heads_peer, w_peer, whole_cot, lse = attn_fwd(
        w_out, cotangent,
        whole_in, ln1_gain[None, :], ln1_shift[None, :], wt, qv_bias[0][:, None], qv_bias[1][:, None],
        qv_bias[1][None, :], khot, qhott, table, kwin, qwin,
    )
    keep, give, gr, dot_t, grad_w_out, grad_w_in, grad_w_back, vec2, grad_b_in = ffn(
        whole_in, heads_out, heads_peer, w_out, w_peer, b_out[None, :], ln2_gain[None, :], ln2_shift[None, :],
        w_in, b_in[None, :], w_back, b_back[None, :], whole_cot,
    )
    early = lax.psum((grad_w_in, grad_w_back, grad_w_out), "dp")
    out_half, grad_query, grad_key, grad_value, gcell = attn_bwd(
        keep, give, qt, kx, kt, vx, dot_t, khot, khott, qhott, qhot, table, kwin, qwin, lse
    )
    grad_table = jnp.einsum(
        "pm,hp->mh", offset_hot, gcell.reshape(heads, CP * CP), precision=highest
    )
    table_rows = -(-grad_table.size // model)
    table_flat = jnp.pad(grad_table.reshape(-1), (0, table_rows * model - grad_table.size))
    ranks = lax.axis_size("dp")
    late_rows = -(-(3 * width + SMALL) // (16 * ranks)) * 16 * ranks
    grad_half, late = close(
        late_rows, whole_in, mixer_in, grad_query, grad_key, grad_value, wt, ln1_gain[None, :], gr,
        vec2, grad_b_in, table_flat.reshape(table_rows, model),
    )
    big, small = dp_sum(ranks, (3 * model, width), late)
    big = big.astype(F32)
    early, big = lax.optimization_barrier((early, big))
    grad_w_in, grad_w_back, grad_w_out = (item.astype(F32) for item in early)
    grad_w_qkv = jnp.transpose(big.reshape(3, model, width), (1, 0, 2))
    grad_g1, grad_c1, grad_g2, grad_c2, grad_b_out, grad_b_back = (small[k] for k in range(6))
    grad_qv_bias = small[6].reshape(2, width)
    hidden_rows = w_in.shape[1] // model
    grad_b_in = small[7 : 7 + hidden_rows].reshape(-1)
    flat = small[7 + hidden_rows : 7 + hidden_rows + table_rows].reshape(-1)
    grad_table = flat[: grad_table.size].reshape(grad_table.shape)
    return (
        out_half,
        grad_half,
        grad_g1,
        grad_c1,
        grad_w_qkv,
        grad_qv_bias,
        grad_table,
        grad_w_out,
        grad_b_out,
        grad_g2,
        grad_c2,
        grad_w_in,
        grad_b_in,
        grad_w_back,
        grad_b_back,
    )


def solution(mesh):
    return jax.shard_map(
        body,
        mesh=mesh,
        in_specs=(
            P("dp", "mp"),
            P("dp"),
            P("dp", None),
            P(),
            P(),
            P(),
            P(None, None, "mp"),
            P(None, "mp"),
            P(None, "mp"),
            P("mp", None),
            P(),
            P(),
            P(),
            P(None, "mp"),
            P("mp"),
            P("mp", None),
            P(),
            P("dp", "mp"),
        ),
        out_specs=(
            P("dp", "mp"),
            P("dp", "mp"),
            P(),
            P(),
            P(None, None, "mp"),
            P(None, "mp"),
            P(None, "mp"),
            P("mp", None),
            P(),
            P(),
            P(),
            P(None, "mp"),
            P("mp"),
            P("mp", None),
            P(),
        ),
        check_vma=False,
    )
```

```python
from functools import partial

import jax
import jax.numpy as jnp
from jax import lax
from jax.experimental import pallas as pl
from jax.experimental.pallas import tpu as pltpu
from jax.sharding import PartitionSpec as P

HEAD_DIM = 32
SIDE = 7
LOCAL_SIDE = 3
CELLS = 49
OFFSETS = 169
CROP_MAX = 8
QB = 128
HALO = 64
SPAN = QB + 2 * HALO
CP = 64
GROUP = 4
SCALE = HEAD_DIM ** (-0.5)
EPS = 1e-05
NEG = -1e30
BLOCK = 256
FFN_ROWS = 128
CLOSE_ROWS = 128
SMALL = 16
MESH = pl.DeviceIdType.MESH
F32 = jnp.float32
BF16 = jnp.bfloat16


def layout(counts, patches, row_count):
    live_crop = jnp.arange(CROP_MAX, dtype=jnp.int32)[None, :] < counts[:, None]
    crop_rows = jnp.where(live_crop, patches, 0).reshape(-1)
    crop_ends = jnp.cumsum(crop_rows)
    used_rows = crop_ends[-1]
    row_ids = jnp.arange(row_count, dtype=jnp.int32)
    passed = crop_ends[None, :] <= row_ids[:, None]
    window = jnp.sum(passed.astype(jnp.int32), axis=1)
    starts = jnp.max(jnp.where(passed, crop_ends[None, :], 0), axis=1)
    finish = jnp.min(jnp.where(passed, row_count + used_rows + 1, crop_ends[None, :]), axis=1)
    length = finish - starts
    offset = row_ids - starts
    grid_side = jnp.where(length >= CELLS, SIDE, LOCAL_SIDE).astype(jnp.int32)
    cell_index = offset // grid_side * SIDE + offset % grid_side
    inside = row_ids < used_rows
    cell_ids = jnp.where(inside, cell_index, 0)
    windows = jnp.where(inside, window, crop_rows.shape[0] + row_ids - used_rows)
    return (cell_ids, windows)


def layer_norm(values, gain, shift):
    center = values - jnp.mean(values, axis=-1, keepdims=True)
    spread = jnp.mean(center * center, axis=-1, keepdims=True)
    return center * lax.rsqrt(spread + EPS) * gain + shift


def dot(a, b):
    return jnp.dot(a, b, preferred_element_type=F32)


def dot_nt(a, b):
    return lax.dot_general(a, b, (((1,), (1,)), ((), ())), preferred_element_type=F32)


def stack_heads(rows_t):
    cols = []
    for j in range(GROUP):
        parts = []
        if j > 0:
            parts.append(jnp.zeros((HEAD_DIM * j, QB), BF16))
        parts.append(rows_t[HEAD_DIM * j : HEAD_DIM * (j + 1)])
        if j < GROUP - 1:
            parts.append(jnp.zeros((HEAD_DIM * (GROUP - 1 - j), QB), BF16))
        cols.append(jnp.concatenate(parts, axis=0))
    return jnp.concatenate(cols, axis=1)


def bias_rows(table, g, cells):
    tall = dot(table[2 * CP * GROUP * g : 2 * CP * GROUP * (g + 1), :], cells).astype(BF16)
    return jnp.concatenate([tall[2 * CP * j : 2 * CP * (j + 1)] for j in range(GROUP)], axis=1)


def dot_tn(a, b):
    return lax.dot_general(a, b, (((0,), (0,)), ((), ())), preferred_element_type=F32)


def peer_of():
    return 1 - lax.axis_index("mp")


def greet():
    barrier = pltpu.get_barrier_semaphore()
    pl.semaphore_signal(barrier, inc=1, device_id={"mp": peer_of()}, device_id_type=MESH)
    pl.semaphore_wait(barrier, 1)


def to_peer(src, dst, send_sem, recv_sem):
    return pltpu.make_async_remote_copy(
        src_ref=src,
        dst_ref=dst,
        send_sem=send_sem,
        recv_sem=recv_sem,
        device_id={"mp": peer_of()},
        device_id_type=MESH,
    )


def rows_copy(src, dst, size, sems, i):
    at = pl.ds(pl.multiple_of(i * size, size), size)
    return to_peer(src.at[at], dst.at[at], sems[0].at[i], sems[1].at[i])


def half_lanes(index, half):
    return pl.ds(pl.multiple_of(index * half, 128), half)


def attn_fwd_kernel(
    groups, w_own, cot_own, tok_low, tok_own, gain, shift, wt, qb_col, vb_col, vb_row, khot, qhott, table, kwin, qwin,
    tok, a_out, qt, kx, kt, vx, o_out, peer_out, w_out, cot, lse,
    a_pad, vt, o_all, o_peer, w_got, cot_got, tok_got, send_sem, recv_sem,
):
    step = pl.program_id(0)
    last = tok.shape[0] // QB - 1
    rows_all = tok.shape[0]
    width = qt.shape[0]
    sems = (send_sem, recv_sem)
    place = lax.axis_index("dp")
    core = lax.rem(place, 2)
    mate = place + 1 - 2 * core
    fetched = w_own.shape[0] // 2
    part = pl.ds(pl.multiple_of(core * fetched, 16), fetched)
    weight = to_peer(w_own.at[part], w_got.at[part], send_sem.at[last + 1], recv_sem.at[last + 1])
    low = tok_low.shape[0]
    rest = to_peer(tok_own, tok_got, send_sem.at[last + 4], recv_sem.at[last + 4])
    swap = to_peer(cot_own, cot_got, send_sem.at[last + 3], recv_sem.at[last + 3])
    handed = dp_copy(w_got.at[part], w_got.at[part], mate, send_sem.at[last + 2], recv_sem.at[last + 2])

    @pl.when(step == 0)
    def _():
        barrier = pltpu.get_barrier_semaphore()
        pl.semaphore_signal(barrier, inc=1, device_id={"mp": peer_of()}, device_id_type=MESH)
        pl.semaphore_signal(barrier, inc=1, device_id={"dp": mate}, device_id_type=MESH)
        pl.semaphore_wait(barrier, 2)
        rest.start()
        weight.start()
        swap.start()
        half = tok_own.shape[1]
        me = lax.axis_index("mp")
        tok[:low, :] = tok_low[...]
        tok[low:, half_lanes(me, half)] = tok_own[...]
        zero = jnp.zeros((HALO, tok.shape[1]), BF16)
        a_pad[:HALO, :] = zero
        a_pad[HALO + rows_all :, :] = zero

        def norm_rows(i, carry):
            at = pl.multiple_of(i * QB, QB)
            a = layer_norm(tok[pl.ds(at, QB), :].astype(F32), gain[...], shift[...]).astype(BF16)
            a_out[pl.ds(at, QB), :] = a
            a_pad[pl.ds(pl.multiple_of(at + HALO, HALO), QB), :] = a
            return carry

        wk = wt[width : 2 * width, :]
        wv = wt[2 * width :, :]

        def project(first, end, first_pad, end_pad):
            q_rows = slice(first, end)
            rows = slice(first_pad, end_pad)
            a_some = a_pad[rows, :]
            qt[:, q_rows] = (dot_nt(wt[:width, :], a_out[q_rows, :]) + qb_col[...]).astype(BF16)
            kx[rows, :] = dot_nt(a_some, wk).astype(BF16)
            kt[:, rows] = dot_nt(wk, a_some).astype(BF16)
            vx[rows, :] = (dot_nt(a_some, wv) + vb_row[...]).astype(BF16)
            vt[:, rows] = (dot_nt(wv, a_some) + vb_col[...]).astype(BF16)

        lax.fori_loop(0, low // QB, norm_rows, 0)
        project(0, low, 0, low)
        rest.wait()
        tok[low:, half_lanes(1 - me, half)] = tok_got[...]
        lax.fori_loop(low // QB, rows_all // QB, norm_rows, 0)
        project(low, rows_all, low, rows_all + 2 * HALO)

    start = pl.multiple_of(step * QB, QB)
    span = pl.ds(start, SPAN)
    mask = jnp.where(kwin[span, :] == qwin[...], 0.0, NEG)
    hot = khot[span, :]
    cells = qhott[...]
    for g in range(groups):
        lanes = slice(128 * g, 128 * (g + 1))
        right = jnp.concatenate(
            [stack_heads(qt[lanes, pl.ds(start, QB)]), bias_rows(table, g, cells)], axis=0
        )
        scores = dot(jnp.concatenate([kx[span, lanes], hot], axis=1), right)
        outs = []
        for j in range(GROUP):
            h = GROUP * g + j
            s = scores[:, QB * j : QB * (j + 1)] * SCALE + mask
            peak = jnp.max(s, axis=0, keepdims=True)
            e = jnp.exp(s - peak)
            mass = jnp.sum(e, axis=0, keepdims=True)
            outs.append(dot(vt[HEAD_DIM * h : HEAD_DIM * (h + 1), span], e.astype(BF16)) / mass)
            lse[h : h + 1, :] = peak + jnp.log(mass)
        o_all[pl.ds(start, QB), lanes] = jnp.concatenate(outs, axis=0).T.astype(BF16)

    @pl.when(step > 0)
    def _():
        rows_copy(o_all, o_peer, QB, sems, step - 1).start()

    @pl.when(step == last - 2)
    def _():
        weight.wait()
        handed.start()

    @pl.when(step == last)
    def _():
        o_out[...] = o_all[...]
        half = cot_own.shape[1]
        me = lax.axis_index("mp")
        cot[:, half_lanes(me, half)] = cot_own[...]
        swap.wait()
        cot[:, half_lanes(1 - me, half)] = cot_got[...]
        rows_copy(o_all, o_peer, QB, sems, last).start()

        def finish(i, carry):
            copy = rows_copy(o_all, o_peer, QB, sems, i)
            copy.wait()
            return carry

        lax.fori_loop(0, last + 1, finish, 0)
        handed.wait()
        w_out[...] = w_got[...]
        peer_out[...] = o_peer[...]


def whole(a):
    return pl.BlockSpec(a.shape, lambda i: (0,) * len(a.shape))


def same(*shape):
    return pl.BlockSpec(shape, lambda i: (0,) * len(shape))


def cols(n):
    return pl.BlockSpec((n, QB), lambda i: (0, i))


def two_sems(n):
    return [pltpu.SemaphoreType.DMA((n,)), pltpu.SemaphoreType.DMA((n,))]


def attn_fwd(w_own, cot_own, tok_low, tok_own, gain, shift, wt, qb_col, vb_col, vb_row, khot, qhott, table, kwin, qwin):
    rows, model = tok_low.shape[0] + tok_own.shape[0], tok_low.shape[1]
    width = wt.shape[0] // 3
    heads = width // HEAD_DIM
    ext = rows + 2 * HALO
    shape = jax.ShapeDtypeStruct
    return pl.pallas_call(
        partial(attn_fwd_kernel, heads // GROUP),
        grid=(rows // QB,),
        in_specs=[pl.BlockSpec(memory_space=pltpu.VMEM)] * 2
        + [whole(tok_low), pl.BlockSpec(memory_space=pltpu.VMEM)]
        + [whole(x) for x in (gain, shift, wt, qb_col, vb_col, vb_row, khot)]
        + [cols(CP), whole(table), whole(kwin), cols(1)],
        out_specs=[
            same(rows, model), same(rows, model), same(width, rows), same(ext, width), same(width, ext), same(ext, width),
            same(rows, width), same(rows, width), same(width, model), same(rows, model),
            cols(heads),
        ],
        out_shape=[
            shape((rows, model), BF16), shape((rows, model), BF16), shape((width, rows), BF16), shape((ext, width), BF16),
            shape((width, ext), BF16), shape((ext, width), BF16), shape((rows, width), BF16),
            shape((rows, width), BF16), shape((width, model), BF16), shape((rows, model), BF16),
            shape((heads, rows), F32),
        ],
        scratch_shapes=[
            pltpu.VMEM((ext, model), BF16), pltpu.VMEM((width, ext), BF16),
            pltpu.VMEM((rows, width), BF16), pltpu.VMEM((rows, width), BF16),
            pltpu.VMEM((width, model), BF16), pltpu.VMEM(cot_own.shape, BF16),
            pltpu.VMEM(tok_own.shape, BF16),
        ] + two_sems(rows // QB + 4),
        compiler_params=pltpu.CompilerParams(collective_id=0, has_side_effects=True),
        name="attn_fwd",
    )(w_own, cot_own, tok_low, tok_own, gain, shift, wt, qb_col, vb_col, vb_row, khot, qhott, table, kwin, qwin)


def ffn_kernel(
    tok, o_own, o_peer, w_own, w_peer, bo, gain, shift, w_in, b_in, w_back, bb, cot,
    keep, give, gr, dot_t, g_out, g_in, g_back, vec, vec_in,
    n_s, r_s, h_s, z_s, du_s, gh_s, gh_p, g_acc, wide_a, wide_b, send_sem, recv_sem,
):
    rows_all, model = tok.shape
    half = keep.shape[1]
    chunks = rows_all // FFN_ROWS
    sems = (send_sem, recv_sem)
    me = lax.axis_index("mp")
    own = half_lanes(me, half)
    other = half_lanes(1 - me, half)
    greet()
    vec[...] = jnp.zeros_like(vec)
    vec_in[...] = jnp.zeros_like(vec_in)

    def forward(c, carry):
        at = pl.ds(pl.multiple_of(c * FFN_ROWS, FFN_ROWS), FFN_ROWS)
        x1 = tok[at, :].astype(F32) + dot(o_own[at, :], w_own[...]) + dot(o_peer[at, :], w_peer[...])
        x1 = x1 + bo[...]
        center = x1 - jnp.mean(x1, axis=-1, keepdims=True)
        r = lax.rsqrt(jnp.mean(center * center, axis=-1, keepdims=True) + EPS)
        n = center * r
        h = (n * gain[...] + shift[...]).astype(BF16)
        wide_b[...] = x1
        n_s[at, :] = n
        r_s[at, :] = r
        h_s[at, :] = h
        u = dot(h, w_in[...]) + b_in[...]
        cdf = 0.5 * (1.0 + lax.erf(u * (0.5**0.5)))
        slope = cdf + u * (jnp.exp(-0.5 * u * u) * 0.3989422804014327)
        z = (u * cdf).astype(BF16)
        z_s[at, :] = z
        du = (dot_nt(cot[at, :], w_back[...]) * slope).astype(BF16)
        du_s[at, :] = du
        gh_s[at, :] = dot_nt(du, w_in[...]).astype(BF16)
        vec_in[...] += jnp.sum(du.astype(F32), axis=0, keepdims=True)
        keep[at, :] = wide_b[:, own] + bb[:, own]
        rows_copy(gh_s, gh_p, FFN_ROWS, sems, c).start()
        return carry

    lax.fori_loop(0, chunks, forward, 0)

    def output(c, carry):
        at = pl.ds(pl.multiple_of(c * FFN_ROWS, FFN_ROWS), FFN_ROWS)
        wide_a[...] = dot(z_s[at, :], w_back[...])
        keep[at, :] += wide_a[:, own]
        give[at, :] = wide_a[:, other].astype(BF16)
        return carry

    lax.fori_loop(0, chunks, output, 0)
    g_acc[...] = jnp.zeros_like(g_acc)

    def back_block(i, carry):
        at = pl.ds(pl.multiple_of(i * BLOCK, BLOCK), BLOCK)
        g_back[at, :] = dot_tn(z_s[:, at], cot[...]).astype(BF16)
        return carry

    lax.fori_loop(0, z_s.shape[1] // BLOCK, back_block, 0)

    def in_block(i, carry):
        at = pl.ds(pl.multiple_of(i * BLOCK, BLOCK), BLOCK)
        g_in[at, :] = dot_tn(h_s[:, at], du_s[...]).astype(BF16)
        return carry

    lax.fori_loop(0, model // BLOCK, in_block, 0)

    def backward(c, carry):
        at = pl.ds(pl.multiple_of(c * FFN_ROWS, FFN_ROWS), FFN_ROWS)
        rows_copy(gh_s, gh_p, FFN_ROWS, sems, c).wait()
        gh = gh_s[at, :].astype(F32) + gh_p[at, :].astype(F32)
        n = n_s[at, :]
        e = gh * gain[...]
        gy = cot[at, :].astype(F32)
        mean_e = jnp.mean(e, axis=-1, keepdims=True)
        mean_n = jnp.mean(e * n, axis=-1, keepdims=True)
        gx1 = gy + r_s[at, :] * (e - mean_e - n * mean_n)
        wide_a[...] = gx1
        go = gx1.astype(BF16)
        g_acc[...] += dot_tn(o_own[at, :], go)
        dot_t[:, at] = dot_nt(w_own[...], go).astype(BF16)
        vec[0:1, :] += jnp.sum(gh * n, axis=0, keepdims=True)
        vec[1:2, :] += jnp.sum(gh, axis=0, keepdims=True)
        vec[2:3, :] += jnp.sum(go.astype(F32), axis=0, keepdims=True)
        vec[3:4, :] += jnp.sum(gy, axis=0, keepdims=True)
        gr[at, :] = wide_a[:, own]
        return carry

    lax.fori_loop(0, chunks, backward, 0)
    g_out[...] = g_acc[...].astype(BF16)


def ffn(tok, o_own, o_peer, w_own, w_peer, bo, gain, shift, w_in, b_in, w_back, bb, cot):
    rows, model = tok.shape
    width = o_own.shape[1]
    hidden = w_in.shape[1]
    half = model // 2
    shape = jax.ShapeDtypeStruct
    vm = pltpu.VMEM
    return pl.pallas_call(
        ffn_kernel,
        in_specs=[pl.BlockSpec(memory_space=pltpu.VMEM)] * 13,
        out_specs=[pl.BlockSpec(memory_space=pltpu.VMEM)] * 9,
        out_shape=[
            shape((rows, half), F32), shape((rows, half), BF16), shape((rows, half), F32),
            shape((width, rows), BF16), shape((width, model), BF16), shape((model, hidden), BF16),
            shape((hidden, model), BF16), shape((8, model), F32), shape((1, hidden), F32),
        ],
        scratch_shapes=[
            vm((rows, model), F32), vm((rows, 1), F32), vm((rows, model), BF16), vm((rows, hidden), BF16),
            vm((rows, hidden), BF16), vm((rows, model), BF16), vm((rows, model), BF16),
            vm((width, model), F32), vm((FFN_ROWS, model), F32), vm((FFN_ROWS, model), F32),
        ] + two_sems(rows // FFN_ROWS),
        compiler_params=pltpu.CompilerParams(collective_id=1, has_side_effects=True),
        name="ffn",
    )(tok, o_own, o_peer, w_own, w_peer, bo, gain, shift, w_in, b_in, w_back, bb, cot)


def attn_bwd_kernel(
    groups, keep, give, qt, kx, kt, vx, dot_t, khot, khott, qhott, qhot, table, kwin, qwin, lse,
    out, dq, dk, dv, gcell, dk_acc, dv_acc, got, send_sem, recv_sem,
):
    step = pl.program_id(0)
    rows_all = dk.shape[0]
    swap = to_peer(give, got, send_sem.at[0], recv_sem.at[0])

    @pl.when(step == 0)
    def _():
        greet()
        swap.start()
        dk_acc[...] = jnp.zeros_like(dk_acc)
        dv_acc[...] = jnp.zeros_like(dv_acc)
        gcell[...] = jnp.zeros_like(gcell)

    start = pl.multiple_of(step * QB, QB)
    span = pl.ds(start, SPAN)
    mask = jnp.where(kwin[span, :] == qwin[...], 0.0, NEG)
    hot = khot[span, :]
    hot_t = khott[:, span]
    cells = qhott[...]
    cells_r = qhot[...]
    for g in range(groups):
        lanes = slice(128 * g, 128 * (g + 1))
        q_stack = stack_heads(qt[lanes, :])
        do_stack = stack_heads(dot_t[lanes, :])
        right = jnp.concatenate([q_stack, bias_rows(table, g, cells)], axis=0)
        scores = dot(jnp.concatenate([kx[span, lanes], hot], axis=1), right)
        dprob = dot(vx[span, lanes], do_stack)
        ps, dss, dqs = [], [], []
        for j in range(GROUP):
            h = GROUP * g + j
            cut = slice(QB * j, QB * (j + 1))
            p = jnp.exp(scores[:, cut] * SCALE + mask - lse[h : h + 1, :])
            t = p * dprob[:, cut]
            inner = jnp.sum(t, axis=0, keepdims=True)
            ds = (t - p * inner).astype(BF16)
            ps.append(p.astype(BF16))
            dss.append(ds)
            both = dot(jnp.concatenate([kt[HEAD_DIM * h : HEAD_DIM * (h + 1), span], hot_t], axis=0), ds)
            dqs.append(both[:HEAD_DIM])
            gcell[CP * h : CP * (h + 1), :] += dot(both[HEAD_DIM:].astype(BF16), cells_r)
        dq[:, lanes] = (jnp.concatenate(dqs, axis=0) * SCALE).T.astype(BF16)
        dk_acc[span, lanes] += dot_nt(jnp.concatenate(dss, axis=1), q_stack)
        dv_acc[span, lanes] += dot_nt(jnp.concatenate(ps, axis=1), do_stack)

    @pl.when(step == rows_all // QB - 1)
    def _():
        inner_rows = pl.ds(HALO, rows_all)
        dk[...] = (dk_acc[inner_rows, :] * SCALE).astype(BF16)
        dv[...] = dv_acc[inner_rows, :].astype(BF16)
        swap.wait()
        out[...] = (keep[...] + got[...].astype(F32)).astype(BF16)


def attn_bwd(keep, give, qt, kx, kt, vx, dot_t, khot, khott, qhott, qhot, table, kwin, qwin, lse):
    width, rows = qt.shape
    heads = width // HEAD_DIM
    ext = rows + 2 * HALO
    half = keep.shape[1]
    shape = jax.ShapeDtypeStruct
    rblk = lambda n: pl.BlockSpec((QB, n), lambda i: (i, 0))
    return pl.pallas_call(
        partial(attn_bwd_kernel, heads // GROUP),
        grid=(rows // QB,),
        in_specs=[
            whole(keep), pl.BlockSpec(memory_space=pltpu.VMEM),
            cols(width), whole(kx), whole(kt), whole(vx), cols(width), whole(khot), whole(khott),
            cols(CP), rblk(CP), whole(table), whole(kwin), cols(1), cols(heads),
        ],
        out_specs=[
            same(rows, half), rblk(width), same(rows, width), same(rows, width), same(CP * heads, CP),
        ],
        out_shape=[
            shape((rows, half), BF16), shape((rows, width), BF16), shape((rows, width), BF16),
            shape((rows, width), BF16), shape((CP * heads, CP), F32),
        ],
        scratch_shapes=[
            pltpu.VMEM((ext, width), F32), pltpu.VMEM((ext, width), F32), pltpu.VMEM((rows, half), BF16),
        ] + two_sems(1),
        compiler_params=pltpu.CompilerParams(collective_id=2, has_side_effects=True),
        name="attn_bwd",
    )(keep, give, qt, kx, kt, vx, dot_t, khot, khott, qhott, qhot, table, kwin, qwin, lse)


def close_kernel(
    tok, a, dq, dk, dv, wt, gain, gr, vec2, vec_in, table, out, late,
    ga_s, give, got, stat, stat_p, wide, vec_s, vec_p, send_sem, recv_sem,
):
    rows_all, model = tok.shape
    width = dq.shape[1]
    half = out.shape[1]
    chunks = rows_all // CLOSE_ROWS
    me = lax.axis_index("mp")
    own = half_lanes(me, half)
    other = half_lanes(1 - me, half)
    greet()
    vec_s[...] = jnp.zeros_like(vec_s)
    main = lambda c: rows_copy(give, got, CLOSE_ROWS, (send_sem.at[0], recv_sem.at[0]), c)
    side = lambda c: rows_copy(stat, stat_p, CLOSE_ROWS, (send_sem.at[1], recv_sem.at[1]), c)
    lane = lax.broadcasted_iota(jnp.int32, (CLOSE_ROWS, 128), 1)

    def norms(at):
        x = tok[at, :].astype(F32)
        center = x - jnp.mean(x, axis=-1, keepdims=True)
        r = lax.rsqrt(jnp.mean(center * center, axis=-1, keepdims=True) + EPS)
        return center * r, r

    def forward(c, carry):
        at = pl.ds(pl.multiple_of(c * CLOSE_ROWS, CLOSE_ROWS), CLOSE_ROWS)
        ga = dot(dq[at, :], wt[:width, :]) + dot(dk[at, :], wt[width : 2 * width, :])
        ga = ga + dot(dv[at, :], wt[2 * width :, :])
        wide[...] = ga
        give[at, :] = wide[:, other].astype(BF16)
        ga_s[at, :] = wide[:, own]
        n, r = norms(at)
        e = ga * gain[...]
        first = jnp.mean(e, axis=-1, keepdims=True)
        second = jnp.mean(e * n, axis=-1, keepdims=True)
        stat[at, :] = jnp.where(lane == 0, first, jnp.where(lane == 1, second, 0.0))
        vec_s[0:1, :] += jnp.sum(ga * n, axis=0, keepdims=True)
        vec_s[1:2, :] += jnp.sum(ga, axis=0, keepdims=True)
        main(c).start()
        side(c).start()
        return carry

    lax.fori_loop(0, chunks, forward, 0)
    vectors = to_peer(vec_s, vec_p, send_sem.at[2, 0], recv_sem.at[2, 0])
    grads = jnp.concatenate([dq[...], dk[...], dv[...]], axis=1)
    for b in range(2):
        block = dot_tn(a[:, width * b : width * (b + 1)], grads).astype(BF16)
        for c in range(3):
            k = 2 * c + b
            goal = (width * (k % 3), width * (k // 3))
            late[goal[0] : goal[0] + width, goal[1] : goal[1] + width] = block[:, width * c : width * (c + 1)]
    vectors.start()
    qv = [jnp.sum(item[...].astype(F32), axis=0, keepdims=True) for item in (dq, dv)]

    def backward(c, carry):
        at = pl.ds(pl.multiple_of(c * CLOSE_ROWS, CLOSE_ROWS), CLOSE_ROWS)
        main(c).wait()
        side(c).wait()
        sums = stat[at, :] + stat_p[at, :]
        n, r = norms(at)
        wide[...] = n
        e = (ga_s[at, :] + got[at, :].astype(F32)) * gain[:, own]
        gx = gr[at, :] + r * (e - sums[:, 0:1] - wide[:, own] * sums[:, 1:2])
        out[at, :] = gx.astype(BF16)
        return carry

    lax.fori_loop(0, chunks, backward, 0)
    vectors.wait()
    first = vec_s[0:2, :] + vec_p[0:2, :]
    parts = [first[0:1], first[1:2]] + [vec2[k : k + 1, :] for k in range(4)]
    parts.append(jnp.concatenate(qv, axis=1))
    parts += [vec_in[:, model * k : model * (k + 1)] for k in range(vec_in.shape[1] // model)]
    parts += [table[k : k + 1, :] for k in range(table.shape[0])]
    parts.append(jnp.zeros((SMALL - len(parts), model), F32))
    late[3 * width : 3 * width + SMALL, :] = jnp.concatenate(parts, axis=0).astype(BF16)
    spare = late.shape[0] - 3 * width - SMALL
    late[3 * width + SMALL :, :] = jnp.zeros((spare, model), BF16)


def close(late_rows, tok, a, dq, dk, dv, wt, gain, gr, vec2, vec_in, table):
    rows, model = tok.shape
    width = dq.shape[1]
    half = gr.shape[1]
    chunks = rows // CLOSE_ROWS
    shape = jax.ShapeDtypeStruct
    vm = pltpu.VMEM
    sems = pltpu.SemaphoreType.DMA((3, chunks))
    return pl.pallas_call(
        close_kernel,
        in_specs=[pl.BlockSpec(memory_space=pltpu.VMEM)] * 11,
        out_specs=[pl.BlockSpec(memory_space=pltpu.VMEM)] * 2,
        out_shape=[shape((rows, half), BF16), shape((late_rows, model), BF16)],
        scratch_shapes=[
            vm((rows, half), F32), vm((rows, half), BF16), vm((rows, half), BF16), vm((rows, 128), F32),
            vm((rows, 128), F32), vm((CLOSE_ROWS, model), F32), vm((8, model), F32), vm((8, model), F32),
            sems, sems,
        ],
        compiler_params=pltpu.CompilerParams(collective_id=3, has_side_effects=True),
        name="close",
    )(tok, a, dq, dk, dv, wt, gain, gr, vec2, vec_in, table)


def dp_copy(src, dst, partner, send_sem, recv_sem):
    return pltpu.make_async_remote_copy(
        src_ref=src,
        dst_ref=dst,
        send_sem=send_sem,
        recv_sem=recv_sem,
        device_id={"dp": partner},
        device_id_type=MESH,
    )


def dp_sum_kernel(flows, x, big, small, out, acc, got, send_sem, recv_sem):
    rows = x.shape[0]
    steps = len(flows[0][0])
    place = lax.axis_index("dp")

    def bit_of(b):
        return lax.rem(lax.div(place, 1 << b), 2)

    def partner_of(b):
        return place + (1 - 2 * bit_of(b)) * (1 << b)

    barrier = pltpu.get_barrier_semaphore()
    for b in range(steps):
        pl.semaphore_signal(barrier, inc=1, device_id={"dp": partner_of(b)}, device_id_type=MESH)
    pl.semaphore_wait(barrier, steps)

    lows = [[0] for _ in flows]
    for k, (order, _, _) in enumerate(flows):
        for s in range(steps):
            lows[k].append(lows[k][s] + bit_of(order[s]) * (rows >> (s + 1)))

    def halve(k, s):
        order, lane, count = flows[k]
        size = rows >> (s + 1)
        lanes = pl.ds(lane, count)
        theirs = pl.multiple_of(lows[k][s] + (1 - bit_of(order[s])) * size, 16)
        copy = dp_copy(
            (x if s == 0 else acc).at[pl.ds(theirs, size), lanes],
            got.at[pl.ds(rows - (rows >> s), size), lanes],
            partner_of(order[s]),
            send_sem.at[k, s],
            recv_sem.at[k, s],
        )
        copy.start()
        return copy

    def add(k, s):
        _, lane, count = flows[k]
        size = rows >> (s + 1)
        base = rows - (rows >> s)
        lanes = slice(lane, lane + count)
        mine = pl.ds(pl.multiple_of(lows[k][s + 1], 16), size)
        total = (x if s == 0 else acc)[mine, lanes].astype(F32) + got[base : base + size, lanes].astype(F32)
        (out if s == steps - 1 else acc)[mine, lanes] = total.astype(BF16)

    def double(k, s):
        order, lane, count = flows[k]
        at = 2 * steps - 1 - s
        region = out.at[pl.ds(pl.multiple_of(lows[k][s + 1], 16), rows >> (s + 1)), pl.ds(lane, count)]
        copy = dp_copy(region, region, partner_of(order[s]), send_sem.at[k, at], recv_sem.at[k, at])
        copy.start()
        return copy

    copies = [halve(k, 0) for k in range(len(flows))]
    for s in range(steps):
        for k in range(len(flows)):
            copies[k].wait()
            add(k, s)
            copies[k] = halve(k, s + 1) if s + 1 < steps else double(k, s)
    for s in reversed(range(steps)):
        for k in range(len(flows)):
            copies[k].wait()
            if s > 0:
                copies[k] = double(k, s - 1)
    tall = big.shape[0] // 2
    for k in range(2):
        big[tall * k : tall * (k + 1), :] = out[:tall, big.shape[1] * k : big.shape[1] * (k + 1)]
    small[...] = out[tall : tall + small.shape[0], :].astype(F32)


def dp_sum(ranks, big_shape, x):
    rows, wide = x.shape
    steps = ranks.bit_length() - 1
    first, second = list(range(steps)), [0] + list(range(2, steps)) + [1]
    flows = [(first, 0, 256), (second, 256, 256), (first, 512, 128), (second, 640, 128)]
    vm = pltpu.VMEM
    sems = pltpu.SemaphoreType.DMA((len(flows), 2 * steps))
    return pl.pallas_call(
        partial(dp_sum_kernel, flows),
        in_specs=[pl.BlockSpec(memory_space=pltpu.VMEM)],
        out_specs=[pl.BlockSpec(memory_space=pltpu.VMEM)] * 2,
        out_shape=[jax.ShapeDtypeStruct(big_shape, BF16), jax.ShapeDtypeStruct((SMALL, wide), F32)],
        scratch_shapes=[vm((rows, wide), BF16)] * 3 + [sems, sems],
        compiler_params=pltpu.CompilerParams(collective_id=4, has_side_effects=True),
        name="dp_sum",
    )(x)


def window_data(crop_counts, crop_patches, rel_index, rel_table, rows):
    highest = lax.Precision.HIGHEST
    heads = rel_table.shape[1]
    cells, wins = layout(crop_counts, crop_patches, rows)
    kcells = jnp.pad(cells, (HALO, HALO))
    kwin = jnp.pad(wins, (HALO, HALO), constant_values=-1)[:, None]
    span_cells = jnp.arange(CP, dtype=jnp.int32)
    wide_cells = jnp.arange(2 * CP, dtype=jnp.int32) % CP
    khot = (kcells[:, None] == wide_cells[None, :]).astype(BF16)
    khott = (span_cells[:, None] == kcells[None, :]).astype(BF16)
    qhott = (span_cells[:, None] == cells[None, :]).astype(BF16)
    qhot = (cells[:, None] == span_cells[None, :]).astype(BF16)
    rel_t = jnp.pad(rel_index.T, ((0, CP - CELLS), (0, CP - CELLS)), constant_values=-1).reshape(-1)
    offset_hot = (rel_t[:, None] == jnp.arange(OFFSETS, dtype=jnp.int32)[None, :]).astype(F32)
    bias = jnp.einsum("pm,mh->hp", offset_hot, rel_table, precision=highest) / SCALE
    high = bias.astype(BF16)
    rest = (bias - high.astype(F32)).astype(BF16)
    table = jnp.stack([high.reshape(heads, CP, CP), rest.reshape(heads, CP, CP)], axis=1)
    return (khot, khott, qhott, qhot, table.reshape(heads * 2 * CP, CP), kwin, wins[None, :], offset_hot)


def body(
    tokens,
    crop_counts,
    crop_patches,
    rel_index,
    ln1_gain,
    ln1_shift,
    w_qkv,
    qv_bias,
    rel_table,
    w_out,
    b_out,
    ln2_gain,
    ln2_shift,
    w_in,
    b_in,
    w_back,
    b_back,
    cotangent,
):
    highest = lax.Precision.HIGHEST
    rows, part_width = tokens.shape
    model = ln1_gain.shape[0]
    width = w_qkv.shape[2]
    heads = width // HEAD_DIM
    khot, khott, qhott, qhot, table, kwin, qwin, offset_hot = window_data(
        crop_counts, crop_patches, rel_index, rel_table, rows
    )
    low = rows // 2
    whole_low = lax.all_gather(tokens[:low], "mp", axis=1, tiled=True)
    wt = jnp.transpose(w_qkv, (1, 2, 0)).reshape(3 * width, model)
    whole_in, mixer_in, qt, kx, kt, vx, heads_out, heads_peer, w_peer, whole_cot, lse = attn_fwd(
        w_out, cotangent, whole_low, tokens[low:], ln1_gain[None, :], ln1_shift[None, :], wt, qv_bias[0][:, None], qv_bias[1][:, None],
        qv_bias[1][None, :], khot, qhott, table, kwin, qwin,
    )
    keep, give, gr, dot_t, grad_w_out, grad_w_in, grad_w_back, vec2, grad_b_in = ffn(
        whole_in, heads_out, heads_peer, w_out, w_peer, b_out[None, :], ln2_gain[None, :], ln2_shift[None, :],
        w_in, b_in[None, :], w_back, b_back[None, :], whole_cot,
    )
    early = lax.psum((grad_w_in, grad_w_back, grad_w_out), "dp")
    out_half, grad_query, grad_key, grad_value, gcell = attn_bwd(
        keep, give, qt, kx, kt, vx, dot_t, khot, khott, qhott, qhot, table, kwin, qwin, lse
    )
    grad_table = jnp.einsum(
        "pm,hp->mh", offset_hot, gcell.reshape(heads, CP * CP), precision=highest
    )
    table_rows = -(-grad_table.size // model)
    table_flat = jnp.pad(grad_table.reshape(-1), (0, table_rows * model - grad_table.size))
    ranks = lax.axis_size("dp")
    late_rows = -(-(3 * width + SMALL) // (16 * ranks)) * 16 * ranks
    grad_half, late = close(
        late_rows, whole_in, mixer_in, grad_query, grad_key, grad_value, wt, ln1_gain[None, :], gr,
        vec2, grad_b_in, table_flat.reshape(table_rows, model),
    )
    big, small = dp_sum(ranks, (3 * model, width), late)
    big = big.astype(F32)
    early, big = lax.optimization_barrier((early, big))
    grad_w_in, grad_w_back, grad_w_out = (item.astype(F32) for item in early)
    grad_w_qkv = jnp.transpose(big.reshape(3, model, width), (1, 0, 2))
    grad_g1, grad_c1, grad_g2, grad_c2, grad_b_out, grad_b_back = (small[k] for k in range(6))
    grad_qv_bias = small[6].reshape(2, width)
    hidden_rows = w_in.shape[1] // model
    grad_b_in = small[7 : 7 + hidden_rows].reshape(-1)
    flat = small[7 + hidden_rows : 7 + hidden_rows + table_rows].reshape(-1)
    grad_table = flat[: grad_table.size].reshape(grad_table.shape)
    return (
        out_half,
        grad_half,
        grad_g1,
        grad_c1,
        grad_w_qkv,
        grad_qv_bias,
        grad_table,
        grad_w_out,
        grad_b_out,
        grad_g2,
        grad_c2,
        grad_w_in,
        grad_b_in,
        grad_w_back,
        grad_b_back,
    )


def solution(mesh):
    return jax.shard_map(
        body,
        mesh=mesh,
        in_specs=(
            P("dp", "mp"),
            P("dp"),
            P("dp", None),
            P(),
            P(),
            P(),
            P(None, None, "mp"),
            P(None, "mp"),
            P(None, "mp"),
            P("mp", None),
            P(),
            P(),
            P(),
            P(None, "mp"),
            P("mp"),
            P("mp", None),
            P(),
            P("dp", "mp"),
        ),
        out_specs=(
            P("dp", "mp"),
            P("dp", "mp"),
            P(),
            P(),
            P(None, None, "mp"),
            P(None, "mp"),
            P(None, "mp"),
            P("mp", None),
            P(),
            P(),
            P(),
            P(None, "mp"),
            P("mp"),
            P("mp", None),
            P(),
        ),
        check_vma=False,
    )
```
